128 devices in a mesh: ep: 32 (over y, x, core), tp: 4 (over z).
Axes of the slice: x: 4, y: 4, z: 4, core: 2. Of those that a mesh axis runs over, the one named last changes fastest.
Arguments:
- tokens: bfloat16 [8192, 7168], P('ep', 'tp'), may hold values from -78 to 78
- norm_gain: bfloat16 [7168], P('tp'), may hold values from 0.5 to 1.5
- expert_ids: int32 [8192, 8], P('ep'), may hold values from 0 to 255, all different within a row
- gate_prob: bfloat16 [8192, 8], P('ep'), may hold values from 0.049804688 to 1
- w_gate: bfloat16 [32, 7168, 2048], P('ep', None, 'tp'), may hold values from -0.0625 to 0.0625
- w_up: bfloat16 [32, 7168, 2048], P('ep', None, 'tp'), may hold values from -0.0625 to 0.0625
- w_down: bfloat16 [32, 2048, 7168], P('ep', 'tp'), may hold values from -0.125 to 0.125
Outputs:
- combined: bfloat16 [8192, 7168], P('ep', 'tp')
The draws below stay inside these ranges and needn't reach their ends.
Inputs may be any that keep to these rules, and one draw needn't show every extreme that they name: `expert_ids`: each row names 8 different experts.
All inputs are finite; a program needn't handle non-finite values.
Results may differ from the reference program's by a relative error of at most 0.01.
Values may be sent and summed in bfloat16 or wider, within the bound.
No kernel may reach another device: no remote copies, remote signals or barrier semaphores. Data moves between devices by JAX's collectives and lax.ppermute only.
A program may use at most 128 MiB of HBM per device.

```python
import math
import jax
import jax.numpy as jnp
from jax import lax

D = 7168
FF = 2048
TOP = 8
TOK_DEV = 256
EXPERTS = 256
WINDOW = 32
TOKENS = 8192
CAP = 16
N_TP = 4


def draw_tokens(key, part):
    base_key = jax.random.fold_in(key, 11)
    row_key = jax.random.fold_in(key, 12)
    col_key = jax.random.fold_in(key, 13)
    rows_scale = jnp.exp(jax.random.uniform(row_key, (TOKENS, 1), jnp.float32, math.log(0.3), math.log(3.0)))
    rising = 3.0 ** (jnp.arange(D, dtype=jnp.float32) / D - 0.5)
    cols_scale = rising * jnp.exp(jax.random.uniform(col_key, (D,), jnp.float32, math.log(0.4), math.log(2.5)))
    base = jnp.clip(jax.random.normal(base_key, (TOKENS, D), jnp.float32), -6.0, 6.0)
    return (base * rows_scale * cols_scale[None, :]).astype(jnp.bfloat16)


def block_levels(key, shape, pieces, low, largest):
    def one(dim, shards_of):
        heights = jax.random.uniform(jax.random.fold_in(jax.random.fold_in(key, 6), dim), (shards_of,), jnp.float32, low / len(pieces), largest / len(pieces))
        return jnp.repeat(jnp.exp(heights), shape[dim] // shards_of).reshape((-1,) + (1,) * (len(shape) - dim - 1))

    factor_of = one(*pieces[0])
    for cut in pieces[1:]:
        factor_of = factor_of * one(*cut)
    return factor_of


def distinct(own_key, rows, amount, top, lift):
    sequence = jax.random.permutation(jax.random.fold_in(own_key, 1), amount)
    boost = sequence
    for power in range(3):
        boost = boost * boost // amount
    boost = boost * lift // amount
    lots = jax.random.randint(jax.random.fold_in(own_key, 2), (rows, amount), 0, 4096) + boost
    sure = jax.random.permutation(jax.random.fold_in(own_key, 3), rows)[jnp.arange(amount) % rows]
    lots = jnp.where(jnp.arange(rows)[:, None] == sure[None, :], 1 << 14, lots)
    score = lots * amount + jnp.arange(amount)
    return lax.top_k(score.astype(jnp.int32), top)[1].astype(jnp.int32)


def noise(own_key, shape, width, reach, shards=(), kind=jnp.bfloat16):
    array = jax.random.normal(own_key, shape, jnp.float32) * width
    if len(shards) > 0:
        array = block_levels(own_key, shape, shards, -0.22, 0.18) * array
    return jnp.clip(array, min=-reach, max=reach).astype(kind)


def setup_inputs(seed: int = 0) -> dict:
    arg_keys = jax.random.split(jax.random.key(seed), 8)
    tokens = draw_tokens(jax.random.fold_in(arg_keys[7], 71), 0)
    norm_gain = jnp.clip(1.0 + 0.1 * jax.random.normal(arg_keys[1], (D,), jnp.float32), 0.5, 1.5).astype(jnp.bfloat16)
    expert_ids = distinct(arg_keys[2], TOKENS, EXPERTS, TOP, 512)
    gate_prob = jnp.clip(jnp.exp(math.log(1.0) - 2.9996462 * jax.random.uniform(arg_keys[3], (TOKENS, TOP), jnp.float32) ** block_levels(arg_keys[3], (TOKENS, TOP), ((0, 32),), -0.2, 0.2)), 0.049804688, 1.0).astype(jnp.bfloat16)
    w_gate = noise(arg_keys[4], (WINDOW, D, FF), D ** -0.5, 0.0625, ((0, 32), (2, 4)))
    w_up = noise(arg_keys[5], (WINDOW, D, FF), D ** -0.5, 0.0625, ((0, 32), (2, 4)))
    w_down = noise(arg_keys[6], (WINDOW, FF, D), FF ** -0.5, 0.125, ((0, 32), (1, 4)))
    return dict(tokens=tokens, norm_gain=norm_gain, expert_ids=expert_ids, gate_prob=gate_prob, w_gate=w_gate, w_up=w_up, w_down=w_down)


epsilon = 1e-06

def slots_of(expert_ids):
    is_live = expert_ids < WINDOW
    matches = (expert_ids[:, :, None] == jnp.arange(WINDOW, dtype=jnp.int32)).astype(jnp.int32)
    counts = lax.optimization_barrier(jnp.sum(matches, axis=1))
    blocked = counts.reshape(-1, TOK_DEV, WINDOW)
    before = (jnp.cumsum(blocked, axis=1) - blocked).reshape(-1, WINDOW)
    slot_index = lax.optimization_barrier(jnp.sum(matches * before[:, None, :], axis=2))
    is_kept = is_live & (slot_index < CAP)
    return (slot_index, is_kept)

def reference(tokens, norm_gain, expert_ids, gate_prob, w_gate, w_up, w_down):
    values = tokens.astype(jnp.float32)
    mean_square = lax.optimization_barrier(jnp.mean(values * values, axis=1, keepdims=True))
    normed = (values * lax.rsqrt(mean_square + epsilon) * norm_gain.astype(jnp.float32)).astype(jnp.bfloat16)
    slot_index, is_kept = slots_of(expert_ids)
    block_count = TOKENS // TOK_DEV
    block_index = (jnp.arange(TOKENS, dtype=jnp.int32) // TOK_DEV)[:, None]
    slot_total = WINDOW * block_count * CAP
    flat_index = jnp.where(is_kept, (expert_ids * block_count + block_index) * CAP + slot_index, slot_total).astype(jnp.int32)
    buffer = jnp.zeros((slot_total, D), jnp.bfloat16)
    for column in range(TOP):
        buffer = buffer.at[flat_index[:, column]].set(normed, mode='drop')
    buffer = buffer.reshape(WINDOW, block_count * CAP, D)
    block_width = FF // N_TP

    def one_expert(operands):
        rows_in, gate_matrix, up_matrix, down_matrix = operands
        gate_act = jnp.dot(rows_in, gate_matrix, preferred_element_type=jnp.float32)
        up_act = jnp.dot(rows_in, up_matrix, preferred_element_type=jnp.float32)
        hidden = (jax.nn.silu(gate_act) * up_act).astype(jnp.bfloat16)
        summed = jnp.zeros((rows_in.shape[0], D), jnp.float32)
        for block_number in range(N_TP):
            lower = block_number * block_width
            down_part = jnp.dot(hidden[:, lower:lower + block_width], down_matrix[lower:lower + block_width], preferred_element_type=jnp.float32)
            rounded = lax.optimization_barrier(down_part.astype(jnp.bfloat16))
            summed = summed + rounded.astype(jnp.float32)
        return summed.astype(jnp.bfloat16)
    expert_out = lax.map(one_expert, (buffer, w_gate, w_up, w_down)).reshape(slot_total, D)
    combined = jnp.zeros((TOKENS, D), jnp.float32)
    for column in range(TOP):
        picked = jnp.take(expert_out, flat_index[:, column], axis=0, mode='fill', fill_value=0).astype(jnp.float32)
        combined = combined + gate_prob[:, column:column + 1].astype(jnp.float32) * picked
    return combined.astype(jnp.bfloat16)
```

```python
import jax
import jax.numpy as jnp
from jax import lax
from jax.experimental import pallas as pl
from jax.experimental.pallas import tpu as pltpu
from jax.sharding import PartitionSpec as P

D = 7168
epsilon = 1e-06
CAP = 16
CHUNKS = (8, 8)


def ring(axis, step):
    n = lax.axis_size(axis)
    return [(i, (i + step) % n) for i in range(n)]


def gate_up(where, pieces, w_gate, w_up):
    rows = pieces[0].shape[0]
    d_all, ff = w_gate.shape
    width = d_all // 8
    spans = []
    at = 0
    for piece in pieces:
        count = piece.shape[1] // width
        spans.append((at, count))
        at += count

    def body(where_ref, *refs):
        n = len(pieces)
        xs, (wg, wu, out, acc_g, acc_u) = refs[:n], refs[n:]
        j = pl.program_id(0)
        for x, (lo, count) in zip(xs, spans):

            @pl.when((j >= lo) & (j < lo + count))
            def _(x=x, lo=lo):
                v = x[...]
                g = jnp.dot(v, wg[...], preferred_element_type=jnp.float32)
                u = jnp.dot(v, wu[...], preferred_element_type=jnp.float32)
                if lo == 0:

                    @pl.when(j == 0)
                    def _():
                        acc_g[...] = g
                        acc_u[...] = u

                    @pl.when(j != 0)
                    def _():
                        acc_g[...] += g
                        acc_u[...] += u
                else:
                    acc_g[...] += g
                    acc_u[...] += u

        @pl.when(j == at - 1)
        def _():
            out[...] = (jax.nn.silu(acc_g[...]) * acc_u[...]).astype(out.dtype)

    def piece_spec(lo, count):
        return pl.BlockSpec((rows, width), lambda j, w: (0, jnp.clip(j - lo, 0, count - 1)))

    w_spec = pl.BlockSpec((width, ff), lambda j, w: ((2 * w[0] + j) % 8, 0))
    return pl.pallas_call(
        body,
        grid_spec=pltpu.PrefetchScalarGridSpec(
            num_scalar_prefetch=1,
            grid=(at,),
            in_specs=[piece_spec(*s) for s in spans] + [w_spec, w_spec],
            out_specs=pl.BlockSpec((rows, ff), lambda j, w: (0, 0)),
            scratch_shapes=[pltpu.VMEM((rows, ff), jnp.float32)] * 2,
        ),
        out_shape=jax.ShapeDtypeStruct((rows, ff), jnp.bfloat16),
        cost_estimate=pl.CostEstimate(
            flops=4 * rows * d_all * ff,
            bytes_accessed=4 * d_all * ff + 2 * rows * d_all,
            transcendentals=rows * ff,
        ),
        name="gate_up",
    )(where, *pieces, w_gate, w_up)


def down(where, hidden, w_down, steps):
    rows, ff = hidden.shape
    d_all = w_down.shape[1]
    width = d_all // 8
    parts = len(steps)

    def column(j):
        block = 2 * steps[0] + j
        for k in range(1, parts):
            block = block + jnp.where(j >= 2 * k, 2 * (steps[k] - steps[k - 1] - 1), 0)
        return block

    def body(where_ref, h, w, *outs):
        j = pl.program_id(0)
        for k, out in enumerate(outs):

            @pl.when(j // 2 == k)
            def _(out=out):
                out[...] = jnp.dot(h[...], w[...], preferred_element_type=jnp.float32).astype(out.dtype)

    def out_spec(k):
        return pl.BlockSpec((rows, width), lambda j, w: (0, jnp.clip(j - 2 * k, 0, 1)))

    return pl.pallas_call(
        body,
        grid_spec=pltpu.PrefetchScalarGridSpec(
            num_scalar_prefetch=1,
            grid=(2 * parts,),
            in_specs=[
                pl.BlockSpec((rows, ff), lambda j, w: (0, 0)),
                pl.BlockSpec((ff, width), lambda j, w: (0, (2 * w[0] + column(j)) % 8)),
            ],
            out_specs=[out_spec(k) for k in range(parts)],
        ),
        out_shape=[jax.ShapeDtypeStruct((rows, 2 * width), jnp.bfloat16)] * parts,
        cost_estimate=pl.CostEstimate(
            flops=4 * rows * width * parts * ff,
            bytes_accessed=4 * width * parts * (ff + rows),
            transcendentals=0,
        ),
        name="down",
    )(where, hidden, w_down)


def place_picks(expert_ids, gate_prob, window):
    ids = expert_ids.T
    probs = gate_prob.T.astype(jnp.float32)
    tok = ids.shape[1]
    same = ids[:, None, :] == jnp.arange(window, dtype=jnp.int32)[None, :, None]
    match = jnp.any(same, axis=0).astype(jnp.bfloat16)
    prob = jnp.sum(jnp.where(same, probs[:, None, :], 0.0), axis=0)
    earlier = (jnp.arange(tok)[:, None] < jnp.arange(tok)[None, :]).astype(jnp.bfloat16)
    before = jnp.dot(match, earlier, preferred_element_type=jnp.float32)
    slot = jnp.where(match > 0, before, -1.0)
    slots = jnp.arange(CAP, dtype=jnp.float32)
    hit = slot[:, None, :] == slots[None, :, None]
    return hit, prob


def local(tokens, norm_gain, expert_ids, gate_prob, w_gate, w_up, w_down):
    window = lax.axis_size("ep")
    n_tp = lax.axis_size("tp")
    z = lax.axis_index("tp")
    w_gate, w_up, w_down = w_gate[0], w_up[0], w_down[0]
    width = tokens.shape[1]
    half = width // 2

    where = z.astype(jnp.int32).reshape(1)
    values = tokens.astype(jnp.float32)
    square_part = jnp.sum(values * values, axis=1)
    everyone = lax.all_to_all(jnp.broadcast_to(square_part[None, None], (n_tp, 1, tokens.shape[0])), "tp", 0, 0, tiled=True)
    inverse_rms = lax.rsqrt(jnp.sum(everyone, axis=(0, 1)) / D + epsilon)
    normed = (values * inverse_rms[:, None] * norm_gain.astype(jnp.float32)).astype(jnp.bfloat16)
    hit, prob = place_picks(expert_ids, gate_prob, window)

    up, dn = ring("tp", 1), ring("tp", -1)

    starts = [sum(CHUNKS[:k]) for k in range(len(CHUNKS))]
    combined = None
    for start, count in zip(starts, CHUNKS):
        own_hit = hit[:, start : start + count]
        rows = window * count
        pick = own_hit.astype(jnp.bfloat16).reshape(rows, -1)
        outgoing = jnp.dot(pick, normed, preferred_element_type=jnp.float32).astype(jnp.bfloat16)
        mine = lax.all_to_all(outgoing.reshape(window, count, width), "ep", 0, 0, tiled=True)
        mine = mine.reshape(rows, width)
        below = lax.ppermute(mine, "tp", up)
        above = lax.ppermute(mine, "tp", dn)
        far_a = lax.ppermute(below[:, :half], "tp", up)
        far_b = lax.ppermute(above[:, half:], "tp", dn)
        hidden = gate_up(where, (mine, above, far_a, far_b, below), w_gate, w_up)
        (part_far,) = down(where, hidden, w_down, (2,))
        got_a = lax.ppermute(part_far[:, :half], "tp", up)
        got_b = lax.ppermute(part_far[:, half:], "tp", dn)
        part_own, part_up, part_dn = down(where, hidden, w_down, (0, 1, 3))
        f32 = jnp.float32
        sum_up = (part_up.astype(f32) + jnp.pad(got_a.astype(f32), ((0, 0), (0, half)))).astype(jnp.bfloat16)
        sum_dn = (part_dn.astype(f32) + jnp.pad(got_b.astype(f32), ((0, 0), (half, 0)))).astype(jnp.bfloat16)
        from_dn = lax.ppermute(sum_up, "tp", up)
        from_up = lax.ppermute(sum_dn, "tp", dn)
        total = (part_own.astype(f32) + from_dn.astype(f32) + from_up.astype(f32)).astype(jnp.bfloat16)
        back = lax.all_to_all(total.reshape(window, count, width), "ep", 0, 0, tiled=True)
        weight = jnp.where(own_hit, prob[:, None, :], 0.0).astype(jnp.bfloat16).reshape(rows, -1)
        share = lax.dot_general(weight, back.reshape(rows, width), (((0,), (0,)), ((), ())), preferred_element_type=f32)
        combined = share if combined is None else combined + share
    return combined.astype(jnp.bfloat16)


def solution(mesh):
    placed = (
        P("ep", "tp"),
        P("tp"),
        P("ep", None),
        P("ep", None),
        P("ep", None, "tp"),
        P("ep", None, "tp"),
        P("ep", "tp", None),
    )
    return jax.shard_map(
        local, mesh=mesh, in_specs=placed, out_specs=P("ep", "tp"), check_vma=False
    )
```

```python
import jax
import jax.numpy as jnp
from jax import lax
from jax.experimental import pallas as pl
from jax.experimental.pallas import tpu as pltpu
from jax.sharding import PartitionSpec as P

D = 7168
epsilon = 1e-06
CAP = 16
EARLY = 384
BULK = (640, 768)
SIDE = 128
F32, BF16 = jnp.float32, jnp.bfloat16


class Copies:
    def __init__(self, sems):
        self.sems, self.used = sems, 0

    def start(self, src, dst):
        copy = pltpu.make_async_copy(src, dst, self.sems.at[self.used])
        self.used += 1
        copy.start()
        return copy


def expert_call(name, where, xs, segs, w_gate, w_up, carry, inv, hidden, w_down, jobs, outs):
    slices = lax.axis_size("tp")
    d_all, ff = (w_down.shape[1], w_down.shape[0]) if w_gate is None else w_gate.shape
    span = d_all // slices
    rows = hidden.shape[0] if hidden is not None else 2 * min(x.shape[0] for x in xs) if len(jobs) else xs[0].shape[0]
    finish = bool(segs) and bool(jobs)
    if not jobs:
        out_shapes = [jax.ShapeDtypeStruct((rows, ff), F32)] * 2
    else:
        out_shapes = [jax.ShapeDtypeStruct(s, BF16) for s in outs]
        if finish:
            out_shapes = [jax.ShapeDtypeStruct((rows, ff), BF16)] + out_shapes
    args = list(xs)
    if segs:
        args += [w_gate, w_up]
    if carry is not None:
        args += list(carry)
    if inv is not None:
        args += [inv]
    if hidden is not None:
        args += [hidden]
    if jobs:
        args += [w_down]
    scratch = []
    for _, _, _, width, _ in segs:
        scratch += [pltpu.VMEM((rows, width), BF16), pltpu.VMEM((width, ff), BF16), pltpu.VMEM((width, ff), BF16)]
    if segs:
        scratch += [pltpu.VMEM((rows, ff), F32)] * 2
    if inv is not None:
        scratch += [pltpu.VMEM((rows, SIDE), BF16)]
    if jobs:
        scratch += [pltpu.VMEM((rows, ff), BF16)]
    for _, _, width, _ in jobs:
        scratch += [pltpu.VMEM((ff, width), BF16), pltpu.VMEM((rows, width), BF16)]
    n_sems = sum(len(s[0]) + 2 for s in segs) + 2 + 1 + 2 + sum(1 + len(j[3]) for j in jobs)
    scratch += [pltpu.SemaphoreType.DMA((n_sems,))]

    def body(where_ref, *refs):
        refs = list(refs)
        take = lambda n: [refs.pop(0) for _ in range(n)]
        x_refs = take(len(xs))
        wg, wu = take(2) if segs else (None, None)
        carried = take(2) if carry is not None else None
        inv_ref = take(1)[0] if inv is not None else None
        hidden_ref = take(1)[0] if hidden is not None else None
        wd = take(1)[0] if jobs else None
        out_refs = take(len(out_shapes))
        seg_bufs = [take(3) for _ in segs]
        accs = take(2) if segs else None
        inv_buf = take(1)[0] if inv is not None else None
        h_buf = take(1)[0] if jobs else None
        job_bufs = [take(2) for _ in jobs]
        copies = Copies(refs.pop(0))
        z = where_ref[0]

        def first(step, offset):
            return pl.multiple_of(lax.rem(z + step, slices) * span + offset, 128)

        waits_in = []
        if carried is not None:
            waits_in = [copies.start(c, a) for c, a in zip(carried, accs)]
        seg_waits = []
        for (parts, step, offset, width, col), (xb, gb, ub) in zip(segs, seg_bufs):
            at = pl.ds(first(step, offset), width)
            mine = []
            for index, row in parts:
                count = x_refs[index].shape[0]
                mine.append(copies.start(x_refs[index].at[:, pl.ds(col, width)], xb.at[pl.ds(row, count), :]))
            mine.append(copies.start(wg.at[at, :], gb))
            mine.append(copies.start(wu.at[at, :], ub))
            seg_waits.append(mine)
        if inv is not None:
            inv_wait = copies.start(inv_ref.at[:, pl.ds(inv_ref.shape[1] - SIDE, SIDE)], inv_buf)
        if hidden is not None:
            hidden_wait = copies.start(hidden_ref, h_buf)
        job_waits = []
        for (step, offset, width, _), (wb, _) in zip(jobs, job_bufs):
            job_waits.append(copies.start(wd.at[:, pl.ds(first(step, offset), width)], wb))
        done = []
        for w in waits_in:
            w.wait()
        for k, (xb, gb, ub) in enumerate(seg_bufs):
            for w in seg_waits[k]:
                w.wait()
            for w_buf, acc in ((gb, accs[0]), (ub, accs[1])):
                term = jnp.dot(xb[...], w_buf[...], preferred_element_type=F32)
                if k == 0 and carried is None:
                    acc[...] = term
                else:
                    acc[...] += term
        if segs and not jobs:
            done += [copies.start(a, o) for a, o in zip(accs, out_refs)]
        if finish:
            inv_wait.wait()
            scale = jnp.sum(inv_buf[...].astype(F32), axis=1, keepdims=True)
            gate = accs[0][...] * scale
            h_buf[...] = (jax.nn.silu(gate) * (accs[1][...] * scale)).astype(BF16)
            done.append(copies.start(h_buf, out_refs.pop(0)))
        if hidden is not None:
            hidden_wait.wait()
        for (_, _, width, targets), (wb, ob), w in zip(jobs, job_bufs, job_waits):
            w.wait()
            ob[...] = jnp.dot(h_buf[...], wb[...], preferred_element_type=F32).astype(BF16)
            for index, row, count, col in targets:
                done.append(copies.start(ob.at[pl.ds(row, count), :], out_refs[index].at[:, pl.ds(col, width)]))
        for copy in done:
            copy.wait()

    hbm = pl.BlockSpec(memory_space=pltpu.HBM)
    flops = sum(4 * rows * s[3] * ff for s in segs) + sum(2 * rows * ff * j[2] for j in jobs)
    return pl.pallas_call(
        body,
        in_specs=[pl.BlockSpec(memory_space=pltpu.SMEM)] + [hbm] * len(args),
        out_specs=[hbm] * len(out_shapes),
        out_shape=out_shapes,
        scratch_shapes=scratch,
        cost_estimate=pl.CostEstimate(flops=flops, bytes_accessed=flops // 256, transcendentals=0),
        name=name,
    )(where, *args)


def place_picks(expert_ids, gate_prob, window):
    ids = expert_ids.T
    probs = gate_prob.T.astype(F32)
    tok = ids.shape[1]
    same = ids[:, None, :] == jnp.arange(window, dtype=jnp.int32)[None, :, None]
    match = jnp.any(same, axis=0).astype(BF16)
    prob = jnp.sum(jnp.where(same, probs[:, None, :], 0.0), axis=0)
    earlier = (jnp.arange(tok)[:, None] < jnp.arange(tok)[None, :]).astype(BF16)
    before = jnp.dot(match, earlier, preferred_element_type=F32)
    slot = jnp.where(match > 0, before, -1.0)
    hit = slot[:, None, :] == jnp.arange(CAP, dtype=F32)[None, :, None]
    pick = hit.astype(BF16).reshape(window * CAP, tok)
    weight = jnp.where(hit, prob[:, None, :], 0.0).astype(BF16).reshape(window * CAP, tok)
    return pick, weight


def three_terms(value):
    rest, terms = value, []
    for _ in range(3):
        term = lax.reduce_precision(rest, 8, 7)
        terms.append(term)
        rest = rest - term
    stacked = jnp.stack(terms, axis=1)
    return jnp.pad(stacked, ((0, 0), (0, SIDE - 3))).astype(BF16)


def local(tokens, norm_gain, expert_ids, gate_prob, w_gate, w_up, w_down):
    window, n_tp = lax.axis_size("ep"), lax.axis_size("tp")
    where = lax.axis_index("tp").astype(jnp.int32).reshape(1)
    w_gate, w_up, w_down = w_gate[0], w_up[0], w_down[0]
    tok = tokens.shape[0]
    rows = window * CAP
    up = [(i, (i + 1) % n_tp) for i in range(n_tp)]
    dn = [(i, (i - 1) % n_tp) for i in range(n_tp)]

    def spread(x):
        half = x.shape[0] // 2
        below, above = lax.ppermute(x, "tp", up), lax.ppermute(x, "tp", dn)
        return below, above, lax.ppermute(below[:half], "tp", up), lax.ppermute(above[half:], "tp", dn)

    def fold(own, above, below, far_a, far_b):
        half = own.shape[0] // 2
        got_a, got_b = lax.ppermute(far_a, "tp", up), lax.ppermute(far_b, "tp", dn)
        sum_up = (above.astype(F32) + jnp.pad(got_a.astype(F32), ((0, half), (0, 0)))).astype(BF16)
        sum_dn = (below.astype(F32) + jnp.pad(got_b.astype(F32), ((half, 0), (0, 0)))).astype(BF16)
        from_dn, from_up = lax.ppermute(sum_up, "tp", up), lax.ppermute(sum_dn, "tp", dn)
        return (own.astype(F32) + from_dn.astype(F32) + from_up.astype(F32)).astype(BF16)

    def exchange(x):
        shaped = x.reshape(window, CAP, x.shape[1])
        return lax.all_to_all(shaped, "ep", 0, 0, tiled=True).reshape(rows, x.shape[1])

    pick, weight = place_picks(expert_ids, gate_prob, window)
    gained = (tokens.astype(F32) * norm_gain.astype(F32)).astype(BF16)

    def dispatch(x):
        return jnp.dot(pick, x, preferred_element_type=F32).astype(BF16)

    offsets = [EARLY, EARLY + BULK[0]]
    mine = [exchange(dispatch(gained[:, o : o + w])) for o, w in zip(offsets, BULK)]
    square_part = jnp.sum(jnp.square(tokens.astype(F32)), axis=1)
    early = jnp.concatenate([gained[:, :EARLY], three_terms(square_part)], axis=1)
    e_below, e_above, e_far_a, e_far_b = spread(early)
    e_far = jnp.concatenate([e_far_a, e_far_b], axis=0)
    all_early = (early, e_above, e_far, e_below)
    squares = sum(jnp.sum(e[:, EARLY : EARLY + 3].astype(F32), axis=1) for e in all_early[1:]) + square_part
    inverse_rms = lax.rsqrt(squares / D + epsilon)
    early_all = jnp.concatenate([e[:, :EARLY] for e in all_early] + [three_terms(inverse_rms)], axis=1)
    early_rows = exchange(dispatch(early_all))
    pieces = [spread(m) for m in mine]

    (m1, m2), ((b1, a1, fa1, fb1), (b2, a2, fa2, fb2)) = mine, pieces
    (o1, o2), (w1, w2) = offsets, BULK
    whole = lambda i: ((i, 0),)
    sums = expert_call(
        "near_features", where, (m1, a1, b1, m2, a2, b2),
        [(whole(i), s, o, w, 0) for i, (s, o, w) in enumerate([(0, o1, w1), (1, o1, w1), (3, o1, w1), (0, o2, w2), (1, o2, w2), (3, o2, w2)])],
        w_gate, w_up, None, None, None, None, [], [],
    )
    half = rows // 2
    split = lambda i: ((i, 0, half, 0), (i + 1, half, half, 0))
    hidden, p_fa1, p_fb1, p_fa2, p_fb2 = expert_call(
        "far_features", where, (early_rows, fa1, fb1, fa2, fb2),
        [(whole(0), k, 0, EARLY, k * EARLY) for k in range(n_tp)] + [(((1, 0), (2, half)), 2, o1, w1, 0), (((3, 0), (4, half)), 2, o2, w2, 0)],
        w_gate, w_up, sums, early_rows, None, w_down,
        [(2, o1, w1, split(0)), (2, o2, w2, split(2))], [(half, w1)] * 2 + [(half, w2)] * 2,
    )
    (p_early,) = expert_call(
        "early_columns", where, (), [], None, None, None, None, hidden, w_down,
        [(k, 0, EARLY, ((0, 0, rows, k * EARLY),)) for k in range(n_tp)], [(rows, n_tp * EARLY)],
    )
    near = [(s, o, w) for o, w in zip(offsets, BULK) for s in (1, 3, 0)]
    p_a1, p_b1, p_o1, p_a2, p_b2, p_o2 = expert_call(
        "near_columns", where, (), [], None, None, None, None, hidden, w_down,
        [(s, o, w, ((i, 0, rows, 0),)) for i, (s, o, w) in enumerate(near)], [(rows, w) for _, _, w in near],
    )

    def combine(back):
        return lax.dot_general(weight, back, (((0,), (0,)), ((), ())), preferred_element_type=F32).astype(BF16)

    early_back = combine(exchange(p_early))
    e = [early_back[:, k * EARLY : (k + 1) * EARLY] for k in range(n_tp)]
    out_early = fold(e[0], e[1], e[3], e[2][: tok // 2], e[2][tok // 2 :])
    out1 = combine(exchange(fold(p_o1, p_a1, p_b1, p_fa1, p_fb1)))
    out2 = combine(exchange(fold(p_o2, p_a2, p_b2, p_fa2, p_fb2)))
    return jnp.concatenate([out_early, out1, out2], axis=1)


def solution(mesh):
    placed = (
        P("ep", "tp"),
        P("tp"),
        P("ep", None),
        P("ep", None),
        P("ep", None, "tp"),
        P("ep", None, "tp"),
        P("ep", "tp", None),
    )
    return jax.shard_map(
        local, mesh=mesh, in_specs=placed, out_specs=P("ep", "tp"), check_vma=False
    )
```

```python
import jax
import jax.numpy as jnp
from jax import lax
from jax.experimental import pallas as pl
from jax.experimental.pallas import tpu as pltpu
from jax.sharding import PartitionSpec as P


D = 7168
epsilon = 1e-06
CAP = 16
EARLY = 640
SIDE = 128
F32, BF16 = jnp.float32, jnp.bfloat16


class Copies:
    def __init__(self, sems):
        self.sems, self.used = sems, 0

    def start(self, src, dst):
        copy = pltpu.make_async_copy(src, dst, self.sems.at[self.used])
        self.used += 1
        copy.start()
        return copy


def expert_call(where, xs, segs, w_gate, w_up, carry, inv, hidden, w_down, jobs, outs):
    slices = lax.axis_size("tp")
    d_all, ff = (w_down.shape[1], w_down.shape[0]) if w_gate is None else w_gate.shape
    span = d_all // slices
    rows = (hidden if hidden is not None else carry[0] if carry is not None else xs[0]).shape[0]
    finish = bool(segs) and bool(jobs)
    if not jobs:
        out_shapes = [jax.ShapeDtypeStruct((rows, ff), F32)] * 2
    else:
        out_shapes = [jax.ShapeDtypeStruct(s, BF16) for s in outs]
        if finish:
            out_shapes = [jax.ShapeDtypeStruct((rows, ff), BF16)] + out_shapes
    args = list(xs)
    if segs:
        args += [w_gate, w_up]
    if carry is not None:
        args += list(carry)
    if inv is not None:
        args += [inv]
    if hidden is not None:
        args += [hidden]
    if jobs:
        args += [w_down]
    scratch = []
    for _, _, _, width, _ in segs:
        scratch += [pltpu.VMEM((rows, width), BF16), pltpu.VMEM((width, ff), BF16), pltpu.VMEM((width, ff), BF16)]
    if segs:
        scratch += [pltpu.VMEM((rows, ff), F32)] * 2
    if inv is not None:
        scratch += [pltpu.VMEM((rows, SIDE), BF16)]
    if jobs:
        scratch += [pltpu.VMEM((rows, ff), BF16)]
    for _, _, width, _ in jobs:
        scratch += [pltpu.VMEM((ff, width), BF16), pltpu.VMEM((rows, width), BF16)]
    n_sems = sum(len(s[0]) + 2 for s in segs) + 2 + 1 + 2 + sum(1 + len(j[3]) for j in jobs)
    scratch += [pltpu.SemaphoreType.DMA((n_sems,))]

    def body(where_ref, *refs):
        refs = list(refs)
        take = lambda n: [refs.pop(0) for _ in range(n)]
        x_refs = take(len(xs))
        wg, wu = take(2) if segs else (None, None)
        carried = take(2) if carry is not None else None
        inv_ref = take(1)[0] if inv is not None else None
        hidden_ref = take(1)[0] if hidden is not None else None
        wd = take(1)[0] if jobs else None
        out_refs = take(len(out_shapes))
        seg_bufs = [take(3) for _ in segs]
        accs = take(2) if segs else None
        inv_buf = take(1)[0] if inv is not None else None
        h_buf = take(1)[0] if jobs else None
        job_bufs = [take(2) for _ in jobs]
        copies = Copies(refs.pop(0))
        z = where_ref[0]

        def first(step, offset):
            return pl.multiple_of(lax.rem(z + step, slices) * span + offset, 128)

        waits_in = []
        if carried is not None:
            waits_in = [copies.start(c, a) for c, a in zip(carried, accs)]
        seg_waits = []
        for (parts, step, offset, width, col), (xb, gb, ub) in zip(segs, seg_bufs):
            at = pl.ds(first(step, offset), width)
            mine = []
            for index, row in parts:
                count = x_refs[index].shape[0]
                mine.append(copies.start(x_refs[index].at[:, pl.ds(col, width)], xb.at[pl.ds(row, count), :]))
            mine.append(copies.start(wg.at[at, :], gb))
            mine.append(copies.start(wu.at[at, :], ub))
            seg_waits.append(mine)
        if inv is not None:
            inv_wait = copies.start(inv_ref.at[:, pl.ds(inv_ref.shape[1] - SIDE, SIDE)], inv_buf)
        if hidden is not None:
            hidden_wait = copies.start(hidden_ref, h_buf)
        job_waits = []
        for (step, offset, width, _), (wb, _) in zip(jobs, job_bufs):
            job_waits.append(copies.start(wd.at[:, pl.ds(first(step, offset), width)], wb))
        done = []
        for w in waits_in:
            w.wait()
        for k, (xb, gb, ub) in enumerate(seg_bufs):
            for w in seg_waits[k]:
                w.wait()
            for w_buf, acc in ((gb, accs[0]), (ub, accs[1])):
                term = jnp.dot(xb[...], w_buf[...], preferred_element_type=F32)
                if k == 0 and carried is None:
                    acc[...] = term
                else:
                    acc[...] += term
        if segs and not jobs:
            done += [copies.start(a, o) for a, o in zip(accs, out_refs)]
        if finish:
            inv_wait.wait()
            scale = jnp.sum(inv_buf[...].astype(F32), axis=1, keepdims=True)
            gate = accs[0][...] * scale
            h_buf[...] = (jax.nn.silu(gate) * (accs[1][...] * scale)).astype(BF16)
            done.append(copies.start(h_buf, out_refs.pop(0)))
        if hidden is not None:
            hidden_wait.wait()
        for (_, _, width, targets), (wb, ob), w in zip(jobs, job_bufs, job_waits):
            w.wait()
            ob[...] = jnp.dot(h_buf[...], wb[...], preferred_element_type=F32).astype(BF16)
            for index, row, count, col in targets:
                done.append(copies.start(ob.at[pl.ds(row, count), :], out_refs[index].at[:, pl.ds(col, width)]))
        for copy in done:
            copy.wait()

    hbm = pl.BlockSpec(memory_space=pltpu.HBM)
    flops = sum(4 * rows * s[3] * ff for s in segs) + sum(2 * rows * ff * j[2] for j in jobs)
    return pl.pallas_call(
        body,
        in_specs=[pl.BlockSpec(memory_space=pltpu.SMEM)] + [hbm] * len(args),
        out_specs=[hbm] * len(out_shapes),
        out_shape=out_shapes,
        scratch_shapes=scratch,
        cost_estimate=pl.CostEstimate(flops=flops, bytes_accessed=flops // 256, transcendentals=0),
    )(where, *args)


def place_picks(expert_ids, gate_prob, window):
    ids = expert_ids.T
    probs = gate_prob.T.astype(F32)
    tok = ids.shape[1]
    same = ids[:, None, :] == jnp.arange(window, dtype=jnp.int32)[None, :, None]
    match = jnp.any(same, axis=0).astype(BF16)
    prob = jnp.sum(jnp.where(same, probs[:, None, :], 0.0), axis=0)
    earlier = (jnp.arange(tok)[:, None] < jnp.arange(tok)[None, :]).astype(BF16)
    before = jnp.dot(match, earlier, preferred_element_type=F32)
    slot = jnp.where(match > 0, before, -1.0)
    hit = slot[:, None, :] == jnp.arange(CAP, dtype=F32)[None, :, None]
    pick = hit.astype(BF16).reshape(window * CAP, tok)
    weight = jnp.where(hit, prob[:, None, :], 0.0).astype(BF16).reshape(window * CAP, tok)
    return pick, weight


def three_terms(value):
    rest, terms = value, []
    for _ in range(3):
        term = lax.reduce_precision(rest, 8, 7)
        terms.append(term)
        rest = rest - term
    stacked = jnp.stack(terms, axis=1)
    return jnp.pad(stacked, ((0, 0), (0, SIDE - 3))).astype(BF16)


def local(tokens, norm_gain, expert_ids, gate_prob, w_gate, w_up, w_down):
    window, n_tp = lax.axis_size("ep"), lax.axis_size("tp")
    where = lax.axis_index("tp").astype(jnp.int32).reshape(1)
    w_gate, w_up, w_down = w_gate[0], w_up[0], w_down[0]
    tok = tokens.shape[0]
    rows = window * CAP
    up = [(i, (i + 1) % n_tp) for i in range(n_tp)]
    dn = [(i, (i - 1) % n_tp) for i in range(n_tp)]

    def spread(x):
        half = x.shape[0] // 2
        below, above = lax.ppermute(x, "tp", up), lax.ppermute(x, "tp", dn)
        return below, above, lax.ppermute(below[:half], "tp", up), lax.ppermute(above[half:], "tp", dn)

    def fold(own, above, below, far_a, far_b):
        half = own.shape[0] // 2
        got_a, got_b = lax.ppermute(far_a, "tp", up), lax.ppermute(far_b, "tp", dn)
        sum_up = (above.astype(F32) + jnp.pad(got_a.astype(F32), ((0, half), (0, 0)))).astype(BF16)
        sum_dn = (below.astype(F32) + jnp.pad(got_b.astype(F32), ((half, 0), (0, 0)))).astype(BF16)
        from_dn, from_up = lax.ppermute(sum_up, "tp", up), lax.ppermute(sum_dn, "tp", dn)
        return (own.astype(F32) + from_dn.astype(F32) + from_up.astype(F32)).astype(BF16)

    def exchange(x):
        shaped = x.reshape(window, CAP, x.shape[1])
        return lax.all_to_all(shaped, "ep", 0, 0, tiled=True).reshape(rows, x.shape[1])

    pick, weight = place_picks(expert_ids, gate_prob, window)
    gained = (tokens.astype(F32) * norm_gain.astype(F32)).astype(BF16)
    bulk = tokens.shape[1] - EARLY
    half = rows // 2

    def dispatch(x):
        return jnp.dot(pick, x, preferred_element_type=F32).astype(BF16)

    square_part = jnp.sum(jnp.square(tokens.astype(F32)), axis=1)
    early = jnp.concatenate([gained[:, :EARLY], three_terms(square_part)], axis=1)
    e_below, e_above, e_far_a, e_far_b = spread(early)
    mine = exchange(dispatch(gained[:, EARLY:]))
    e_far = jnp.concatenate([e_far_a, e_far_b], axis=0)
    all_early = (early, e_above, e_far, e_below)
    squares = sum(jnp.sum(e[:, EARLY : EARLY + 3].astype(F32), axis=1) for e in all_early[1:]) + square_part
    inverse_rms = lax.rsqrt(squares / D + epsilon)
    early_all = jnp.concatenate([e[:, :EARLY] for e in all_early] + [three_terms(inverse_rms)], axis=1)
    early_rows = exchange(dispatch(early_all))
    below, above, far_a, far_b = spread(mine)

    whole = lambda i: ((i, 0),)
    near_sums = expert_call(
        where, (mine, above, below),
        [(whole(i), step, EARLY, bulk, 0) for i, step in enumerate((0, 1, 3))],
        w_gate, w_up, None, None, None, None, [], [],
    )
    sums = expert_call(
        where, (early_rows,),
        [(whole(0), k, 0, EARLY, k * EARLY) for k in range(n_tp)],
        w_gate, w_up, near_sums, None, None, None, [], [],
    )
    hidden, p_far_a, p_far_b = expert_call(
        where, (far_a, far_b),
        [(((0, 0), (1, half)), 2, EARLY, bulk, 0)],
        w_gate, w_up, sums, early_rows, None, w_down,
        [(2, EARLY, bulk, ((0, 0, half, 0), (1, half, half, 0)))], [(half, bulk)] * 2,
    )
    (p_early,) = expert_call(
        where, (), [], None, None, None, None, hidden, w_down,
        [(k, 0, EARLY, ((0, 0, rows, k * EARLY),)) for k in range(n_tp)], [(rows, n_tp * EARLY)],
    )
    p_above, p_below, p_own = expert_call(
        where, (), [], None, None, None, None, hidden, w_down,
        [(step, EARLY, bulk, ((i, 0, rows, 0),)) for i, step in enumerate((1, 3, 0))], [(rows, bulk)] * 3,
    )

    def combine(back):
        return lax.dot_general(weight, back, (((0,), (0,)), ((), ())), preferred_element_type=F32).astype(BF16)

    early_back = combine(exchange(p_early))
    e = [early_back[:, k * EARLY : (k + 1) * EARLY] for k in range(n_tp)]
    out_early = fold(e[0], e[1], e[3], e[2][: tok // 2], e[2][tok // 2 :])
    folded = fold(p_own, p_above, p_below, p_far_a, p_far_b)
    out_bulk = combine(exchange(folded))
    return jnp.concatenate([out_early, out_bulk], axis=1)


def solution(mesh):
    placed = (
        P("ep", "tp"),
        P("tp"),
        P("ep", None),
        P("ep", None),
        P("ep", None, "tp"),
        P("ep", None, "tp"),
        P("ep", "tp", None),
    )

    return jax.shard_map(local, mesh=mesh, in_specs=placed, out_specs=P("ep", "tp"), check_vma=False)
```

```python
import jax
import jax.numpy as jnp
from jax import lax
from jax.experimental import pallas as pl
from jax.experimental.pallas import tpu as pltpu
from jax.sharding import PartitionSpec as P


D = 7168
epsilon = 1e-06
CAP = 16
EARLY = 640
SIDE = 128
F32, BF16 = jnp.float32, jnp.bfloat16


class Copies:
    def __init__(self, sems):
        self.sems, self.used = sems, 0

    def start(self, src, dst):
        copy = pltpu.make_async_copy(src, dst, self.sems.at[self.used])
        self.used += 1
        copy.start()
        return copy


def expert_call(where, weights, xs=(), segs=(), carry=(), inv=None, hidden=None, jobs=(), outs=()):
    slices = lax.axis_size("tp")
    w_gate, w_up, w_down = weights
    d_all, ff = w_gate.shape
    span = d_all // slices
    finish = bool(segs) and bool(jobs)
    rows = hidden.shape[0] if hidden is not None else carry[0].shape[0] if carry else sum(xs[i].shape[0] for i in segs[0][0])
    results = [((rows, ff), F32)] * 2 if not jobs else [((rows, ff), BF16)] * finish + [(s, BF16) for s in outs]
    resident = list(xs) + list(carry) + ([] if inv is None else [inv]) + ([] if hidden is None else [hidden])
    streamed = ([w_gate, w_up] if segs else []) + ([w_down] if jobs else [])
    columns = []
    for step, offset, width, *_ in jobs:
        if (step, offset, width) not in columns:
            columns.append((step, offset, width))
    scratch = []
    for _, _, _, width, _ in segs:
        scratch += [pltpu.VMEM((width, ff), BF16)] * 2
    if finish:
        scratch += [pltpu.VMEM((rows, ff), F32)] * 2
    scratch += [pltpu.VMEM((ff, width), BF16) for _, _, width in columns]
    scratch += [pltpu.SemaphoreType.DMA((2 * len(segs) + len(columns),))]

    def body(where_ref, *refs):
        refs = list(refs)
        take = lambda n: [refs.pop(0) for _ in range(n)]
        x_refs, carried = take(len(xs)), take(len(carry))
        inv_ref = take(inv is not None)
        hidden_ref = take(hidden is not None)
        wg, wu = take(2) if segs else (None, None)
        wd = take(bool(jobs))
        out_refs = take(len(results))
        seg_bufs = [take(2) for _ in segs]
        accs = take(2) if finish else out_refs
        col_bufs = take(len(columns))
        copies = Copies(refs.pop(0))
        z = where_ref[0]

        def first(step, offset):
            return pl.multiple_of(lax.rem(z + step, slices) * span + offset, 128)

        seg_waits, col_waits = [], []
        for (_, step, offset, width, _), (gb, ub) in zip(segs, seg_bufs):
            at = pl.ds(first(step, offset), width)
            seg_waits.append([copies.start(wg.at[at, :], gb), copies.start(wu.at[at, :], ub)])
        for (step, offset, width), wb in zip(columns, col_bufs):
            col_waits.append(copies.start(wd[0].at[:, pl.ds(first(step, offset), width)], wb))
        for k, (index, _, _, width, col) in enumerate(segs):
            x = [x_refs[i][:, col : col + width] for i in index]
            x = x[0] if len(x) == 1 else jnp.concatenate(x, axis=0)
            for w in seg_waits[k]:
                w.wait()
            for w_buf, acc, base in zip(seg_bufs[k], accs, carried or (None, None)):
                term = jnp.dot(x, w_buf[...], preferred_element_type=F32)
                if k:
                    acc[...] += term
                elif base is None:
                    acc[...] = term
                else:
                    acc[...] = base[...] + term
        if finish:
            scale = jnp.sum(inv_ref[0][:, -SIDE:].astype(F32), axis=1, keepdims=True)
            gate = accs[0][...] * scale
            hidden_ref = [out_refs.pop(0)]
            hidden_ref[0][...] = (jax.nn.silu(gate) * (accs[1][...] * scale)).astype(BF16)
        waited = set()
        for step, offset, width, row, count, targets in jobs:
            k = columns.index((step, offset, width))
            if k not in waited:
                col_waits[k].wait()
                waited.add(k)
            term = jnp.dot(hidden_ref[0][row : row + count, :], col_bufs[k][...], preferred_element_type=F32).astype(BF16)
            for index, top, n, col in targets:
                out_refs[index][:, col : col + width] = term[top : top + n, :]

    vmem = pl.BlockSpec(memory_space=pltpu.VMEM)
    flops = sum(4 * rows * s[3] * ff for s in segs) + sum(2 * j[4] * ff * j[2] for j in jobs)
    return pl.pallas_call(
        body,
        in_specs=[pl.BlockSpec(memory_space=pltpu.SMEM)] + [vmem] * len(resident) + [pl.BlockSpec(memory_space=pltpu.HBM)] * len(streamed),
        out_specs=[vmem] * len(results),
        out_shape=[pltpu.VMEM(s, t) for s, t in results],
        scratch_shapes=scratch,
        cost_estimate=pl.CostEstimate(flops=flops, bytes_accessed=flops // 256, transcendentals=0),
        compiler_params=pltpu.CompilerParams(vmem_limit_bytes=24 * 2**20),
    )(where, *[pltpu.with_memory_space_constraint(x, pltpu.VMEM) for x in resident], *[pltpu.with_memory_space_constraint(w, pltpu.HBM) for w in streamed])


def place_picks(expert_ids, gate_prob, window):
    ids = expert_ids.T
    probs = gate_prob.T.astype(F32)
    tok = ids.shape[1]
    same = ids[:, None, :] == jnp.arange(window, dtype=jnp.int32)[None, :, None]
    match = jnp.any(same, axis=0).astype(BF16)
    prob = jnp.sum(jnp.where(same, probs[:, None, :], 0.0), axis=0)
    earlier = (jnp.arange(tok)[:, None] < jnp.arange(tok)[None, :]).astype(BF16)
    before = jnp.dot(match, earlier, preferred_element_type=F32)
    slot = jnp.where(match > 0, before, -1.0)
    hit = slot[:, None, :] == jnp.arange(CAP, dtype=F32)[None, :, None]
    pick = hit.astype(BF16).reshape(window * CAP, tok)
    weight = jnp.where(hit, prob[:, None, :], 0.0).astype(BF16).reshape(window * CAP, tok)
    return pick, weight


def three_terms(value):
    rest, terms = value, []
    for _ in range(3):
        term = lax.reduce_precision(rest, 8, 7)
        terms.append(term)
        rest = rest - term
    stacked = jnp.stack(terms, axis=1)
    return jnp.pad(stacked, ((0, 0), (0, SIDE - 3))).astype(BF16)


def local(tokens, norm_gain, expert_ids, gate_prob, w_gate, w_up, w_down):
    window, n_tp = lax.axis_size("ep"), lax.axis_size("tp")
    where = lax.axis_index("tp").astype(jnp.int32).reshape(1)
    w_gate, w_up, w_down = w_gate[0], w_up[0], w_down[0]
    tok = tokens.shape[0]
    rows = window * CAP
    up = [(i, (i + 1) % n_tp) for i in range(n_tp)]
    dn = [(i, (i - 1) % n_tp) for i in range(n_tp)]

    def spread(x):
        half = x.shape[0] // 2
        below, above = lax.ppermute(x, "tp", up), lax.ppermute(x, "tp", dn)
        return below, above, lax.ppermute(below[:half], "tp", up), lax.ppermute(above[half:], "tp", dn)

    def fold(own, above, below, far_a, far_b):
        half = own.shape[0] // 2
        got_a, got_b = lax.ppermute(far_a, "tp", up), lax.ppermute(far_b, "tp", dn)
        sum_up = (above.astype(F32) + jnp.pad(got_a.astype(F32), ((0, half), (0, 0)))).astype(BF16)
        sum_dn = (below.astype(F32) + jnp.pad(got_b.astype(F32), ((half, 0), (0, 0)))).astype(BF16)
        from_dn, from_up = lax.ppermute(sum_up, "tp", up), lax.ppermute(sum_dn, "tp", dn)
        return (own.astype(F32) + from_dn.astype(F32) + from_up.astype(F32)).astype(BF16)

    def spread_halves(low, high):
        below_low, above_high = lax.ppermute(low, "tp", up), lax.ppermute(high, "tp", dn)
        below_high, above_low = lax.ppermute(high, "tp", up), lax.ppermute(low, "tp", dn)
        far = lax.ppermute(below_low, "tp", up), lax.ppermute(above_high, "tp", dn)
        return (below_low, below_high), (above_low, above_high), far

    def add(*terms):
        return sum(t.astype(F32) for t in terms).astype(BF16)

    def fold_halves(own, above, below, far):
        got_low, got_high = lax.ppermute(far[0], "tp", up), lax.ppermute(far[1], "tp", dn)
        dn_high, up_low = lax.ppermute(above[1], "tp", up), lax.ppermute(below[0], "tp", dn)
        dn_low = lax.ppermute(add(above[0], got_low), "tp", up)
        up_high = lax.ppermute(add(below[1], got_high), "tp", dn)
        return jnp.concatenate([add(own[0], dn_low, up_low), add(own[1], dn_high, up_high)], axis=0)

    def exchange(x):
        shaped = x.reshape(window, CAP, x.shape[1])
        return lax.all_to_all(shaped, "ep", 0, 0, tiled=True).reshape(rows, x.shape[1])

    pick, weight = place_picks(expert_ids, gate_prob, window)
    gained = (tokens.astype(F32) * norm_gain.astype(F32)).astype(BF16)
    bulk = tokens.shape[1] - EARLY
    half = rows // 2

    def dispatch(x):
        return jnp.dot(pick, x, preferred_element_type=F32).astype(BF16)

    square_part = jnp.sum(jnp.square(tokens.astype(F32)), axis=1)
    early = jnp.concatenate([gained[:, :EARLY], three_terms(square_part)], axis=1)
    e_below, e_above, e_far_a, e_far_b = spread(early)
    mine = exchange(dispatch(gained[:, EARLY:]))
    e_far = jnp.concatenate([e_far_a, e_far_b], axis=0)
    all_early = (early, e_above, e_far, e_below)
    squares = sum(jnp.sum(e[:, EARLY : EARLY + 3].astype(F32), axis=1) for e in all_early[1:]) + square_part
    inverse_rms = lax.rsqrt(squares / D + epsilon)
    early_all = jnp.concatenate([e[:, :EARLY] for e in all_early] + [three_terms(inverse_rms)], axis=1)
    early_rows = exchange(dispatch(early_all))
    below, above, far = spread_halves(mine[:half], mine[half:])

    weights = (w_gate, w_up, w_down)
    sums = expert_call(where, weights, [mine], [((0,), 0, EARLY, bulk, 0)])
    sums = expert_call(
        where, weights, [*above, *below],
        [((0, 1), 1, EARLY, bulk, 0), ((2, 3), 3, EARLY, bulk, 0)], sums,
    )
    sums = expert_call(
        where, weights, [early_rows],
        [((0,), k, 0, EARLY, k * EARLY) for k in range(n_tp)], sums,
    )
    low, high = (0, half), (half, half)
    hidden, f_low, f_high, a_high, b_low = expert_call(
        where, weights, far, [((0, 1), 2, EARLY, bulk, 0)], sums, inv=early_rows[:, -SIDE:],
        jobs=[
            (2, EARLY, bulk, 0, rows, ((0, 0, half, 0), (1, half, half, 0))),
            (1, EARLY, bulk, *high, ((2, 0, half, 0),)),
            (3, EARLY, bulk, *low, ((3, 0, half, 0),)),
        ],
        outs=[(half, bulk)] * 4,
    )
    (p_early,) = expert_call(
        where, weights, hidden=hidden,
        jobs=[(k, 0, EARLY, 0, rows, ((0, 0, rows, k * EARLY),)) for k in range(n_tp)], outs=[(rows, n_tp * EARLY)],
    )
    a_low, b_high, o_low, o_high = expert_call(
        where, weights, hidden=hidden,
        jobs=[
            (1, EARLY, bulk, *low, ((0, 0, half, 0),)),
            (3, EARLY, bulk, *high, ((1, 0, half, 0),)),
            (0, EARLY, bulk, 0, rows, ((2, 0, half, 0), (3, half, half, 0))),
        ],
        outs=[(half, bulk)] * 4,
    )

    def combine(back):
        return lax.dot_general(weight, back, (((0,), (0,)), ((), ())), preferred_element_type=F32).astype(BF16)

    early_back = combine(exchange(p_early))
    e = [early_back[:, k * EARLY : (k + 1) * EARLY] for k in range(n_tp)]
    out_early = fold(e[0], e[1], e[3], e[2][: tok // 2], e[2][tok // 2 :])
    folded = fold_halves((o_low, o_high), (a_low, a_high), (b_low, b_high), (f_low, f_high))
    out_bulk = combine(exchange(folded))
    return jnp.concatenate([out_early, out_bulk], axis=1)


def solution(mesh):
    placed = (
        P("ep", "tp"),
        P("tp"),
        P("ep", None),
        P("ep", None),
        P("ep", None, "tp"),
        P("ep", None, "tp"),
        P("ep", "tp", None),
    )

    return jax.shard_map(local, mesh=mesh, in_specs=placed, out_specs=P("ep", "tp"), check_vma=False)
```

```python
import jax
import jax.numpy as jnp
from jax import lax
from jax.experimental import pallas as pl
from jax.experimental.pallas import tpu as pltpu
from jax.sharding import PartitionSpec as P


D = 7168
epsilon = 1e-06
CAP = 16
EARLY = 512
SIDE = 128
F32, BF16 = jnp.float32, jnp.bfloat16


class Copies:
    def __init__(self, sems):
        self.sems, self.used = sems, 0

    def start(self, src, dst):
        copy = pltpu.make_async_copy(src, dst, self.sems.at[self.used])
        self.used += 1
        copy.start()
        return copy


def expert_call(where, weights, xs=(), segs=(), carry=(), inv=None, hidden=None, jobs=(), outs=()):
    slices = lax.axis_size("tp")
    w_gate, w_up, w_down = weights
    d_all, ff = w_gate.shape
    span = d_all // slices
    finish = bool(segs) and bool(jobs)
    rows = hidden.shape[0] if hidden is not None else carry[0].shape[0] if carry else sum(xs[i].shape[0] for i in segs[0][0])
    results = [((rows, ff), F32)] * 2 if not jobs else [((rows, ff), BF16)] * finish + [(s, BF16) for s in outs]
    resident = list(xs) + list(carry) + ([] if inv is None else [inv]) + ([] if hidden is None else [hidden])
    streamed = ([w_gate, w_up] if segs else []) + ([w_down] if jobs else [])
    columns = []
    for step, offset, width, *_ in jobs:
        if (step, offset, width) not in columns:
            columns.append((step, offset, width))
    scratch = []
    for _, _, _, width, _ in segs:
        scratch += [pltpu.VMEM((width, ff), BF16)] * 2
    if finish:
        scratch += [pltpu.VMEM((rows, ff), F32)] * 2
    scratch += [pltpu.VMEM((ff, width), BF16) for _, _, width in columns]
    scratch += [pltpu.SemaphoreType.DMA((2 * len(segs) + len(columns),))]

    def body(where_ref, *refs):
        refs = list(refs)
        take = lambda n: [refs.pop(0) for _ in range(n)]
        x_refs, carried = take(len(xs)), take(len(carry))
        inv_ref = take(inv is not None)
        hidden_ref = take(hidden is not None)
        wg, wu = take(2) if segs else (None, None)
        wd = take(bool(jobs))
        out_refs = take(len(results))
        seg_bufs = [take(2) for _ in segs]
        accs = take(2) if finish else out_refs
        col_bufs = take(len(columns))
        copies = Copies(refs.pop(0))
        z = where_ref[0]

        def first(step, offset):
            return pl.multiple_of(lax.rem(z + step, slices) * span + offset, 128)

        seg_waits, col_waits = [], []
        for (_, step, offset, width, _), (gb, ub) in zip(segs, seg_bufs):
            at = pl.ds(first(step, offset), width)
            seg_waits.append([copies.start(wg.at[at, :], gb), copies.start(wu.at[at, :], ub)])
        for (step, offset, width), wb in zip(columns, col_bufs):
            col_waits.append(copies.start(wd[0].at[:, pl.ds(first(step, offset), width)], wb))
        for k, (index, _, _, width, col) in enumerate(segs):
            x = [x_refs[i][:, col : col + width] for i in index]
            x = x[0] if len(x) == 1 else jnp.concatenate(x, axis=0)
            for w in seg_waits[k]:
                w.wait()
            for w_buf, acc, base in zip(seg_bufs[k], accs, carried or (None, None)):
                term = jnp.dot(x, w_buf[...], preferred_element_type=F32)
                if k:
                    acc[...] += term
                elif base is None:
                    acc[...] = term
                else:
                    acc[...] = base[...] + term
        if finish:
            scale = jnp.sum(inv_ref[0][:, -SIDE:].astype(F32), axis=1, keepdims=True)
            gate = accs[0][...] * scale
            hidden_ref = [out_refs.pop(0)]
            hidden_ref[0][...] = (jax.nn.silu(gate) * (accs[1][...] * scale)).astype(BF16)
        waited = set()
        for step, offset, width, row, count, targets in jobs:
            k = columns.index((step, offset, width))
            if k not in waited:
                col_waits[k].wait()
                waited.add(k)
            term = jnp.dot(hidden_ref[0][row : row + count, :], col_bufs[k][...], preferred_element_type=F32).astype(BF16)
            for index, top, n, col in targets:
                out_refs[index][:, col : col + width] = term[top : top + n, :]

    vmem = pl.BlockSpec(memory_space=pltpu.VMEM)
    flops = sum(4 * rows * s[3] * ff for s in segs) + sum(2 * j[4] * ff * j[2] for j in jobs)
    return pl.pallas_call(
        body,
        in_specs=[pl.BlockSpec(memory_space=pltpu.SMEM)] + [vmem] * len(resident) + [pl.BlockSpec(memory_space=pltpu.HBM)] * len(streamed),
        out_specs=[vmem] * len(results),
        out_shape=[pltpu.VMEM(s, t) for s, t in results],
        scratch_shapes=scratch,
        cost_estimate=pl.CostEstimate(flops=flops, bytes_accessed=flops // 256, transcendentals=0),
        compiler_params=pltpu.CompilerParams(vmem_limit_bytes=24 * 2**20),
    )(where, *[pltpu.with_memory_space_constraint(x, pltpu.VMEM) for x in resident], *[pltpu.with_memory_space_constraint(w, pltpu.HBM) for w in streamed])


def join_sums(low, high):
    half, width = low[0].shape

    def body(*refs):
        out = refs[-1]
        for k in (0, 1):
            a, b, c = (r[...].astype(F32) for r in refs[3 * k : 3 * k + 3])
            out[k * half : (k + 1) * half, :] = (a + b + c).astype(BF16)

    return pl.pallas_call(
        body,
        out_shape=jax.ShapeDtypeStruct((2 * half, width), BF16),
        cost_estimate=pl.CostEstimate(flops=6 * half * width, bytes_accessed=16 * half * width, transcendentals=0),
        compiler_params=pltpu.CompilerParams(vmem_limit_bytes=16 * 2**20),
        name="join_sums",
    )(*low, *high)


def place_picks(expert_ids, gate_prob, window):
    ids = expert_ids.T
    probs = gate_prob.T.astype(F32)
    tok = ids.shape[1]
    same = ids[:, None, :] == jnp.arange(window, dtype=jnp.int32)[None, :, None]
    match = jnp.any(same, axis=0).astype(BF16)
    prob = jnp.sum(jnp.where(same, probs[:, None, :], 0.0), axis=0)
    earlier = (jnp.arange(tok)[:, None] < jnp.arange(tok)[None, :]).astype(BF16)
    before = jnp.dot(match, earlier, preferred_element_type=F32)
    slot = jnp.where(match > 0, before, -1.0)
    hit = slot[:, None, :] == jnp.arange(CAP, dtype=F32)[None, :, None]
    pick = hit.astype(BF16).reshape(window * CAP, tok)
    weight = jnp.where(hit, prob[:, None, :], 0.0).astype(BF16).reshape(window * CAP, tok)
    return pick, weight


def three_terms(value):
    rest, terms = value, []
    for _ in range(3):
        term = lax.reduce_precision(rest, 8, 7)
        terms.append(term)
        rest = rest - term
    stacked = jnp.stack(terms, axis=1)
    return jnp.pad(stacked, ((0, 0), (0, SIDE - 3))).astype(BF16)


def local(tokens, norm_gain, expert_ids, gate_prob, w_gate, w_up, w_down):
    window, n_tp = lax.axis_size("ep"), lax.axis_size("tp")
    where = lax.axis_index("tp").astype(jnp.int32).reshape(1)
    w_gate, w_up, w_down = w_gate[0], w_up[0], w_down[0]
    tok = tokens.shape[0]
    rows = window * CAP
    up = [(i, (i + 1) % n_tp) for i in range(n_tp)]
    dn = [(i, (i - 1) % n_tp) for i in range(n_tp)]

    def spread(x):
        half = x.shape[0] // 2
        below, above = lax.ppermute(x, "tp", up), lax.ppermute(x, "tp", dn)
        return below, above, lax.ppermute(below[:half], "tp", up), lax.ppermute(above[half:], "tp", dn)

    def fold(own, above, below, far_a, far_b):
        half = own.shape[0] // 2
        got_a, got_b = lax.ppermute(far_a, "tp", up), lax.ppermute(far_b, "tp", dn)
        sum_up = (above.astype(F32) + jnp.pad(got_a.astype(F32), ((0, half), (0, 0)))).astype(BF16)
        sum_dn = (below.astype(F32) + jnp.pad(got_b.astype(F32), ((half, 0), (0, 0)))).astype(BF16)
        from_dn, from_up = lax.ppermute(sum_up, "tp", up), lax.ppermute(sum_dn, "tp", dn)
        return (own.astype(F32) + from_dn.astype(F32) + from_up.astype(F32)).astype(BF16)

    def spread_halves(low, high):
        below_low, above_high = lax.ppermute(low, "tp", up), lax.ppermute(high, "tp", dn)
        below_high, above_low = lax.ppermute(high, "tp", up), lax.ppermute(low, "tp", dn)
        far = lax.ppermute(below_low, "tp", up), lax.ppermute(above_high, "tp", dn)
        return (below_low, below_high), (above_low, above_high), far

    def add(*terms):
        return sum(t.astype(F32) for t in terms).astype(BF16)

    def fold_halves(own, above, below, far):
        got_low, got_high = lax.ppermute(far[0], "tp", up), lax.ppermute(far[1], "tp", dn)
        dn_high, up_low = lax.ppermute(above[1], "tp", up), lax.ppermute(below[0], "tp", dn)
        dn_low = lax.ppermute(add(above[0], got_low), "tp", up)
        up_high = lax.ppermute(add(below[1], got_high), "tp", dn)
        return join_sums((own[0], dn_low, up_low), (own[1], dn_high, up_high))

    def exchange(x):
        shaped = x.reshape(window, CAP, x.shape[1])
        return lax.all_to_all(shaped, "ep", 0, 0, tiled=True).reshape(rows, x.shape[1])

    pick, weight = place_picks(expert_ids, gate_prob, window)
    gained = (tokens.astype(F32) * norm_gain.astype(F32)).astype(BF16)
    bulk = tokens.shape[1] - EARLY
    half = rows // 2

    def dispatch(x):
        return jnp.dot(pick, x, preferred_element_type=F32).astype(BF16)

    square_part = jnp.sum(jnp.square(tokens.astype(F32)), axis=1)
    early = jnp.concatenate([gained[:, :EARLY], three_terms(square_part)], axis=1)
    e_below, e_above, e_far_a, e_far_b = spread(early)
    mine = exchange(dispatch(gained[:, EARLY:]))
    e_far = jnp.concatenate([e_far_a, e_far_b], axis=0)
    all_early = (early, e_above, e_far, e_below)
    squares = sum(jnp.sum(e[:, EARLY : EARLY + 3].astype(F32), axis=1) for e in all_early[1:]) + square_part
    inverse_rms = lax.rsqrt(squares / D + epsilon)
    early_all = jnp.concatenate([e[:, :EARLY] for e in all_early] + [three_terms(inverse_rms)], axis=1)
    picked = dispatch(early_all)
    early_rows = exchange(picked)
    below, above, far = spread_halves(mine[:half], mine[half:])

    weights = (w_gate, w_up, w_down)
    sums = expert_call(where, weights, [mine], [((0,), 0, EARLY, bulk, 0)])
    sums = expert_call(
        where, weights, [*above, *below],
        [((0, 1), 1, EARLY, bulk, 0), ((2, 3), 3, EARLY, bulk, 0)], sums,
    )
    sums = expert_call(
        where, weights, [early_rows],
        [((0,), k, 0, EARLY, k * EARLY) for k in range(n_tp)], sums,
    )
    low, high = (0, half), (half, half)
    hidden, f_low, f_high, a_high, b_low = expert_call(
        where, weights, far, [((0, 1), 2, EARLY, bulk, 0)], sums, inv=early_rows[:, -SIDE:],
        jobs=[
            (2, EARLY, bulk, 0, rows, ((0, 0, half, 0), (1, half, half, 0))),
            (1, EARLY, bulk, *high, ((2, 0, half, 0),)),
            (3, EARLY, bulk, *low, ((3, 0, half, 0),)),
        ],
        outs=[(half, bulk)] * 4,
    )
    (p_early,) = expert_call(
        where, weights, hidden=hidden,
        jobs=[(k, 0, EARLY, 0, rows, ((0, 0, rows, k * EARLY),)) for k in range(n_tp)], outs=[(rows, n_tp * EARLY)],
    )
    a_low, b_high, o_low, o_high = expert_call(
        where, weights, hidden=hidden,
        jobs=[
            (1, EARLY, bulk, *low, ((0, 0, half, 0),)),
            (3, EARLY, bulk, *high, ((1, 0, half, 0),)),
            (0, EARLY, bulk, 0, rows, ((2, 0, half, 0), (3, half, half, 0))),
        ],
        outs=[(half, bulk)] * 4,
    )

    def combine(back):
        return lax.dot_general(weight, back, (((0,), (0,)), ((), ())), preferred_element_type=F32).astype(BF16)

    early_back = combine(exchange(p_early))
    e = [early_back[:, k * EARLY : (k + 1) * EARLY] for k in range(n_tp)]
    out_early = fold(e[0], e[1], e[3], e[2][: tok // 2], e[2][tok // 2 :])
    folded = fold_halves((o_low, o_high), (a_low, a_high), (b_low, b_high), (f_low, f_high))
    out_bulk = combine(exchange(folded))
    return jnp.concatenate([out_early, out_bulk], axis=1)


def solution(mesh):
    placed = (
        P("ep", "tp"),
        P("tp"),
        P("ep", None),
        P("ep", None),
        P("ep", None, "tp"),
        P("ep", None, "tp"),
        P("ep", "tp", None),
    )

    return jax.shard_map(local, mesh=mesh, in_specs=placed, out_specs=P("ep", "tp"), check_vma=False)
```

```python
import jax
import jax.numpy as jnp
from jax import lax
from jax.experimental import pallas as pl
from jax.experimental.pallas import tpu as pltpu
from jax.sharding import PartitionSpec as P


D = 7168
epsilon = 1e-06
CAP = 16
EARLY = 512
SIDE = 128
F32, BF16 = jnp.float32, jnp.bfloat16


class Copies:
    def __init__(self, sems):
        self.sems, self.used = sems, 0

    def start(self, src, dst):
        copy = pltpu.make_async_copy(src, dst, self.sems.at[self.used])
        self.used += 1
        copy.start()
        return copy


def expert_call(where, weights, xs=(), segs=(), carry=(), inv=None, hidden=None, jobs=(), outs=()):
    slices = lax.axis_size("tp")
    w_gate, w_up, w_down = weights
    d_all, ff = w_gate.shape
    span = d_all // slices
    finish = bool(segs) and bool(jobs)
    rows = hidden.shape[0] if hidden is not None else sum(xs[i].shape[0] for i in segs[0][0])
    results = [((rows, ff), F32)] * 2 if not jobs else [((rows, ff), BF16)] * finish + [(s, BF16) for s in outs]
    resident = [] if hidden is None else [hidden]
    streamed = list(xs) + list(carry) + ([w_gate, w_up] if segs else []) + ([w_down] if jobs else [])
    columns = []
    for step, offset, width, *_ in jobs:
        if (step, offset, width) not in columns:
            columns.append((step, offset, width))
    scratch = []
    for _, _, _, width, _ in segs:
        scratch += [pltpu.VMEM((rows, width), BF16)] + [pltpu.VMEM((width, ff), BF16)] * 2
    scratch += [pltpu.VMEM((rows, ff), F32)] * len(carry)
    if finish:
        scratch += [pltpu.VMEM((rows, ff), F32)] * 2
    if inv is not None:
        scratch += [pltpu.VMEM((rows, SIDE), BF16)]
    scratch += [pltpu.VMEM((ff, width), BF16) for _, _, width in columns]
    n_sems = sum(len(s[0]) + 2 for s in segs) + len(carry) + (inv is not None) + len(columns)
    scratch += [pltpu.SemaphoreType.DMA((n_sems,))]

    def body(where_ref, *refs):
        refs = list(refs)
        take = lambda n: [refs.pop(0) for _ in range(n)]
        hidden_ref = take(hidden is not None)
        x_refs, carried = take(len(xs)), take(len(carry))
        wg, wu = take(2) if segs else (None, None)
        wd = take(bool(jobs))
        out_refs = take(len(results))
        seg_bufs = [take(3) for _ in segs]
        carry_bufs = take(len(carry))
        accs = take(2) if finish else out_refs
        inv_buf = take(inv is not None)
        col_bufs = take(len(columns))
        copies = Copies(refs.pop(0))
        z = where_ref[0]

        def first(step, offset):
            return pl.multiple_of(lax.rem(z + step, slices) * span + offset, 128)

        seg_waits, col_waits = [], []
        for (index, step, offset, width, col), (xb, gb, ub) in zip(segs, seg_bufs):
            at = pl.ds(first(step, offset), width)
            waits, row = [], 0
            for i in index:
                count = x_refs[i].shape[0]
                waits.append(copies.start(x_refs[i].at[:, pl.ds(col, width)], xb.at[pl.ds(row, count), :]))
                row += count
            seg_waits.append(waits + [copies.start(wg.at[at, :], gb), copies.start(wu.at[at, :], ub)])
        carry_waits = [copies.start(c, b) for c, b in zip(carried, carry_bufs)]
        if inv is not None:
            inv_wait = copies.start(x_refs[inv[0]].at[:, pl.ds(inv[1], SIDE)], inv_buf[0])
        for (step, offset, width), wb in zip(columns, col_bufs):
            col_waits.append(copies.start(wd[0].at[:, pl.ds(first(step, offset), width)], wb))
        for k, (xb, *w_bufs) in enumerate(seg_bufs):
            for w in seg_waits[k]:
                w.wait()
            for n, (w_buf, acc) in enumerate(zip(w_bufs, accs)):
                term = jnp.dot(xb[...], w_buf[...], preferred_element_type=F32)
                if k:
                    term = acc[...] + term
                if carry and k == len(segs) - 1:
                    carry_waits[n].wait()
                    term = term + carry_bufs[n][...]
                acc[...] = term
        if finish:
            inv_wait.wait()
            scale = jnp.sum(inv_buf[0][...].astype(F32), axis=1, keepdims=True)
            gate = accs[0][...] * scale
            hidden_ref = [out_refs.pop(0)]
            hidden_ref[0][...] = (jax.nn.silu(gate) * (accs[1][...] * scale)).astype(BF16)
        waited = set()
        for step, offset, width, row, count, targets in jobs:
            k = columns.index((step, offset, width))
            if k not in waited:
                col_waits[k].wait()
                waited.add(k)
            term = jnp.dot(hidden_ref[0][row : row + count, :], col_bufs[k][...], preferred_element_type=F32).astype(BF16)
            for index, top, n, col in targets:
                out_refs[index][:, col : col + width] = term[top : top + n, :]

    vmem, hbm = pl.BlockSpec(memory_space=pltpu.VMEM), pl.BlockSpec(memory_space=pltpu.HBM)
    flops = sum(4 * rows * s[3] * ff for s in segs) + sum(2 * j[4] * ff * j[2] for j in jobs)
    return pl.pallas_call(
        body,
        in_specs=[pl.BlockSpec(memory_space=pltpu.SMEM)] + [vmem] * len(resident) + [hbm] * len(streamed),
        out_specs=[vmem] * len(results),
        out_shape=[pltpu.VMEM(s, t) if jobs else jax.ShapeDtypeStruct(s, t) for s, t in results],
        scratch_shapes=scratch,
        cost_estimate=pl.CostEstimate(flops=flops, bytes_accessed=flops // 256, transcendentals=0),
        compiler_params=pltpu.CompilerParams(vmem_limit_bytes=28 * 2**20),
    )(
        where,
        *[pltpu.with_memory_space_constraint(x, pltpu.VMEM) for x in resident],
        *[pltpu.with_memory_space_constraint(x, pltpu.HBM) for x in streamed],
    )


def side_columns(value):
    lane = lax.broadcasted_iota(jnp.int32, (value.shape[0], SIDE), 1)
    out = jnp.zeros((value.shape[0], SIDE), F32)
    for k in range(3):
        term = value.astype(BF16).astype(F32)
        out = jnp.where(lane == k, term, out)
        value = value - term
    return out.astype(BF16)


def head(tokens, norm_gain, ids, window):
    tok, width = tokens.shape
    rows, bulk = window * CAP, width - EARLY

    def body(tokens_ref, gain_ref, ids_ref, pick_ref, bulk_ref, early_ref):
        expert = lax.broadcasted_iota(jnp.int32, (window, tok), 0)
        match = jnp.zeros((window, tok), F32)
        for k in range(ids.shape[0]):
            match = match + jnp.where(ids_ref[k : k + 1, :] == expert, 1.0, 0.0)
        earlier = lax.broadcasted_iota(jnp.int32, (tok, tok), 0) < lax.broadcasted_iota(jnp.int32, (tok, tok), 1)
        earlier = jnp.where(earlier, 1.0, 0.0).astype(BF16)
        before = jnp.dot(match.astype(BF16), earlier, preferred_element_type=F32)
        slot = jnp.where(match > 0.0, before, -1.0)
        row = lax.broadcasted_iota(jnp.int32, (rows, window), 0)
        own = (row // CAP) == lax.broadcasted_iota(jnp.int32, (rows, window), 1)
        spread = jnp.dot(jnp.where(own, 1.0, 0.0).astype(BF16), slot.astype(BF16), preferred_element_type=F32)
        wanted = (lax.broadcasted_iota(jnp.int32, (rows, tok), 0) % CAP).astype(F32)
        pick = jnp.where(spread == wanted, 1.0, 0.0).astype(BF16)
        pick_ref[...] = pick
        values = tokens_ref[...].astype(F32)
        gained = (values * gain_ref[...].astype(F32)).astype(BF16)
        bulk_ref[...] = jnp.dot(pick, gained[:, EARLY:], preferred_element_type=F32).astype(BF16)
        early_ref[:, :EARLY] = gained[:, :EARLY]
        early_ref[:, EARLY:] = side_columns(jnp.sum(values * values, axis=1, keepdims=True))

    return pl.pallas_call(
        body,
        out_shape=[jax.ShapeDtypeStruct(s, BF16) for s in ((rows, tok), (rows, bulk), (tok, EARLY + SIDE))],
        cost_estimate=pl.CostEstimate(flops=2 * rows * tok * bulk, bytes_accessed=2 * tok * width, transcendentals=0),
        compiler_params=pltpu.CompilerParams(vmem_limit_bytes=24 * 2**20),
        name="head",
    )(tokens, norm_gain.reshape(1, width), ids)


def join_sums(low, high):
    half, width = low[0].shape

    def body(*refs):
        out = refs[-1]
        for k in (0, 1):
            a, b, c = (r[...].astype(F32) for r in refs[3 * k : 3 * k + 3])
            out[k * half : (k + 1) * half, :] = (a + b + c).astype(BF16)

    return pl.pallas_call(
        body,
        out_shape=jax.ShapeDtypeStruct((2 * half, width), BF16),
        cost_estimate=pl.CostEstimate(flops=6 * half * width, bytes_accessed=16 * half * width, transcendentals=0),
        compiler_params=pltpu.CompilerParams(vmem_limit_bytes=16 * 2**20),
        name="join_sums",
    )(*low, *high)


def three_terms(value):
    rest, terms = value, []
    for _ in range(3):
        term = lax.reduce_precision(rest, 8, 7)
        terms.append(term)
        rest = rest - term
    stacked = jnp.stack(terms, axis=1)
    return jnp.pad(stacked, ((0, 0), (0, SIDE - 3))).astype(BF16)


def local(tokens, norm_gain, expert_ids, gate_prob, w_gate, w_up, w_down):
    window, n_tp = lax.axis_size("ep"), lax.axis_size("tp")
    where = lax.axis_index("tp").astype(jnp.int32).reshape(1)
    w_gate, w_up, w_down = w_gate[0], w_up[0], w_down[0]
    tok = tokens.shape[0]
    rows = window * CAP
    up = [(i, (i + 1) % n_tp) for i in range(n_tp)]
    dn = [(i, (i - 1) % n_tp) for i in range(n_tp)]

    def spread(x):
        half = x.shape[0] // 2
        below, above = lax.ppermute(x, "tp", up), lax.ppermute(x, "tp", dn)
        return below, above, lax.ppermute(below[:half], "tp", up), lax.ppermute(above[half:], "tp", dn)

    def fold(own, above, below, far_a, far_b):
        half = own.shape[0] // 2
        got_a, got_b = lax.ppermute(far_a, "tp", up), lax.ppermute(far_b, "tp", dn)
        sum_up = (above.astype(F32) + jnp.pad(got_a.astype(F32), ((0, half), (0, 0)))).astype(BF16)
        sum_dn = (below.astype(F32) + jnp.pad(got_b.astype(F32), ((half, 0), (0, 0)))).astype(BF16)
        from_dn, from_up = lax.ppermute(sum_up, "tp", up), lax.ppermute(sum_dn, "tp", dn)
        return (own.astype(F32) + from_dn.astype(F32) + from_up.astype(F32)).astype(BF16)

    def spread_halves(low, high):
        below_low, above_high = lax.ppermute(low, "tp", up), lax.ppermute(high, "tp", dn)
        below_high, above_low = lax.ppermute(high, "tp", up), lax.ppermute(low, "tp", dn)
        far = lax.ppermute(below_low, "tp", up), lax.ppermute(above_high, "tp", dn)
        return (below_low, below_high), (above_low, above_high), far

    def add(*terms):
        return sum(t.astype(F32) for t in terms).astype(BF16)

    def fold_halves(own, above, below, far):
        got_low, got_high = lax.ppermute(far[0], "tp", up), lax.ppermute(far[1], "tp", dn)
        dn_high, up_low = lax.ppermute(above[1], "tp", up), lax.ppermute(below[0], "tp", dn)
        dn_low = lax.ppermute(add(above[0], got_low), "tp", up)
        up_high = lax.ppermute(add(below[1], got_high), "tp", dn)
        return join_sums((own[0], dn_low, up_low), (own[1], dn_high, up_high))

    def exchange(x):
        shaped = x.reshape(window, CAP, x.shape[1])
        return lax.all_to_all(shaped, "ep", 0, 0, tiled=True).reshape(rows, x.shape[1])

    bulk = tokens.shape[1] - EARLY
    half = rows // 2
    ids, probs = expert_ids.T, gate_prob.T.astype(F32)
    pick, picked_bulk, early = head(tokens, norm_gain, ids, window)
    same = ids[:, None, :] == jnp.arange(window, dtype=jnp.int32)[None, :, None]
    prob = jnp.sum(jnp.where(same, probs[:, None, :], 0.0), axis=0)
    by_slot = jnp.broadcast_to(prob[:, None, :], (window, CAP, tok)).reshape(rows, tok)
    weight = jnp.where(pick > 0, by_slot, 0.0).astype(BF16)

    def dispatch(x):
        return jnp.dot(pick, x, preferred_element_type=F32).astype(BF16)

    e_below, e_above, e_far_a, e_far_b = spread(early)
    mine = exchange(picked_bulk)
    e_far = jnp.concatenate([e_far_a, e_far_b], axis=0)
    all_early = (early, e_above, e_far, e_below)
    squares = sum(jnp.sum(e[:, EARLY : EARLY + 3].astype(F32), axis=1) for e in all_early)
    inverse_rms = lax.rsqrt(squares / D + epsilon)
    early_all = jnp.concatenate([e[:, :EARLY] for e in all_early] + [three_terms(inverse_rms)], axis=1)
    picked = dispatch(early_all)
    early_rows = exchange(picked)
    below, above, far = spread_halves(mine[:half], mine[half:])

    weights = (w_gate, w_up, w_down)
    sums = expert_call(where, weights, [mine], [((0,), 0, EARLY, bulk, 0)])
    sums = expert_call(
        where, weights, [*above, *below],
        [((0, 1), 1, EARLY, bulk, 0), ((2, 3), 3, EARLY, bulk, 0)], sums,
    )
    low, high = (0, half), (half, half)
    hidden, f_low, f_high, a_high, b_low = expert_call(
        where, weights, [early_rows, *far],
        [((0,), k, 0, EARLY, k * EARLY) for k in range(n_tp)] + [((1, 2), 2, EARLY, bulk, 0)],
        sums, inv=(0, n_tp * EARLY),
        jobs=[
            (2, EARLY, bulk, 0, rows, ((0, 0, half, 0), (1, half, half, 0))),
            (1, EARLY, bulk, *high, ((2, 0, half, 0),)),
            (3, EARLY, bulk, *low, ((3, 0, half, 0),)),
        ],
        outs=[(half, bulk)] * 4,
    )
    (p_early,) = expert_call(
        where, weights, hidden=hidden,
        jobs=[(k, 0, EARLY, 0, rows, ((0, 0, rows, k * EARLY),)) for k in range(n_tp)], outs=[(rows, n_tp * EARLY)],
    )
    a_low, b_high, o_low, o_high = expert_call(
        where, weights, hidden=hidden,
        jobs=[
            (1, EARLY, bulk, *low, ((0, 0, half, 0),)),
            (3, EARLY, bulk, *high, ((1, 0, half, 0),)),
            (0, EARLY, bulk, 0, rows, ((2, 0, half, 0), (3, half, half, 0))),
        ],
        outs=[(half, bulk)] * 4,
    )

    def combine(back):
        return lax.dot_general(weight, back, (((0,), (0,)), ((), ())), preferred_element_type=F32).astype(BF16)

    early_back = combine(exchange(p_early))
    e = [early_back[:, k * EARLY : (k + 1) * EARLY] for k in range(n_tp)]
    out_early = fold(e[0], e[1], e[3], e[2][: tok // 2], e[2][tok // 2 :])
    folded = fold_halves((o_low, o_high), (a_low, a_high), (b_low, b_high), (f_low, f_high))
    out_bulk = combine(exchange(folded))
    return jnp.concatenate([out_early, out_bulk], axis=1)


def solution(mesh):
    placed = (
        P("ep", "tp"),
        P("tp"),
        P("ep", None),
        P("ep", None),
        P("ep", None, "tp"),
        P("ep", None, "tp"),
        P("ep", "tp", None),
    )

    return jax.shard_map(local, mesh=mesh, in_specs=placed, out_specs=P("ep", "tp"), check_vma=False)
```

```python
import jax
import jax.numpy as jnp
from jax import lax
from jax.experimental import pallas as pl
from jax.experimental.pallas import tpu as pltpu
from jax.sharding import PartitionSpec as P


D = 7168
epsilon = 1e-06
CAP = 16
EARLY = 512
SIDE = 128
F32, BF16 = jnp.float32, jnp.bfloat16


class Copies:
    def __init__(self, sems):
        self.sems, self.used = sems, 0

    def start(self, src, dst):
        copy = pltpu.make_async_copy(src, dst, self.sems.at[self.used])
        self.used += 1
        copy.start()
        return copy


def expert_call(where, weights, xs=(), segs=(), carry=(), inv=None, hidden=None, jobs=(), outs=(), stash=((), ()), held=None, stored=()):
    slices = lax.axis_size("tp")
    w_gate, w_up, w_down = weights
    d_all, ff = w_gate.shape
    span = d_all // slices
    finish = bool(segs) and bool(jobs)
    rows = hidden.shape[0] if hidden is not None else sum(xs[i].shape[0] for i in segs[0][0])

    def columns_of(some):
        found = []
        for step, offset, width, *_ in some:
            if (step, offset, width) not in found:
                found.append((step, offset, width))
        return found

    def weight_shapes(seg_list, column_list):
        shapes = []
        for _, _, _, width, _ in seg_list:
            shapes += [(width, ff)] * 2
        return shapes + [(ff, width) for _, _, width in column_list]

    columns, later = columns_of(jobs), columns_of(stash[1])
    results = [((rows, ff), F32)] * 2 if not jobs else [((rows, ff), BF16)] * finish + [(s, BF16) for s in outs]
    results += [(s, BF16) for s in weight_shapes(stash[0], later)]
    resident = list(xs) + list(carry) + ([] if hidden is None else [hidden]) + list(held or ())
    streamed = ([] if held else [w_gate, w_up, w_down]) + list(stored)
    buffers = [] if held else weight_shapes(segs, columns)
    scratch = [pltpu.VMEM(s, BF16) for s in buffers]
    if finish:
        scratch += [pltpu.VMEM((rows, ff), F32)] * 2
    scratch += [pltpu.VMEM((rows, ff), F32)] * len(stored)
    n_copies = len(stored) + len(buffers) + len(weight_shapes(stash[0], later))
    scratch += [pltpu.SemaphoreType.DMA((max(n_copies, 1),))]

    def body(where_ref, *refs):
        refs = list(refs)
        take = lambda n: [refs.pop(0) for _ in range(n)]
        x_refs, carried = take(len(xs)), take(len(carry))
        hidden_ref = take(hidden is not None)
        held_refs = take(len(held or ()))
        wg, wu, wd = (None,) * 3 if held else take(3)
        stored_refs = take(len(stored))
        out_refs = take(len(results))
        bufs = take(len(buffers)) if not held else held_refs
        accs = take(2) if finish else out_refs[:2]
        stored_bufs = take(len(stored))
        copies = Copies(refs.pop(0))
        z = where_ref[0]

        def bring(seg_list, column_list, into):
            waits = []
            for _, step, offset, width, _ in seg_list:
                at = pl.ds(pl.multiple_of(lax.rem(z + step, slices) * span + offset, 128), width)
                waits += [copies.start(w.at[at, :], into[len(waits) + n]) for n, w in enumerate((wg, wu))]
            for step, offset, width in column_list:
                at = pl.ds(pl.multiple_of(lax.rem(z + step, slices) * span + offset, 128), width)
                waits.append(copies.start(wd.at[:, at], into[len(waits)]))
            return waits

        waits = [] if held else bring(segs, columns, bufs)
        stored_waits = [copies.start(r, b) for r, b in zip(stored_refs, stored_bufs)]
        n_stash = len(weight_shapes(stash[0], later))
        stash_waits = bring(stash[0], later, out_refs[len(out_refs) - n_stash :]) if n_stash else []
        for k, (index, _, _, width, col) in enumerate(segs):
            x = [x_refs[i][:, col : col + width] for i in index]
            x = x[0] if len(x) == 1 else jnp.concatenate(x, axis=0)
            for n, acc in enumerate(accs):
                if waits:
                    waits[2 * k + n].wait()
                term = jnp.dot(x, bufs[2 * k + n][...], preferred_element_type=F32)
                if k:
                    term = acc[...] + term
                elif carry:
                    term = carried[n][...] + term
                if stored and k == len(segs) - 1:
                    stored_waits[n].wait()
                    term = stored_bufs[n][...] + term
                acc[...] = term
        if finish:
            scale = jnp.sum(x_refs[inv[0]][:, inv[1] : inv[1] + SIDE].astype(F32), axis=1, keepdims=True)
            gate = accs[0][...] * scale
            hidden_ref = [out_refs.pop(0)]
            hidden_ref[0][...] = (jax.nn.silu(gate) * (accs[1][...] * scale)).astype(BF16)
        waited = set()
        for step, offset, width, row, count, targets in jobs:
            k = columns.index((step, offset, width))
            if waits and k not in waited:
                waits[2 * len(segs) + k].wait()
                waited.add(k)
            w = bufs[2 * len(segs) + k]
            term = jnp.dot(hidden_ref[0][row : row + count, :], w[...], preferred_element_type=F32).astype(BF16)
            for index, top, n, col in targets:
                out_refs[index][:, col : col + width] = term[top : top + n, :]
        for w in stash_waits:
            w.wait()

    vmem, hbm = pl.BlockSpec(memory_space=pltpu.VMEM), pl.BlockSpec(memory_space=pltpu.HBM)
    flops = sum(4 * rows * s[3] * ff for s in segs) + sum(2 * j[4] * ff * j[2] for j in jobs)
    return pl.pallas_call(
        body,
        in_specs=[pl.BlockSpec(memory_space=pltpu.SMEM)] + [vmem] * len(resident) + [hbm] * len(streamed),
        out_specs=[vmem] * len(results),
        out_shape=[pltpu.VMEM(s, t) for s, t in results],
        scratch_shapes=scratch,
        cost_estimate=pl.CostEstimate(flops=flops, bytes_accessed=flops // 256, transcendentals=0),
        compiler_params=pltpu.CompilerParams(vmem_limit_bytes=20 * 2**20),
    )(
        where,
        *[pltpu.with_memory_space_constraint(x, pltpu.VMEM) for x in resident],
        *[pltpu.with_memory_space_constraint(x, pltpu.HBM) for x in streamed],
    )


def side_columns(value):
    lane = lax.broadcasted_iota(jnp.int32, (value.shape[0], SIDE), 1)
    out = jnp.zeros((value.shape[0], SIDE), F32)
    for k in range(3):
        term = value.astype(BF16).astype(F32)
        out = jnp.where(lane == k, term, out)
        value = value - term
    return out.astype(BF16)


def head(tokens, norm_gain, ids, window):
    tok, width = tokens.shape
    rows, bulk = window * CAP, width - EARLY

    def body(tokens_hbm, gain_ref, ids_ref, pick_ref, bulk_ref, early_ref, tokens_ref, sem):
        load = pltpu.make_async_copy(tokens_hbm, tokens_ref, sem)
        load.start()
        expert = lax.broadcasted_iota(jnp.int32, (window, tok), 0)
        match = jnp.zeros((window, tok), F32)
        for k in range(ids.shape[0]):
            match = match + jnp.where(ids_ref[k : k + 1, :] == expert, 1.0, 0.0)
        earlier = lax.broadcasted_iota(jnp.int32, (tok, tok), 0) < lax.broadcasted_iota(jnp.int32, (tok, tok), 1)
        earlier = jnp.where(earlier, 1.0, 0.0).astype(BF16)
        before = jnp.dot(match.astype(BF16), earlier, preferred_element_type=F32)
        slot = jnp.where(match > 0.0, before, -1.0)
        row = lax.broadcasted_iota(jnp.int32, (rows, window), 0)
        own = (row // CAP) == lax.broadcasted_iota(jnp.int32, (rows, window), 1)
        spread = jnp.dot(jnp.where(own, 1.0, 0.0).astype(BF16), slot.astype(BF16), preferred_element_type=F32)
        wanted = (lax.broadcasted_iota(jnp.int32, (rows, tok), 0) % CAP).astype(F32)
        pick = jnp.where(spread == wanted, 1.0, 0.0).astype(BF16)
        pick_ref[...] = pick
        gain = gain_ref[...].astype(F32).reshape(1, width)
        load.wait()
        values = tokens_ref[...].astype(F32)
        gained = (values * gain).astype(BF16)
        bulk_ref[...] = jnp.dot(pick, gained[:, EARLY:], preferred_element_type=F32).astype(BF16)
        early_ref[:, :EARLY] = gained[:, :EARLY]
        early_ref[:, EARLY:] = side_columns(jnp.sum(values * values, axis=1, keepdims=True))

    return pl.pallas_call(
        body,
        in_specs=[pl.BlockSpec(memory_space=pltpu.HBM)] + [pl.BlockSpec(memory_space=pltpu.VMEM)] * 2,
        scratch_shapes=[pltpu.VMEM((tok, width), BF16), pltpu.SemaphoreType.DMA],
        out_shape=[jax.ShapeDtypeStruct(s, BF16) for s in ((rows, tok), (rows, bulk), (tok, EARLY + SIDE))],
        cost_estimate=pl.CostEstimate(flops=2 * rows * tok * bulk, bytes_accessed=2 * tok * width, transcendentals=0),
        compiler_params=pltpu.CompilerParams(vmem_limit_bytes=24 * 2**20),
        name="head",
    )(pltpu.with_memory_space_constraint(tokens, pltpu.HBM), norm_gain, ids)


def join_sums(low, high):
    half, width = low[0].shape

    def body(*refs):
        out = refs[-1]
        for k in (0, 1):
            a, b, c = (r[...].astype(F32) for r in refs[3 * k : 3 * k + 3])
            out[k * half : (k + 1) * half, :] = (a + b + c).astype(BF16)

    return pl.pallas_call(
        body,
        out_shape=jax.ShapeDtypeStruct((2 * half, width), BF16),
        cost_estimate=pl.CostEstimate(flops=6 * half * width, bytes_accessed=16 * half * width, transcendentals=0),
        compiler_params=pltpu.CompilerParams(vmem_limit_bytes=16 * 2**20),
        name="join_sums",
    )(*low, *high)


def three_terms(value):
    rest, terms = value, []
    for _ in range(3):
        term = lax.reduce_precision(rest, 8, 7)
        terms.append(term)
        rest = rest - term
    stacked = jnp.stack(terms, axis=1)
    return jnp.pad(stacked, ((0, 0), (0, SIDE - 3))).astype(BF16)


def local(tokens, norm_gain, expert_ids, gate_prob, w_gate, w_up, w_down):
    window, n_tp = lax.axis_size("ep"), lax.axis_size("tp")
    where = lax.axis_index("tp").astype(jnp.int32).reshape(1)
    w_gate, w_up, w_down = w_gate[0], w_up[0], w_down[0]
    tok = tokens.shape[0]
    rows = window * CAP
    up = [(i, (i + 1) % n_tp) for i in range(n_tp)]
    dn = [(i, (i - 1) % n_tp) for i in range(n_tp)]

    def spread(x):
        half = x.shape[0] // 2
        below, above = lax.ppermute(x, "tp", up), lax.ppermute(x, "tp", dn)
        return below, above, lax.ppermute(below[:half], "tp", up), lax.ppermute(above[half:], "tp", dn)

    def fold(own, above, below, far_a, far_b):
        half = own.shape[0] // 2
        got_a, got_b = lax.ppermute(far_a, "tp", up), lax.ppermute(far_b, "tp", dn)
        sum_up = (above.astype(F32) + jnp.pad(got_a.astype(F32), ((0, half), (0, 0)))).astype(BF16)
        sum_dn = (below.astype(F32) + jnp.pad(got_b.astype(F32), ((half, 0), (0, 0)))).astype(BF16)
        from_dn, from_up = lax.ppermute(sum_up, "tp", up), lax.ppermute(sum_dn, "tp", dn)
        return (own.astype(F32) + from_dn.astype(F32) + from_up.astype(F32)).astype(BF16)

    def spread_halves(low, high):
        below_low, above_high = lax.ppermute(low, "tp", up), lax.ppermute(high, "tp", dn)
        below_high, above_low = lax.ppermute(high, "tp", up), lax.ppermute(low, "tp", dn)
        far = lax.ppermute(below_low, "tp", up), lax.ppermute(above_high, "tp", dn)
        return (below_low, below_high), (above_low, above_high), far

    def add(*terms):
        return sum(t.astype(F32) for t in terms).astype(BF16)

    def fold_halves(own, above, below, far):
        got_low, got_high = lax.ppermute(far[0], "tp", up), lax.ppermute(far[1], "tp", dn)
        dn_high, up_low = lax.ppermute(above[1], "tp", up), lax.ppermute(below[0], "tp", dn)
        dn_low = lax.ppermute(add(above[0], got_low), "tp", up)
        up_high = lax.ppermute(add(below[1], got_high), "tp", dn)
        return join_sums((own[0], dn_low, up_low), (own[1], dn_high, up_high))

    def exchange(x):
        shaped = x.reshape(window, CAP, x.shape[1])
        return lax.all_to_all(shaped, "ep", 0, 0, tiled=True).reshape(rows, x.shape[1])

    bulk = tokens.shape[1] - EARLY
    half = rows // 2
    ids, probs = expert_ids.T, gate_prob.T.astype(F32)
    pick, picked_bulk, early = head(tokens, norm_gain, ids, window)
    same = ids[:, None, :] == jnp.arange(window, dtype=jnp.int32)[None, :, None]
    prob = jnp.sum(jnp.where(same, probs[:, None, :], 0.0), axis=0)
    by_slot = jnp.broadcast_to(prob[:, None, :], (window, CAP, tok)).reshape(rows, tok)
    weight = jnp.where(pick > 0, by_slot, 0.0).astype(BF16)

    def dispatch(x):
        return jnp.dot(pick, x, preferred_element_type=F32).astype(BF16)

    e_below, e_above, e_far_a, e_far_b = spread(early)
    mine = exchange(picked_bulk)
    e_far = jnp.concatenate([e_far_a, e_far_b], axis=0)
    all_early = (early, e_above, e_far, e_below)
    squares = sum(jnp.sum(e[:, EARLY : EARLY + 3].astype(F32), axis=1) for e in all_early)
    inverse_rms = lax.rsqrt(squares / D + epsilon)
    early_all = jnp.concatenate([e[:, :EARLY] for e in all_early] + [three_terms(inverse_rms)], axis=1)
    picked = dispatch(early_all)
    early_rows = exchange(picked)
    below, above, far = spread_halves(mine[:half], mine[half:])

    weights = (w_gate, w_up, w_down)
    low, high = (0, half), (half, half)
    far_segs = [((0, 1), 2, EARLY, bulk, 0)]
    far_jobs = [
        (2, EARLY, bulk, 0, rows, ((0, 0, half, 0), (1, half, half, 0))),
        (1, EARLY, bulk, *high, ((2, 0, half, 0),)),
        (3, EARLY, bulk, *low, ((3, 0, half, 0),)),
    ]
    sums = expert_call(where, weights, [mine], [((0,), 0, EARLY, bulk, 0)])
    sums = expert_call(
        where, weights, [*above, *below],
        [((0, 1), 1, EARLY, bulk, 0), ((2, 3), 3, EARLY, bulk, 0)], sums,
    )
    *sums, = expert_call(
        where, weights, [early_rows],
        [((0,), k, 0, EARLY, k * EARLY) for k in range(n_tp)], stored=sums, stash=(far_segs, far_jobs),
    )
    hidden, f_low, f_high, a_high, b_low = expert_call(
        where, weights, [*far, early_rows], far_segs, sums[:2], inv=(2, n_tp * EARLY),
        jobs=far_jobs, outs=[(half, bulk)] * 4, held=sums[2:],
    )
    (p_early,) = expert_call(
        where, weights, hidden=hidden,
        jobs=[(k, 0, EARLY, 0, rows, ((0, 0, rows, k * EARLY),)) for k in range(n_tp)], outs=[(rows, n_tp * EARLY)],
    )
    a_low, b_high, o_low, o_high = expert_call(
        where, weights, hidden=hidden,
        jobs=[
            (1, EARLY, bulk, *low, ((0, 0, half, 0),)),
            (3, EARLY, bulk, *high, ((1, 0, half, 0),)),
            (0, EARLY, bulk, 0, rows, ((2, 0, half, 0), (3, half, half, 0))),
        ],
        outs=[(half, bulk)] * 4,
    )

    def combine(back):
        return lax.dot_general(weight, back, (((0,), (0,)), ((), ())), preferred_element_type=F32).astype(BF16)

    early_back = combine(exchange(p_early))
    e = [early_back[:, k * EARLY : (k + 1) * EARLY] for k in range(n_tp)]
    out_early = fold(e[0], e[1], e[3], e[2][: tok // 2], e[2][tok // 2 :])
    folded = fold_halves((o_low, o_high), (a_low, a_high), (b_low, b_high), (f_low, f_high))
    out_bulk = combine(exchange(folded))
    return jnp.concatenate([out_early, out_bulk], axis=1)


def solution(mesh):
    placed = (
        P("ep", "tp"),
        P("tp"),
        P("ep", None),
        P("ep", None),
        P("ep", None, "tp"),
        P("ep", None, "tp"),
        P("ep", "tp", None),
    )

    return jax.shard_map(local, mesh=mesh, in_specs=placed, out_specs=P("ep", "tp"), check_vma=False)
```

```python
import jax
import jax.numpy as jnp
from jax import lax
from jax.experimental import pallas as pl
from jax.experimental.pallas import tpu as pltpu
from jax.sharding import PartitionSpec as P


D = 7168
epsilon = 1e-06
CAP = 16
EARLY = 512
SIDE = 128
F32, BF16 = jnp.float32, jnp.bfloat16


class Copies:
    def __init__(self, sems):
        self.sems, self.used = sems, 0

    def start(self, src, dst):
        copy = pltpu.make_async_copy(src, dst, self.sems.at[self.used])
        self.used += 1
        copy.start()
        return copy


def expert_call(where, weights, xs=(), segs=(), carry=(), inv=None, hidden=None, jobs=(), outs=(), stash=((), ()), held=(), stored=(), keep=None):
    slices = lax.axis_size("tp")
    w_gate, w_up, w_down = weights
    d_all, ff = w_gate.shape
    span = d_all // slices
    finish = bool(segs) and bool(jobs)
    rows = hidden.shape[0] if hidden is not None else sum(xs[i].shape[0] for i in segs[0][0])

    def columns_of(some):
        found = []
        for step, offset, width, *_ in some:
            if (step, offset, width) not in found:
                found.append((step, offset, width))
        return found

    def weight_shapes(seg_list, column_list):
        shapes = []
        for _, _, _, width, _ in seg_list:
            shapes += [(width, ff)] * 2
        return shapes + [(ff, width) for _, _, width in column_list]

    columns, later = columns_of(jobs), columns_of(stash[1])
    results = [((rows, ff), F32)] * 2 if not jobs else [((rows, ff), BF16)] * finish + [(s, BF16) for s in outs]
    results = [(s, t) for s, t in results] + ([((rows, SIDE), BF16)] if keep else [])
    n_out = len(results)
    results += [(s, BF16) for s in weight_shapes(stash[0], later)]
    needed = weight_shapes(segs, columns)[len(held) :]
    streams = bool(needed) or len(results) > n_out
    resident = list(xs) + list(carry) + ([] if hidden is None else [hidden]) + list(held)
    streamed = ([w_gate, w_up, w_down] if streams else []) + list(stored)
    scratch = [pltpu.VMEM(s, BF16) for s in needed]
    if finish:
        scratch += [pltpu.VMEM((rows, ff), F32)] * 2
    scratch += [pltpu.VMEM((rows, ff), F32)] * len(stored)
    n_copies = len(stored) + len(needed) + len(results) - n_out
    scratch += [pltpu.SemaphoreType.DMA((max(n_copies, 1),))]

    def body(where_ref, *refs):
        refs = list(refs)
        take = lambda n: [refs.pop(0) for _ in range(n)]
        x_refs, carried = take(len(xs)), take(len(carry))
        hidden_ref = take(hidden is not None)
        held_refs = take(len(held))
        wg, wu, wd = take(3) if streams else (None,) * 3
        stored_refs = take(len(stored))
        out_refs = take(len(results))
        bufs = held_refs + take(len(needed))
        accs = take(2) if finish else out_refs[:2]
        stored_bufs = take(len(stored))
        copies = Copies(refs.pop(0))
        z = where_ref[0]

        def bring(seg_list, column_list, into, skip):
            waits, n = [None] * skip, 0
            for _, step, offset, width, _ in seg_list:
                at = pl.ds(pl.multiple_of(lax.rem(z + step, slices) * span + offset, 128), width)
                for w in (wg, wu):
                    if n >= skip:
                        waits.append(copies.start(w.at[at, :], into[n]))
                    n += 1
            for step, offset, width in column_list:
                at = pl.ds(pl.multiple_of(lax.rem(z + step, slices) * span + offset, 128), width)
                if n >= skip:
                    waits.append(copies.start(wd.at[:, at], into[n]))
                n += 1
            return waits

        def arrived(wait):
            if wait is not None:
                wait.wait()

        waits = bring(segs, columns, bufs, len(held))
        stored_waits = [copies.start(r, b) for r, b in zip(stored_refs, stored_bufs)]
        stash_waits = bring(stash[0], later, out_refs[n_out:], 0)
        if keep:
            out_refs[2][...] = x_refs[keep[0]][:, keep[1] : keep[1] + SIDE]
        for k, (index, _, _, width, col) in enumerate(segs):
            x = [x_refs[i][:, col : col + width] for i in index]
            x = x[0] if len(x) == 1 else jnp.concatenate(x, axis=0)
            for n, acc in enumerate(accs):
                arrived(waits[2 * k + n])
                term = jnp.dot(x, bufs[2 * k + n][...], preferred_element_type=F32)
                if k:
                    term = acc[...] + term
                elif carry:
                    term = carried[n][...] + term
                if stored and k == len(segs) - 1:
                    stored_waits[n].wait()
                    term = stored_bufs[n][...] + term
                acc[...] = term
        if finish:
            scale = jnp.sum(x_refs[inv][...].astype(F32), axis=1, keepdims=True)
            gate = accs[0][...] * scale
            hidden_ref = [out_refs.pop(0)]
            hidden_ref[0][...] = (jax.nn.silu(gate) * (accs[1][...] * scale)).astype(BF16)
        waited = set()
        for step, offset, width, row, count, targets in jobs:
            k = columns.index((step, offset, width))
            if k not in waited:
                arrived(waits[2 * len(segs) + k])
                waited.add(k)
            w = bufs[2 * len(segs) + k]
            term = jnp.dot(hidden_ref[0][row : row + count, :], w[...], preferred_element_type=F32).astype(BF16)
            for index, top, n, col in targets:
                out_refs[index][:, col : col + width] = term[top : top + n, :]
        for w in stash_waits:
            w.wait()

    vmem, hbm = pl.BlockSpec(memory_space=pltpu.VMEM), pl.BlockSpec(memory_space=pltpu.HBM)
    flops = sum(4 * rows * s[3] * ff for s in segs) + sum(2 * j[4] * ff * j[2] for j in jobs)
    return pl.pallas_call(
        body,
        in_specs=[pl.BlockSpec(memory_space=pltpu.SMEM)] + [vmem] * len(resident) + [hbm] * len(streamed),
        out_specs=[vmem] * len(results),
        out_shape=[pltpu.VMEM(s, t) for s, t in results],
        scratch_shapes=scratch,
        cost_estimate=pl.CostEstimate(flops=flops, bytes_accessed=flops // 256, transcendentals=0),
        compiler_params=pltpu.CompilerParams(vmem_limit_bytes=20 * 2**20),
    )(
        where,
        *[pltpu.with_memory_space_constraint(x, pltpu.VMEM) for x in resident],
        *[pltpu.with_memory_space_constraint(x, pltpu.HBM) for x in streamed],
    )


def side_columns(value):
    lane = lax.broadcasted_iota(jnp.int32, (value.shape[0], SIDE), 1)
    out = jnp.zeros((value.shape[0], SIDE), F32)
    for k in range(3):
        term = value.astype(BF16).astype(F32)
        out = jnp.where(lane == k, term, out)
        value = value - term
    return out.astype(BF16)


def head(tokens, norm_gain, ids, window):
    tok, width = tokens.shape
    rows, bulk = window * CAP, width - EARLY

    def body(ids_hbm, gain_hbm, tokens_hbm, pick_ref, bulk_ref, early_ref, ids_ref, gain_ref, tokens_ref, sems):
        copies = Copies(sems)
        pairs = ((ids_hbm, ids_ref), (gain_hbm, gain_ref), (tokens_hbm, tokens_ref))
        ids_load, gain_load, load = [copies.start(*pair) for pair in pairs]
        ids_load.wait()
        expert = lax.broadcasted_iota(jnp.int32, (window, tok), 0)
        match = jnp.zeros((window, tok), F32)
        for k in range(ids.shape[0]):
            match = match + jnp.where(ids_ref[k : k + 1, :] == expert, 1.0, 0.0)
        earlier = lax.broadcasted_iota(jnp.int32, (tok, tok), 0) < lax.broadcasted_iota(jnp.int32, (tok, tok), 1)
        earlier = jnp.where(earlier, 1.0, 0.0).astype(BF16)
        before = jnp.dot(match.astype(BF16), earlier, preferred_element_type=F32)
        slot = jnp.where(match > 0.0, before, -1.0)
        row = lax.broadcasted_iota(jnp.int32, (rows, window), 0)
        own = (row // CAP) == lax.broadcasted_iota(jnp.int32, (rows, window), 1)
        spread = jnp.dot(jnp.where(own, 1.0, 0.0).astype(BF16), slot.astype(BF16), preferred_element_type=F32)
        wanted = (lax.broadcasted_iota(jnp.int32, (rows, tok), 0) % CAP).astype(F32)
        pick = jnp.where(spread == wanted, 1.0, 0.0).astype(BF16)
        pick_ref[...] = pick
        gain_load.wait()
        gain = gain_ref[...].astype(F32).reshape(1, width)
        load.wait()
        values = tokens_ref[...].astype(F32)
        gained = (values * gain).astype(BF16)
        bulk_ref[...] = jnp.dot(pick, gained[:, EARLY:], preferred_element_type=F32).astype(BF16)
        early_ref[:, :EARLY] = gained[:, :EARLY]
        early_ref[:, EARLY:] = side_columns(jnp.sum(values * values, axis=1, keepdims=True))

    return pl.pallas_call(
        body,
        in_specs=[pl.BlockSpec(memory_space=pltpu.HBM)] * 3,
        scratch_shapes=[pltpu.VMEM(x.shape, x.dtype) for x in (ids, norm_gain, tokens)] + [pltpu.SemaphoreType.DMA((3,))],
        out_shape=[jax.ShapeDtypeStruct(s, BF16) for s in ((rows, tok), (rows, bulk), (tok, EARLY + SIDE))],
        cost_estimate=pl.CostEstimate(flops=2 * rows * tok * bulk, bytes_accessed=2 * tok * width, transcendentals=0),
        compiler_params=pltpu.CompilerParams(vmem_limit_bytes=24 * 2**20),
        name="head",
    )(*[pltpu.with_memory_space_constraint(x, pltpu.HBM) for x in (ids, norm_gain, tokens)])


def join_sums(low, high):
    half, width = low[0].shape

    def body(*refs):
        out = refs[-1]
        for k in (0, 1):
            a, b, c = (r[...].astype(F32) for r in refs[3 * k : 3 * k + 3])
            out[k * half : (k + 1) * half, :] = (a + b + c).astype(BF16)

    return pl.pallas_call(
        body,
        out_shape=jax.ShapeDtypeStruct((2 * half, width), BF16),
        cost_estimate=pl.CostEstimate(flops=6 * half * width, bytes_accessed=16 * half * width, transcendentals=0),
        compiler_params=pltpu.CompilerParams(vmem_limit_bytes=16 * 2**20),
        name="join_sums",
    )(*low, *high)


def three_terms(value):
    rest, terms = value, []
    for _ in range(3):
        term = lax.reduce_precision(rest, 8, 7)
        terms.append(term)
        rest = rest - term
    stacked = jnp.stack(terms, axis=1)
    return jnp.pad(stacked, ((0, 0), (0, SIDE - 3))).astype(BF16)


def local(tokens, norm_gain, expert_ids, gate_prob, w_gate, w_up, w_down):
    window, n_tp = lax.axis_size("ep"), lax.axis_size("tp")
    where = lax.axis_index("tp").astype(jnp.int32).reshape(1)
    w_gate, w_up, w_down = w_gate[0], w_up[0], w_down[0]
    tok = tokens.shape[0]
    rows = window * CAP
    up = [(i, (i + 1) % n_tp) for i in range(n_tp)]
    dn = [(i, (i - 1) % n_tp) for i in range(n_tp)]

    def spread(x):
        half = x.shape[0] // 2
        below, above = lax.ppermute(x, "tp", up), lax.ppermute(x, "tp", dn)
        return below, above, lax.ppermute(below[:half], "tp", up), lax.ppermute(above[half:], "tp", dn)

    def fold(own, above, below, far_a, far_b):
        half = own.shape[0] // 2
        got_a, got_b = lax.ppermute(far_a, "tp", up), lax.ppermute(far_b, "tp", dn)
        sum_up = (above.astype(F32) + jnp.pad(got_a.astype(F32), ((0, half), (0, 0)))).astype(BF16)
        sum_dn = (below.astype(F32) + jnp.pad(got_b.astype(F32), ((half, 0), (0, 0)))).astype(BF16)
        from_dn, from_up = lax.ppermute(sum_up, "tp", up), lax.ppermute(sum_dn, "tp", dn)
        return (own.astype(F32) + from_dn.astype(F32) + from_up.astype(F32)).astype(BF16)

    def spread_halves(low, high):
        below_low, above_high = lax.ppermute(low, "tp", up), lax.ppermute(high, "tp", dn)
        below_high, above_low = lax.ppermute(high, "tp", up), lax.ppermute(low, "tp", dn)
        far = lax.ppermute(below_low, "tp", up), lax.ppermute(above_high, "tp", dn)
        return (below_low, below_high), (above_low, above_high), far

    def add(*terms):
        return sum(t.astype(F32) for t in terms).astype(BF16)

    def fold_halves(own, above, below, far):
        got_low, got_high = lax.ppermute(far[0], "tp", up), lax.ppermute(far[1], "tp", dn)
        dn_high, up_low = lax.ppermute(above[1], "tp", up), lax.ppermute(below[0], "tp", dn)
        dn_low = lax.ppermute(add(above[0], got_low), "tp", up)
        up_high = lax.ppermute(add(below[1], got_high), "tp", dn)
        return join_sums((own[0], dn_low, up_low), (own[1], dn_high, up_high))

    def exchange(x):
        shaped = x.reshape(window, CAP, x.shape[1])
        return lax.all_to_all(shaped, "ep", 0, 0, tiled=True).reshape(rows, x.shape[1])

    bulk = tokens.shape[1] - EARLY
    half = rows // 2
    ids, probs = expert_ids.T, gate_prob.T.astype(F32)
    pick, picked_bulk, early = head(tokens, norm_gain, ids, window)
    same = ids[:, None, :] == jnp.arange(window, dtype=jnp.int32)[None, :, None]
    prob = jnp.sum(jnp.where(same, probs[:, None, :], 0.0), axis=0)
    by_slot = jnp.broadcast_to(prob[:, None, :], (window, CAP, tok)).reshape(rows, tok)
    weight = jnp.where(pick > 0, by_slot, 0.0).astype(BF16)

    def dispatch(x):
        return jnp.dot(pick, x, preferred_element_type=F32).astype(BF16)

    e_below, e_above, e_far_a, e_far_b = spread(early)
    mine = exchange(picked_bulk)
    e_far = jnp.concatenate([e_far_a, e_far_b], axis=0)
    all_early = (early, e_above, e_far, e_below)
    squares = sum(jnp.sum(e[:, EARLY : EARLY + 3].astype(F32), axis=1) for e in all_early)
    inverse_rms = lax.rsqrt(squares / D + epsilon)
    early_all = jnp.concatenate([e[:, :EARLY] for e in all_early] + [three_terms(inverse_rms)], axis=1)
    picked = dispatch(early_all)
    early_rows = exchange(picked)
    below, above, far = spread_halves(mine[:half], mine[half:])

    weights = (w_gate, w_up, w_down)
    low, high = (0, half), (half, half)
    far_segs = [((0, 1), 2, EARLY, bulk, 0)]
    far_jobs = [
        (2, EARLY, bulk, 0, rows, ((0, 0, half, 0), (1, half, half, 0))),
        (1, EARLY, bulk, *high, ((2, 0, half, 0),)),
        (3, EARLY, bulk, *low, ((3, 0, half, 0),)),
    ]
    sums = expert_call(where, weights, [mine], [((0,), 0, EARLY, bulk, 0)])
    sums = expert_call(
        where, weights, [*above, *below],
        [((0, 1), 1, EARLY, bulk, 0), ((2, 3), 3, EARLY, bulk, 0)], sums,
    )
    early_jobs = [(k, 0, EARLY, 0, rows, ((0, 0, rows, k * EARLY),)) for k in range(n_tp)]
    *early_sums, scale, far_gate, far_up = expert_call(
        where, weights, [early_rows],
        [((0,), k, 0, EARLY, k * EARLY) for k in range(n_tp)], keep=(0, n_tp * EARLY), stash=(far_segs, ()),
    )
    hidden, f_low, f_high, a_high, b_low, *early_down = expert_call(
        where, weights, [*far, scale], far_segs, early_sums, inv=2, stored=sums,
        jobs=far_jobs, outs=[(half, bulk)] * 4, held=(far_gate, far_up), stash=((), early_jobs),
    )
    (p_early,) = expert_call(
        where, weights, hidden=hidden, jobs=early_jobs, outs=[(rows, n_tp * EARLY)], held=early_down,
    )
    a_low, b_high, o_low, o_high = expert_call(
        where, weights, hidden=hidden,
        jobs=[
            (1, EARLY, bulk, *low, ((0, 0, half, 0),)),
            (3, EARLY, bulk, *high, ((1, 0, half, 0),)),
            (0, EARLY, bulk, 0, rows, ((2, 0, half, 0), (3, half, half, 0))),
        ],
        outs=[(half, bulk)] * 4,
    )

    def combine(back):
        return lax.dot_general(weight, back, (((0,), (0,)), ((), ())), preferred_element_type=F32).astype(BF16)

    early_back = combine(exchange(p_early))
    e = [early_back[:, k * EARLY : (k + 1) * EARLY] for k in range(n_tp)]
    out_early = fold(e[0], e[1], e[3], e[2][: tok // 2], e[2][tok // 2 :])
    folded = fold_halves((o_low, o_high), (a_low, a_high), (b_low, b_high), (f_low, f_high))
    out_bulk = combine(exchange(folded))
    return jnp.concatenate([out_early, out_bulk], axis=1)


def solution(mesh):
    placed = (
        P("ep", "tp"),
        P("tp"),
        P("ep", None),
        P("ep", None),
        P("ep", None, "tp"),
        P("ep", None, "tp"),
        P("ep", "tp", None),
    )

    return jax.shard_map(local, mesh=mesh, in_specs=placed, out_specs=P("ep", "tp"), check_vma=False)
```

```python
import jax
import jax.numpy as jnp
from jax import lax
from jax.experimental import pallas as pl
from jax.experimental.pallas import tpu as pltpu
from jax.sharding import PartitionSpec as P


D = 7168
epsilon = 1e-06
CAP = 16
EARLY = 512
SIDE = 128
F32, BF16 = jnp.float32, jnp.bfloat16


class Copies:
    def __init__(self, sems):
        self.sems, self.used = sems, 0

    def start(self, src, dst):
        copy = pltpu.make_async_copy(src, dst, self.sems.at[self.used])
        self.used += 1
        copy.start()
        return copy


def expert_call(where, weights, xs=(), segs=(), carry=(), inv=None, hidden=None, jobs=(), outs=(), stash=((), ()), held=(), stored=(), keep=None, fetch=False):
    slices = lax.axis_size("tp")
    w_gate, w_up, w_down = weights
    d_all, ff = w_gate.shape
    span = d_all // slices
    finish = bool(segs) and bool(jobs)
    rows = hidden.shape[0] if hidden is not None else sum(xs[i].shape[0] for i in segs[0][0])

    def columns_of(some):
        found = []
        for step, offset, width, *_ in some:
            if (step, offset, width) not in found:
                found.append((step, offset, width))
        return found

    def weight_shapes(seg_list, column_list):
        shapes = []
        for _, _, _, width, _ in seg_list:
            shapes += [(width, ff)] * 2
        return shapes + [(ff, width) for _, _, width in column_list]

    columns, later = columns_of(jobs), columns_of(stash[1])
    results = [((rows, ff), F32)] * 2 if not jobs else [((rows, ff), BF16)] * finish + [(s, BF16) for s in outs]
    results = [(s, t) for s, t in results] + ([((rows, SIDE), BF16)] if keep else [])
    n_out = len(results)
    results += [(s, BF16) for s in weight_shapes(stash[0], later)]
    needed = weight_shapes(segs, columns)[len(held) :]
    streams = bool(needed) or len(results) > n_out
    resident = ([] if fetch else list(xs)) + list(carry) + ([] if hidden is None else [hidden]) + list(held)
    streamed = ([w_gate, w_up, w_down] if streams else []) + list(stored) + (list(xs) if fetch else [])
    fetched = [(rows, seg[3]) for seg in segs] if fetch else []
    scratch = [pltpu.VMEM(s, BF16) for s in needed]
    if finish:
        scratch += [pltpu.VMEM((rows, ff), F32)] * 2
    scratch += [pltpu.VMEM((rows, ff), F32)] * len(stored)
    scratch += [pltpu.VMEM(shape, BF16) for shape in fetched]
    n_copies = len(fetched) + bool(fetch and keep) + len(stored) + len(needed) + len(results) - n_out
    scratch += [pltpu.SemaphoreType.DMA((max(n_copies, 1),))]

    def body(where_ref, *refs):
        refs = list(refs)
        take = lambda n: [refs.pop(0) for _ in range(n)]
        x_refs, carried = take(0 if fetch else len(xs)), take(len(carry))
        hidden_ref = take(hidden is not None)
        held_refs = take(len(held))
        wg, wu, wd = take(3) if streams else (None,) * 3
        stored_refs = take(len(stored))
        x_refs = take(len(xs)) if fetch else x_refs
        out_refs = take(len(results))
        bufs = held_refs + take(len(needed))
        accs = take(2) if finish else out_refs[:2]
        stored_bufs = take(len(stored))
        x_bufs = take(len(fetched))
        copies = Copies(refs.pop(0))
        z = where_ref[0]

        def bring(seg_list, column_list, into, skip):
            waits, n = [None] * skip, 0
            for _, step, offset, width, _ in seg_list:
                at = pl.ds(pl.multiple_of(lax.rem(z + step, slices) * span + offset, 128), width)
                for w in (wg, wu):
                    if n >= skip:
                        waits.append(copies.start(w.at[at, :], into[n]))
                    n += 1
            for step, offset, width in column_list:
                at = pl.ds(pl.multiple_of(lax.rem(z + step, slices) * span + offset, 128), width)
                if n >= skip:
                    waits.append(copies.start(wd.at[:, at], into[n]))
                n += 1
            return waits

        def arrived(wait):
            if wait is not None:
                wait.wait()

        x_waits = [
            copies.start(x_refs[index[0]].at[:, pl.ds(col, width)], buf)
            for (index, _, _, width, col), buf in zip(segs, x_bufs)
        ]
        waits = bring(segs, columns, bufs, len(held))
        stored_waits = [copies.start(r, b) for r, b in zip(stored_refs, stored_bufs)]
        stash_waits = bring(stash[0], later, out_refs[n_out:], 0)
        if keep:
            scale_cols = x_refs[keep[0]].at[:, pl.ds(keep[1], SIDE)]
            if fetch:
                stash_waits.append(copies.start(scale_cols, out_refs[2]))
            else:
                out_refs[2][...] = scale_cols[...]
        for k, (index, _, _, width, col) in enumerate(segs):
            if fetch:
                x_waits[k].wait()
                x = [x_bufs[k][...]]
            else:
                x = [x_refs[i][:, col : col + width] for i in index]
            x = x[0] if len(x) == 1 else jnp.concatenate(x, axis=0)
            for n, acc in enumerate(accs):
                arrived(waits[2 * k + n])
                term = jnp.dot(x, bufs[2 * k + n][...], preferred_element_type=F32)
                if k:
                    term = acc[...] + term
                elif carry:
                    term = carried[n][...] + term
                if stored and k == len(segs) - 1:
                    stored_waits[n].wait()
                    term = stored_bufs[n][...] + term
                acc[...] = term
        if finish:
            scale = jnp.sum(x_refs[inv][...].astype(F32), axis=1, keepdims=True)
            gate = accs[0][...] * scale
            hidden_ref = [out_refs.pop(0)]
            hidden_ref[0][...] = (jax.nn.silu(gate) * (accs[1][...] * scale)).astype(BF16)
        waited = set()
        for step, offset, width, row, count, targets in jobs:
            k = columns.index((step, offset, width))
            if k not in waited:
                arrived(waits[2 * len(segs) + k])
                waited.add(k)
            w = bufs[2 * len(segs) + k]
            term = jnp.dot(hidden_ref[0][row : row + count, :], w[...], preferred_element_type=F32).astype(BF16)
            for index, top, n, col in targets:
                out_refs[index][:, col : col + width] = term[top : top + n, :]
        for w in stash_waits:
            w.wait()

    vmem, hbm = pl.BlockSpec(memory_space=pltpu.VMEM), pl.BlockSpec(memory_space=pltpu.HBM)
    flops = sum(4 * rows * s[3] * ff for s in segs) + sum(2 * j[4] * ff * j[2] for j in jobs)
    return pl.pallas_call(
        body,
        in_specs=[pl.BlockSpec(memory_space=pltpu.SMEM)] + [vmem] * len(resident) + [hbm] * len(streamed),
        out_specs=[vmem] * len(results),
        out_shape=[pltpu.VMEM(s, t) for s, t in results],
        scratch_shapes=scratch,
        cost_estimate=pl.CostEstimate(flops=flops, bytes_accessed=flops // 256, transcendentals=0),
        compiler_params=pltpu.CompilerParams(vmem_limit_bytes=20 * 2**20),
    )(
        where,
        *[pltpu.with_memory_space_constraint(x, pltpu.VMEM) for x in resident],
        *[pltpu.with_memory_space_constraint(x, pltpu.HBM) for x in streamed],
    )


def side_columns(value):
    lane = lax.broadcasted_iota(jnp.int32, (value.shape[0], SIDE), 1)
    out = jnp.zeros((value.shape[0], SIDE), F32)
    for k in range(3):
        term = value.astype(BF16).astype(F32)
        out = jnp.where(lane == k, term, out)
        value = value - term
    return out.astype(BF16)


def head(tokens, norm_gain, ids, window):
    tok, width = tokens.shape
    rows, bulk = window * CAP, width - EARLY

    def body(ids_hbm, gain_hbm, tokens_hbm, pick_ref, bulk_ref, early_ref, ids_ref, gain_ref, tokens_ref, sems):
        copies = Copies(sems)
        pairs = ((ids_hbm, ids_ref), (gain_hbm, gain_ref), (tokens_hbm, tokens_ref))
        ids_load, gain_load, load = [copies.start(*pair) for pair in pairs]
        ids_load.wait()
        expert = lax.broadcasted_iota(jnp.int32, (window, tok), 0)
        match = jnp.zeros((window, tok), F32)
        for k in range(ids.shape[0]):
            match = match + jnp.where(ids_ref[k : k + 1, :] == expert, 1.0, 0.0)
        earlier = lax.broadcasted_iota(jnp.int32, (tok, tok), 0) < lax.broadcasted_iota(jnp.int32, (tok, tok), 1)
        earlier = jnp.where(earlier, 1.0, 0.0).astype(BF16)
        before = jnp.dot(match.astype(BF16), earlier, preferred_element_type=F32)
        slot = jnp.where(match > 0.0, before, -1.0)
        row = lax.broadcasted_iota(jnp.int32, (rows, window), 0)
        own = (row // CAP) == lax.broadcasted_iota(jnp.int32, (rows, window), 1)
        spread = jnp.dot(jnp.where(own, 1.0, 0.0).astype(BF16), slot.astype(BF16), preferred_element_type=F32)
        wanted = (lax.broadcasted_iota(jnp.int32, (rows, tok), 0) % CAP).astype(F32)
        pick = jnp.where(spread == wanted, 1.0, 0.0).astype(BF16)
        pick_ref[...] = pick
        gain_load.wait()
        gain = gain_ref[...].astype(F32).reshape(1, width)
        load.wait()
        values = tokens_ref[...].astype(F32)
        gained = (values * gain).astype(BF16)
        bulk_ref[...] = jnp.dot(pick, gained[:, EARLY:], preferred_element_type=F32).astype(BF16)
        early_ref[:, :EARLY] = gained[:, :EARLY]
        early_ref[:, EARLY:] = side_columns(jnp.sum(values * values, axis=1, keepdims=True))

    return pl.pallas_call(
        body,
        in_specs=[pl.BlockSpec(memory_space=pltpu.HBM)] * 3,
        scratch_shapes=[pltpu.VMEM(x.shape, x.dtype) for x in (ids, norm_gain, tokens)] + [pltpu.SemaphoreType.DMA((3,))],
        out_shape=[jax.ShapeDtypeStruct(s, BF16) for s in ((rows, tok), (rows, bulk), (tok, EARLY + SIDE))],
        cost_estimate=pl.CostEstimate(flops=2 * rows * tok * bulk, bytes_accessed=2 * tok * width, transcendentals=0),
        compiler_params=pltpu.CompilerParams(vmem_limit_bytes=24 * 2**20),
        name="head",
    )(*[pltpu.with_memory_space_constraint(x, pltpu.HBM) for x in (ids, norm_gain, tokens)])


def join_sums(low, high):
    half, width = low[0].shape

    def body(*refs):
        out = refs[-1]
        for k in (0, 1):
            a, b, c = (r[...].astype(F32) for r in refs[3 * k : 3 * k + 3])
            out[k * half : (k + 1) * half, :] = (a + b + c).astype(BF16)

    return pl.pallas_call(
        body,
        out_shape=jax.ShapeDtypeStruct((2 * half, width), BF16),
        cost_estimate=pl.CostEstimate(flops=6 * half * width, bytes_accessed=16 * half * width, transcendentals=0),
        compiler_params=pltpu.CompilerParams(vmem_limit_bytes=16 * 2**20),
        name="join_sums",
    )(*low, *high)


def three_terms(value):
    rest, terms = value, []
    for _ in range(3):
        term = lax.reduce_precision(rest, 8, 7)
        terms.append(term)
        rest = rest - term
    stacked = jnp.stack(terms, axis=1)
    return jnp.pad(stacked, ((0, 0), (0, SIDE - 3))).astype(BF16)


def local(tokens, norm_gain, expert_ids, gate_prob, w_gate, w_up, w_down):
    window, n_tp = lax.axis_size("ep"), lax.axis_size("tp")
    where = lax.axis_index("tp").astype(jnp.int32).reshape(1)
    w_gate, w_up, w_down = w_gate[0], w_up[0], w_down[0]
    tok = tokens.shape[0]
    rows = window * CAP
    up = [(i, (i + 1) % n_tp) for i in range(n_tp)]
    dn = [(i, (i - 1) % n_tp) for i in range(n_tp)]

    def spread(x):
        half = x.shape[0] // 2
        below, above = lax.ppermute(x, "tp", up), lax.ppermute(x, "tp", dn)
        return below, above, lax.ppermute(below[:half], "tp", up), lax.ppermute(above[half:], "tp", dn)

    def fold(own, above, below, far_a, far_b):
        half = own.shape[0] // 2
        got_a, got_b = lax.ppermute(far_a, "tp", up), lax.ppermute(far_b, "tp", dn)
        sum_up = (above.astype(F32) + jnp.pad(got_a.astype(F32), ((0, half), (0, 0)))).astype(BF16)
        sum_dn = (below.astype(F32) + jnp.pad(got_b.astype(F32), ((half, 0), (0, 0)))).astype(BF16)
        from_dn, from_up = lax.ppermute(sum_up, "tp", up), lax.ppermute(sum_dn, "tp", dn)
        return (own.astype(F32) + from_dn.astype(F32) + from_up.astype(F32)).astype(BF16)

    def spread_halves(low, high):
        below_low, above_high = lax.ppermute(low, "tp", up), lax.ppermute(high, "tp", dn)
        below_high, above_low = lax.ppermute(high, "tp", up), lax.ppermute(low, "tp", dn)
        far = lax.ppermute(below_low, "tp", up), lax.ppermute(above_high, "tp", dn)
        return (below_low, below_high), (above_low, above_high), far

    def add(*terms):
        return sum(t.astype(F32) for t in terms).astype(BF16)

    def fold_halves(own, above, below, far):
        got_low, got_high = lax.ppermute(far[0], "tp", up), lax.ppermute(far[1], "tp", dn)
        dn_high, up_low = lax.ppermute(above[1], "tp", up), lax.ppermute(below[0], "tp", dn)
        dn_low = lax.ppermute(add(above[0], got_low), "tp", up)
        up_high = lax.ppermute(add(below[1], got_high), "tp", dn)
        return join_sums((own[0], dn_low, up_low), (own[1], dn_high, up_high))

    def exchange(x):
        shaped = x.reshape(window, CAP, x.shape[1])
        return lax.all_to_all(shaped, "ep", 0, 0, tiled=True).reshape(rows, x.shape[1])

    bulk = tokens.shape[1] - EARLY
    half = rows // 2
    ids, probs = expert_ids.T, gate_prob.T.astype(F32)
    pick, picked_bulk, early = head(tokens, norm_gain, ids, window)
    same = ids[:, None, :] == jnp.arange(window, dtype=jnp.int32)[None, :, None]
    prob = jnp.sum(jnp.where(same, probs[:, None, :], 0.0), axis=0)
    by_slot = jnp.broadcast_to(prob[:, None, :], (window, CAP, tok)).reshape(rows, tok)
    weight = jnp.where(pick > 0, by_slot, 0.0).astype(BF16)

    def dispatch(x):
        return jnp.dot(pick, x, preferred_element_type=F32).astype(BF16)

    e_below, e_above, e_far_a, e_far_b = spread(early)
    mine = exchange(picked_bulk)
    e_far = jnp.concatenate([e_far_a, e_far_b], axis=0)
    all_early = (early, e_above, e_far, e_below)
    squares = sum(jnp.sum(e[:, EARLY : EARLY + 3].astype(F32), axis=1) for e in all_early)
    inverse_rms = lax.rsqrt(squares / D + epsilon)
    early_all = jnp.concatenate([e[:, :EARLY] for e in all_early] + [three_terms(inverse_rms)], axis=1)
    picked = dispatch(early_all)
    early_rows = exchange(picked)
    below, above, far = spread_halves(mine[:half], mine[half:])

    weights = (w_gate, w_up, w_down)
    low, high = (0, half), (half, half)
    far_segs = [((0, 1), 2, EARLY, bulk, 0)]
    far_jobs = [
        (2, EARLY, bulk, 0, rows, ((0, 0, half, 0), (1, half, half, 0))),
        (1, EARLY, bulk, *high, ((2, 0, half, 0),)),
        (3, EARLY, bulk, *low, ((3, 0, half, 0),)),
    ]
    sums = expert_call(where, weights, [mine], [((0,), 0, EARLY, bulk, 0)])
    sums = expert_call(
        where, weights, [*above, *below],
        [((0, 1), 1, EARLY, bulk, 0), ((2, 3), 3, EARLY, bulk, 0)], sums,
    )
    early_jobs = [(k, 0, EARLY, 0, rows, ((0, 0, rows, k * EARLY),)) for k in range(n_tp)]
    gate_sum, up_sum, scale, *far_held = expert_call(
        where, weights, [early_rows], [((0,), k, 0, EARLY, k * EARLY) for k in range(n_tp)],
        stored=sums, keep=(0, n_tp * EARLY), stash=(far_segs, far_jobs), fetch=True,
    )
    hidden, f_low, f_high, a_high, b_low, *early_down = expert_call(
        where, weights, [*far, scale], far_segs, (gate_sum, up_sum), inv=2,
        jobs=far_jobs, outs=[(half, bulk)] * 4, held=far_held, stash=((), early_jobs),
    )
    (p_early,) = expert_call(
        where, weights, hidden=hidden, jobs=early_jobs, outs=[(rows, n_tp * EARLY)], held=early_down,
    )
    a_low, b_high, o_low, o_high = expert_call(
        where, weights, hidden=hidden,
        jobs=[
            (1, EARLY, bulk, *low, ((0, 0, half, 0),)),
            (3, EARLY, bulk, *high, ((1, 0, half, 0),)),
            (0, EARLY, bulk, 0, rows, ((2, 0, half, 0), (3, half, half, 0))),
        ],
        outs=[(half, bulk)] * 4,
    )

    def combine(back):
        return lax.dot_general(weight, back, (((0,), (0,)), ((), ())), preferred_element_type=F32).astype(BF16)

    early_back = combine(exchange(p_early))
    e = [early_back[:, k * EARLY : (k + 1) * EARLY] for k in range(n_tp)]
    out_early = fold(e[0], e[1], e[3], e[2][: tok // 2], e[2][tok // 2 :])
    folded = fold_halves((o_low, o_high), (a_low, a_high), (b_low, b_high), (f_low, f_high))
    out_bulk = combine(exchange(folded))
    return jnp.concatenate([out_early, out_bulk], axis=1)


def solution(mesh):
    placed = (
        P("ep", "tp"),
        P("tp"),
        P("ep", None),
        P("ep", None),
        P("ep", None, "tp"),
        P("ep", None, "tp"),
        P("ep", "tp", None),
    )

    return jax.shard_map(local, mesh=mesh, in_specs=placed, out_specs=P("ep", "tp"), check_vma=False)
```

```python
import jax
import jax.numpy as jnp
from jax import lax
from jax.experimental import pallas as pl
from jax.experimental.pallas import tpu as pltpu
from jax.sharding import PartitionSpec as P


D = 7168
epsilon = 1e-06
CAP = 16
EARLY = 512
SIDE = 128
F32, BF16 = jnp.float32, jnp.bfloat16


class Copies:
    def __init__(self, sems):
        self.sems, self.used = sems, 0

    def start(self, src, dst):
        copy = pltpu.make_async_copy(src, dst, self.sems.at[self.used])
        self.used += 1
        copy.start()
        return copy


def expert_call(where, weights, xs=(), segs=(), carry=(), inv=None, hidden=None, jobs=(), outs=(), stash=((), ()), held=(), stored=(), keep=None, leave=False):
    slices = lax.axis_size("tp")
    w_gate, w_up, w_down = weights
    d_all, ff = w_gate.shape
    span = d_all // slices
    finish = bool(segs) and bool(jobs)
    rows = hidden.shape[0] if hidden is not None else sum(xs[i].shape[0] for i in segs[0][0])

    def columns_of(some):
        found = []
        for step, offset, width, *_ in some:
            if (step, offset, width) not in found:
                found.append((step, offset, width))
        return found

    def weight_shapes(seg_list, column_list):
        shapes = []
        for _, _, _, width, _ in seg_list:
            shapes += [(width, ff)] * 2
        return shapes + [(ff, width) for _, _, width in column_list]

    columns, later = columns_of(jobs), columns_of(stash[1])
    results = [((rows, ff), F32)] * 2 if not jobs else [((rows, ff), BF16)] * finish + [(s, BF16) for s in outs]
    results = [(s, t) for s, t in results] + ([((rows, SIDE), BF16)] if keep else [])
    n_out = len(results)
    results += [(s, BF16) for s in weight_shapes(stash[0], later)]
    needed = weight_shapes(segs, columns)[len(held) :]
    streams = bool(needed) or len(results) > n_out
    resident = list(xs) + list(carry) + ([] if hidden is None else [hidden]) + list(held)
    streamed = ([w_gate, w_up, w_down] if streams else []) + list(stored)
    scratch = [pltpu.VMEM(s, BF16) for s in needed]
    if finish:
        scratch += [pltpu.VMEM((rows, ff), F32)] * 2
    scratch += [pltpu.VMEM((rows, ff), F32)] * len(stored)
    scratch += [pltpu.VMEM(s, BF16) for s in outs] * leave
    n_copies = len(jobs) * leave + len(stored) + len(needed) + len(results) - n_out
    scratch += [pltpu.SemaphoreType.DMA((max(n_copies, 1),))]

    def body(where_ref, *refs):
        refs = list(refs)
        take = lambda n: [refs.pop(0) for _ in range(n)]
        x_refs, carried = take(len(xs)), take(len(carry))
        hidden_ref = take(hidden is not None)
        held_refs = take(len(held))
        wg, wu, wd = take(3) if streams else (None,) * 3
        stored_refs = take(len(stored))
        out_refs = take(len(results))
        bufs = held_refs + take(len(needed))
        accs = take(2) if finish else out_refs[:2]
        stored_bufs = take(len(stored))
        staged = take(int(leave))
        copies = Copies(refs.pop(0))
        z = where_ref[0]

        def bring(seg_list, column_list, into, skip):
            waits, n = [None] * skip, 0
            for _, step, offset, width, _ in seg_list:
                at = pl.ds(pl.multiple_of(lax.rem(z + step, slices) * span + offset, 128), width)
                for w in (wg, wu):
                    if n >= skip:
                        waits.append(copies.start(w.at[at, :], into[n]))
                    n += 1
            for step, offset, width in column_list:
                at = pl.ds(pl.multiple_of(lax.rem(z + step, slices) * span + offset, 128), width)
                if n >= skip:
                    waits.append(copies.start(wd.at[:, at], into[n]))
                n += 1
            return waits

        def arrived(wait):
            if wait is not None:
                wait.wait()

        waits = bring(segs, columns, bufs, len(held))
        stored_waits = [copies.start(r, b) for r, b in zip(stored_refs, stored_bufs)]
        stash_waits = bring(stash[0], later, out_refs[n_out:], 0)
        if keep:
            out_refs[2][...] = x_refs[keep[0]][:, keep[1] : keep[1] + SIDE]
        for k, (index, _, _, width, col) in enumerate(segs):
            x = [x_refs[i][:, col : col + width] for i in index]
            x = x[0] if len(x) == 1 else jnp.concatenate(x, axis=0)
            for n, acc in enumerate(accs):
                arrived(waits[2 * k + n])
                term = jnp.dot(x, bufs[2 * k + n][...], preferred_element_type=F32)
                if k:
                    term = acc[...] + term
                elif carry:
                    term = carried[n][...] + term
                if stored and k == len(segs) - 1:
                    stored_waits[n].wait()
                    term = stored_bufs[n][...] + term
                acc[...] = term
        if finish:
            scale = jnp.sum(x_refs[inv][...].astype(F32), axis=1, keepdims=True)
            gate = accs[0][...] * scale
            hidden_ref = [out_refs.pop(0)]
            hidden_ref[0][...] = (jax.nn.silu(gate) * (accs[1][...] * scale)).astype(BF16)
        waited = set()
        for step, offset, width, row, count, targets in jobs:
            k = columns.index((step, offset, width))
            if k not in waited:
                arrived(waits[2 * len(segs) + k])
                waited.add(k)
            w = bufs[2 * len(segs) + k]
            term = jnp.dot(hidden_ref[0][row : row + count, :], w[...], preferred_element_type=F32).astype(BF16)
            for index, top, n, col in targets:
                to = staged[0] if leave else out_refs[index]
                to[:, col : col + width] = term[top : top + n, :]
                if leave:
                    at = pl.ds(col, width)
                    stash_waits.append(copies.start(to.at[:, at], out_refs[index].at[:, at]))
        for w in stash_waits:
            w.wait()

    vmem, hbm = pl.BlockSpec(memory_space=pltpu.VMEM), pl.BlockSpec(memory_space=pltpu.HBM)
    flops = sum(4 * rows * s[3] * ff for s in segs) + sum(2 * j[4] * ff * j[2] for j in jobs)
    return pl.pallas_call(
        body,
        in_specs=[pl.BlockSpec(memory_space=pltpu.SMEM)] + [vmem] * len(resident) + [hbm] * len(streamed),
        out_specs=[hbm if leave else vmem] * len(results),
        out_shape=[jax.ShapeDtypeStruct(s, t) if leave else pltpu.VMEM(s, t) for s, t in results],
        scratch_shapes=scratch,
        cost_estimate=pl.CostEstimate(flops=flops, bytes_accessed=flops // 256, transcendentals=0),
        compiler_params=pltpu.CompilerParams(vmem_limit_bytes=20 * 2**20),
    )(
        where,
        *[pltpu.with_memory_space_constraint(x, pltpu.VMEM) for x in resident],
        *[pltpu.with_memory_space_constraint(x, pltpu.HBM) for x in streamed],
    )


def side_columns(value):
    lane = lax.broadcasted_iota(jnp.int32, (value.shape[0], SIDE), 1)
    out = jnp.zeros((value.shape[0], SIDE), F32)
    for k in range(3):
        term = value.astype(BF16).astype(F32)
        out = jnp.where(lane == k, term, out)
        value = value - term
    return out.astype(BF16)


def head(tokens, norm_gain, ids, window):
    tok, width = tokens.shape
    rows, bulk = window * CAP, width - EARLY

    def body(ids_hbm, gain_hbm, tokens_hbm, pick_ref, bulk_ref, early_ref, ids_ref, gain_ref, tokens_ref, sems):
        copies = Copies(sems)
        pairs = ((ids_hbm, ids_ref), (gain_hbm, gain_ref), (tokens_hbm, tokens_ref))
        ids_load, gain_load, load = [copies.start(*pair) for pair in pairs]
        ids_load.wait()
        expert = lax.broadcasted_iota(jnp.int32, (window, tok), 0)
        match = jnp.zeros((window, tok), F32)
        for k in range(ids.shape[0]):
            match = match + jnp.where(ids_ref[k : k + 1, :] == expert, 1.0, 0.0)
        earlier = lax.broadcasted_iota(jnp.int32, (tok, tok), 0) < lax.broadcasted_iota(jnp.int32, (tok, tok), 1)
        earlier = jnp.where(earlier, 1.0, 0.0).astype(BF16)
        before = jnp.dot(match.astype(BF16), earlier, preferred_element_type=F32)
        slot = jnp.where(match > 0.0, before, -1.0)
        row = lax.broadcasted_iota(jnp.int32, (rows, window), 0)
        own = (row // CAP) == lax.broadcasted_iota(jnp.int32, (rows, window), 1)
        spread = jnp.dot(jnp.where(own, 1.0, 0.0).astype(BF16), slot.astype(BF16), preferred_element_type=F32)
        wanted = (lax.broadcasted_iota(jnp.int32, (rows, tok), 0) % CAP).astype(F32)
        pick = jnp.where(spread == wanted, 1.0, 0.0).astype(BF16)
        pick_ref[...] = pick
        gain_load.wait()
        gain = gain_ref[...].astype(F32).reshape(1, width)
        load.wait()
        values = tokens_ref[...].astype(F32)
        gained = (values * gain).astype(BF16)
        bulk_ref[...] = jnp.dot(pick, gained[:, EARLY:], preferred_element_type=F32).astype(BF16)
        early_ref[:, :EARLY] = gained[:, :EARLY]
        early_ref[:, EARLY:] = side_columns(jnp.sum(values * values, axis=1, keepdims=True))

    return pl.pallas_call(
        body,
        in_specs=[pl.BlockSpec(memory_space=pltpu.HBM)] * 3,
        scratch_shapes=[pltpu.VMEM(x.shape, x.dtype) for x in (ids, norm_gain, tokens)] + [pltpu.SemaphoreType.DMA((3,))],
        out_shape=[jax.ShapeDtypeStruct(s, BF16) for s in ((rows, tok), (rows, bulk), (tok, EARLY + SIDE))],
        cost_estimate=pl.CostEstimate(flops=2 * rows * tok * bulk, bytes_accessed=2 * tok * width, transcendentals=0),
        compiler_params=pltpu.CompilerParams(vmem_limit_bytes=24 * 2**20),
        name="head",
    )(*[pltpu.with_memory_space_constraint(x, pltpu.HBM) for x in (ids, norm_gain, tokens)])


def join_sums(low, high):
    half, width = low[0].shape

    def body(*refs):
        out = refs[-1]
        for k in (0, 1):
            a, b, c = (r[...].astype(F32) for r in refs[3 * k : 3 * k + 3])
            out[k * half : (k + 1) * half, :] = (a + b + c).astype(BF16)

    return pl.pallas_call(
        body,
        out_shape=jax.ShapeDtypeStruct((2 * half, width), BF16),
        cost_estimate=pl.CostEstimate(flops=6 * half * width, bytes_accessed=16 * half * width, transcendentals=0),
        compiler_params=pltpu.CompilerParams(vmem_limit_bytes=16 * 2**20),
        name="join_sums",
    )(*low, *high)


def early_near(pick, pieces, n_slices):
    rows = pick.shape[0]

    def body(pick_ref, *refs):
        xs, out, buf, sems = refs[: len(pieces)], refs[-3], refs[-2], refs[-1]
        copies = Copies(sems)
        waits = []
        for k, (number, _) in enumerate(pieces):
            buf[k] = jnp.dot(pick_ref[...], xs[k][:, :EARLY], preferred_element_type=F32).astype(BF16)
            waits.append(copies.start(buf.at[k], out.at[:, pl.ds(number * EARLY, EARLY)]))
        for w in waits:
            w.wait()

    return pl.pallas_call(
        body,
        out_specs=pl.BlockSpec(memory_space=pltpu.HBM),
        out_shape=jax.ShapeDtypeStruct((rows, n_slices * EARLY + SIDE), BF16),
        scratch_shapes=[pltpu.VMEM((len(pieces), rows, EARLY), BF16), pltpu.SemaphoreType.DMA((len(pieces),))],
        compiler_params=pltpu.CompilerParams(vmem_limit_bytes=16 * 2**20),
        name="early_near",
    )(pick, *[x for _, x in pieces])


def early_rest(pick, number, halves, others, partial, d_all):
    rows, _ = pick.shape

    def body(pick_ref, low, high, *refs):
        xs, (_, out, buf, sems) = refs[: len(others)], refs[len(others) :]
        copies = Copies(sems)
        total = jnp.concatenate([r[:, EARLY:].astype(F32) for r in (low, high)], axis=0)
        for x in xs:
            total = total + x[:, EARLY:].astype(F32)
        inverse = lax.rsqrt(jnp.sum(total, axis=1, keepdims=True) / d_all + epsilon)
        x = jnp.concatenate([low[:, :EARLY], high[:, :EARLY]], axis=0)
        buf[:, :EARLY] = jnp.dot(pick_ref[...], x, preferred_element_type=F32).astype(BF16)
        first = copies.start(buf.at[:, pl.ds(0, EARLY)], out.at[:, pl.ds(number * EARLY, EARLY)])
        buf[:, EARLY:] = jnp.dot(pick_ref[...], side_columns(inverse), preferred_element_type=F32).astype(BF16)
        second = copies.start(buf.at[:, pl.ds(EARLY, SIDE)], out.at[:, pl.ds(partial.shape[1] - SIDE, SIDE)])
        first.wait()
        second.wait()

    vmem, hbm = pl.BlockSpec(memory_space=pltpu.VMEM), pl.BlockSpec(memory_space=pltpu.HBM)
    return pl.pallas_call(
        body,
        in_specs=[vmem] * (3 + len(others)) + [hbm],
        out_specs=hbm,
        out_shape=jax.ShapeDtypeStruct(partial.shape, BF16),
        scratch_shapes=[pltpu.VMEM((rows, EARLY + SIDE), BF16), pltpu.SemaphoreType.DMA((2,))],
        input_output_aliases={3 + len(others): 0},
        compiler_params=pltpu.CompilerParams(vmem_limit_bytes=16 * 2**20),
        name="early_rest",
    )(pick, *halves, *others, partial)


def local(tokens, norm_gain, expert_ids, gate_prob, w_gate, w_up, w_down):
    window, n_tp = lax.axis_size("ep"), lax.axis_size("tp")
    where = lax.axis_index("tp").astype(jnp.int32).reshape(1)
    w_gate, w_up, w_down = w_gate[0], w_up[0], w_down[0]
    tok = tokens.shape[0]
    rows = window * CAP
    up = [(i, (i + 1) % n_tp) for i in range(n_tp)]
    dn = [(i, (i - 1) % n_tp) for i in range(n_tp)]

    def spread(x):
        half = x.shape[0] // 2
        below, above = lax.ppermute(x, "tp", up), lax.ppermute(x, "tp", dn)
        return below, above, lax.ppermute(below[:half], "tp", up), lax.ppermute(above[half:], "tp", dn)

    def fold(own, above, below, far_a, far_b):
        half = own.shape[0] // 2
        got_a, got_b = lax.ppermute(far_a, "tp", up), lax.ppermute(far_b, "tp", dn)
        sum_up = (above.astype(F32) + jnp.pad(got_a.astype(F32), ((0, half), (0, 0)))).astype(BF16)
        sum_dn = (below.astype(F32) + jnp.pad(got_b.astype(F32), ((half, 0), (0, 0)))).astype(BF16)
        from_dn, from_up = lax.ppermute(sum_up, "tp", up), lax.ppermute(sum_dn, "tp", dn)
        return (own.astype(F32) + from_dn.astype(F32) + from_up.astype(F32)).astype(BF16)

    def spread_halves(low, high):
        below_low, above_high = lax.ppermute(low, "tp", up), lax.ppermute(high, "tp", dn)
        below_high, above_low = lax.ppermute(high, "tp", up), lax.ppermute(low, "tp", dn)
        far = lax.ppermute(below_low, "tp", up), lax.ppermute(above_high, "tp", dn)
        return (below_low, below_high), (above_low, above_high), far

    def add(*terms):
        return sum(t.astype(F32) for t in terms).astype(BF16)

    def fold_halves(own, above, below, far):
        got_low, got_high = lax.ppermute(far[0], "tp", up), lax.ppermute(far[1], "tp", dn)
        dn_high, up_low = lax.ppermute(above[1], "tp", up), lax.ppermute(below[0], "tp", dn)
        dn_low = lax.ppermute(add(above[0], got_low), "tp", up)
        up_high = lax.ppermute(add(below[1], got_high), "tp", dn)
        return join_sums((own[0], dn_low, up_low), (own[1], dn_high, up_high))

    def exchange(x):
        shaped = x.reshape(window, CAP, x.shape[1])
        return lax.all_to_all(shaped, "ep", 0, 0, tiled=True).reshape(rows, x.shape[1])

    bulk = tokens.shape[1] - EARLY
    half = rows // 2
    ids, probs = expert_ids.T, gate_prob.T.astype(F32)
    pick, picked_bulk, early = head(tokens, norm_gain, ids, window)
    same = ids[:, None, :] == jnp.arange(window, dtype=jnp.int32)[None, :, None]
    prob = jnp.sum(jnp.where(same, probs[:, None, :], 0.0), axis=0)
    by_slot = jnp.broadcast_to(prob[:, None, :], (window, CAP, tok)).reshape(rows, tok)
    weight = jnp.where(pick > 0, by_slot, 0.0).astype(BF16)

    e_below, e_above, e_far_a, e_far_b = spread(early)
    mine = exchange(picked_bulk)
    picked_near = early_near(pick, ((0, early), (1, e_above), (3, e_below)), n_tp)
    picked = early_rest(pick, 2, (e_far_a, e_far_b), (early, e_above, e_below), picked_near, D)
    early_rows = exchange(picked)
    below, above, far = spread_halves(mine[:half], mine[half:])

    weights = (w_gate, w_up, w_down)
    low, high = (0, half), (half, half)
    far_segs = [((0, 1), 2, EARLY, bulk, 0)]
    far_jobs = [
        (2, EARLY, bulk, 0, rows, ((0, 0, half, 0), (1, half, half, 0))),
        (1, EARLY, bulk, *high, ((2, 0, half, 0),)),
        (3, EARLY, bulk, *low, ((3, 0, half, 0),)),
    ]
    sums = expert_call(where, weights, [mine], [((0,), 0, EARLY, bulk, 0)])
    sums = expert_call(
        where, weights, [*above, *below],
        [((0, 1), 1, EARLY, bulk, 0), ((2, 3), 3, EARLY, bulk, 0)], sums,
    )
    early_jobs = [(k, 0, EARLY, 0, rows, ((0, 0, rows, k * EARLY),)) for k in range(n_tp)]
    gate_sum, up_sum, scale, *far_held = expert_call(
        where, weights, [early_rows], [((0,), k, 0, EARLY, k * EARLY) for k in range(n_tp)],
        stored=sums, keep=(0, n_tp * EARLY), stash=(far_segs, far_jobs),
    )
    hidden, f_low, f_high, a_high, b_low = expert_call(
        where, weights, [*far, scale], far_segs, (gate_sum, up_sum), inv=2,
        jobs=far_jobs, outs=[(half, bulk)] * 4, held=far_held,
    )
    (p_early,) = expert_call(where, weights, hidden=hidden, jobs=early_jobs, outs=[(rows, n_tp * EARLY)], leave=True)
    a_low, b_high, o_low, o_high = expert_call(
        where, weights, hidden=hidden,
        jobs=[
            (1, EARLY, bulk, *low, ((0, 0, half, 0),)),
            (3, EARLY, bulk, *high, ((1, 0, half, 0),)),
            (0, EARLY, bulk, 0, rows, ((2, 0, half, 0), (3, half, half, 0))),
        ],
        outs=[(half, bulk)] * 4,
    )

    def combine(back):
        return lax.dot_general(weight, back, (((0,), (0,)), ((), ())), preferred_element_type=F32).astype(BF16)

    early_back = combine(exchange(p_early))
    e = [early_back[:, k * EARLY : (k + 1) * EARLY] for k in range(n_tp)]
    out_early = fold(e[0], e[1], e[3], e[2][: tok // 2], e[2][tok // 2 :])
    folded = fold_halves((o_low, o_high), (a_low, a_high), (b_low, b_high), (f_low, f_high))
    out_bulk = combine(exchange(folded))
    return jnp.concatenate([out_early, out_bulk], axis=1)


def solution(mesh):
    placed = (
        P("ep", "tp"),
        P("tp"),
        P("ep", None),
        P("ep", None),
        P("ep", None, "tp"),
        P("ep", None, "tp"),
        P("ep", "tp", None),
    )

    return jax.shard_map(local, mesh=mesh, in_specs=placed, out_specs=P("ep", "tp"), check_vma=False)
```

```python
import jax
import jax.numpy as jnp
from jax import lax
from jax.experimental import pallas as pl
from jax.experimental.pallas import tpu as pltpu
from jax.sharding import PartitionSpec as P


D = 7168
epsilon = 1e-06
CAP = 16
EARLY = 512
SIDE = 128
F32, BF16 = jnp.float32, jnp.bfloat16


class Copies:
    def __init__(self, sems):
        self.sems, self.used = sems, 0

    def start(self, src, dst):
        copy = pltpu.make_async_copy(src, dst, self.sems.at[self.used])
        self.used += 1
        copy.start()
        return copy


def expert_call(where, weights, xs=(), segs=(), carry=(), inv=None, hidden=None, jobs=(), outs=(), stash=((), ()), held=(), stored=(), keep=None, leave=False):
    slices = lax.axis_size("tp")
    w_gate, w_up, w_down = weights
    d_all, ff = w_gate.shape
    span = d_all // slices
    finish = bool(segs) and bool(jobs)
    rows = hidden.shape[0] if hidden is not None else sum(xs[i].shape[0] for i in segs[0][0])

    def columns_of(some):
        found = []
        for step, offset, width, *_ in some:
            if (step, offset, width) not in found:
                found.append((step, offset, width))
        return found

    def weight_shapes(seg_list, column_list):
        shapes = []
        for _, _, _, width, _ in seg_list:
            shapes += [(width, ff)] * 2
        return shapes + [(ff, width) for _, _, width in column_list]

    columns, later = columns_of(jobs), columns_of(stash[1])
    results = [((rows, ff), F32)] * 2 if not jobs else [((rows, ff), BF16)] * finish + [(s, BF16) for s in outs]
    results = [(s, t) for s, t in results] + ([((rows, SIDE), BF16)] if keep else [])
    n_out = len(results)
    results += [(s, BF16) for s in weight_shapes(stash[0], later)]
    needed = weight_shapes(segs, columns)[len(held) :]
    streams = bool(needed) or len(results) > n_out
    resident = list(xs) + list(carry) + ([] if hidden is None else [hidden]) + list(held)
    streamed = ([w_gate, w_up, w_down] if streams else []) + list(stored)
    scratch = [pltpu.VMEM(s, BF16) for s in needed]
    if finish:
        scratch += [pltpu.VMEM((rows, ff), F32)] * 2
    scratch += [pltpu.VMEM((rows, ff), F32)] * len(stored)
    scratch += [pltpu.VMEM(s, BF16) for s in outs] * leave
    n_copies = len(jobs) * leave + len(stored) + len(needed) + len(results) - n_out
    scratch += [pltpu.SemaphoreType.DMA((max(n_copies, 1),))]

    def body(where_ref, *refs):
        refs = list(refs)
        take = lambda n: [refs.pop(0) for _ in range(n)]
        x_refs, carried = take(len(xs)), take(len(carry))
        hidden_ref = take(hidden is not None)
        held_refs = take(len(held))
        wg, wu, wd = take(3) if streams else (None,) * 3
        stored_refs = take(len(stored))
        out_refs = take(len(results))
        bufs = held_refs + take(len(needed))
        accs = take(2) if finish else out_refs[:2]
        stored_bufs = take(len(stored))
        staged = take(int(leave))
        copies = Copies(refs.pop(0))
        z = where_ref[0]

        def bring(seg_list, column_list, into, skip):
            waits, n = [None] * skip, 0
            for _, step, offset, width, _ in seg_list:
                at = pl.ds(pl.multiple_of(lax.rem(z + step, slices) * span + offset, 128), width)
                for w in (wg, wu):
                    if n >= skip:
                        waits.append(copies.start(w.at[at, :], into[n]))
                    n += 1
            for step, offset, width in column_list:
                at = pl.ds(pl.multiple_of(lax.rem(z + step, slices) * span + offset, 128), width)
                if n >= skip:
                    waits.append(copies.start(wd.at[:, at], into[n]))
                n += 1
            return waits

        def arrived(wait):
            if wait is not None:
                wait.wait()

        waits = bring(segs, columns, bufs, len(held))
        stored_waits = [copies.start(r, b) for r, b in zip(stored_refs, stored_bufs)]
        stash_waits = bring(stash[0], later, out_refs[n_out:], 0)
        if keep:
            out_refs[2][...] = x_refs[keep[0]][:, keep[1] : keep[1] + SIDE]
        for k, (index, _, _, width, col) in enumerate(segs):
            x = [x_refs[i][:, col : col + width] for i in index]
            x = x[0] if len(x) == 1 else jnp.concatenate(x, axis=0)
            for n, acc in enumerate(accs):
                arrived(waits[2 * k + n])
                term = jnp.dot(x, bufs[2 * k + n][...], preferred_element_type=F32)
                if k:
                    term = acc[...] + term
                elif carry:
                    term = carried[n][...] + term
                if stored and k == len(segs) - 1:
                    stored_waits[n].wait()
                    term = stored_bufs[n][...] + term
                acc[...] = term
        if finish:
            scale = jnp.sum(x_refs[inv][...].astype(F32), axis=1, keepdims=True)
            gate = accs[0][...] * scale
            hidden_ref = [out_refs.pop(0)]
            hidden_ref[0][...] = (jax.nn.silu(gate) * (accs[1][...] * scale)).astype(BF16)
        waited = set()
        for step, offset, width, row, count, targets in jobs:
            k = columns.index((step, offset, width))
            if k not in waited:
                arrived(waits[2 * len(segs) + k])
                waited.add(k)
            w = bufs[2 * len(segs) + k]
            term = jnp.dot(hidden_ref[0][row : row + count, :], w[...], preferred_element_type=F32).astype(BF16)
            for index, top, n, col in targets:
                to = staged[0] if leave else out_refs[index]
                to[:, col : col + width] = term[top : top + n, :]
                if leave:
                    at = pl.ds(col, width)
                    stash_waits.append(copies.start(to.at[:, at], out_refs[index].at[:, at]))
        for w in stash_waits:
            w.wait()

    vmem, hbm = pl.BlockSpec(memory_space=pltpu.VMEM), pl.BlockSpec(memory_space=pltpu.HBM)
    flops = sum(4 * rows * s[3] * ff for s in segs) + sum(2 * j[4] * ff * j[2] for j in jobs)
    return pl.pallas_call(
        body,
        in_specs=[pl.BlockSpec(memory_space=pltpu.SMEM)] + [vmem] * len(resident) + [hbm] * len(streamed),
        out_specs=[hbm if leave else vmem] * len(results),
        out_shape=[jax.ShapeDtypeStruct(s, t) if leave else pltpu.VMEM(s, t) for s, t in results],
        scratch_shapes=scratch,
        cost_estimate=pl.CostEstimate(flops=flops, bytes_accessed=flops // 256, transcendentals=0),
        compiler_params=pltpu.CompilerParams(vmem_limit_bytes=20 * 2**20),
    )(
        where,
        *[pltpu.with_memory_space_constraint(x, pltpu.VMEM) for x in resident],
        *[pltpu.with_memory_space_constraint(x, pltpu.HBM) for x in streamed],
    )


def side_columns(value):
    lane = lax.broadcasted_iota(jnp.int32, (value.shape[0], SIDE), 1)
    out = jnp.zeros((value.shape[0], SIDE), F32)
    for k in range(3):
        term = value.astype(BF16).astype(F32)
        out = jnp.where(lane == k, term, out)
        value = value - term
    return out.astype(BF16)


def head(tokens, norm_gain, ids, window):
    tok, width = tokens.shape
    rows, bulk = window * CAP, width - EARLY

    def body(ids_hbm, gain_hbm, tokens_hbm, pick_ref, bulk_ref, early_ref, ids_ref, gain_ref, tokens_ref, sems):
        copies = Copies(sems)
        pairs = ((ids_hbm, ids_ref), (gain_hbm, gain_ref), (tokens_hbm, tokens_ref))
        ids_load, gain_load, load = [copies.start(*pair) for pair in pairs]
        ids_load.wait()
        expert = lax.broadcasted_iota(jnp.int32, (window, tok), 0)
        match = jnp.zeros((window, tok), F32)
        for k in range(ids.shape[0]):
            match = match + jnp.where(ids_ref[k : k + 1, :] == expert, 1.0, 0.0)
        earlier = lax.broadcasted_iota(jnp.int32, (tok, tok), 0) < lax.broadcasted_iota(jnp.int32, (tok, tok), 1)
        earlier = jnp.where(earlier, 1.0, 0.0).astype(BF16)
        before = jnp.dot(match.astype(BF16), earlier, preferred_element_type=F32)
        slot = jnp.where(match > 0.0, before, -1.0)
        row = lax.broadcasted_iota(jnp.int32, (rows, window), 0)
        own = (row // CAP) == lax.broadcasted_iota(jnp.int32, (rows, window), 1)
        spread = jnp.dot(jnp.where(own, 1.0, 0.0).astype(BF16), slot.astype(BF16), preferred_element_type=F32)
        wanted = (lax.broadcasted_iota(jnp.int32, (rows, tok), 0) % CAP).astype(F32)
        pick = jnp.where(spread == wanted, 1.0, 0.0).astype(BF16)
        pick_ref[...] = pick
        gain_load.wait()
        gain = gain_ref[...].astype(F32).reshape(1, width)
        load.wait()
        values = tokens_ref[...].astype(F32)
        gained = (values * gain).astype(BF16)
        bulk_ref[...] = jnp.dot(pick, gained[:, EARLY:], preferred_element_type=F32).astype(BF16)
        early_ref[:, :EARLY] = gained[:, :EARLY]
        early_ref[:, EARLY:] = side_columns(jnp.sum(values * values, axis=1, keepdims=True))

    return pl.pallas_call(
        body,
        in_specs=[pl.BlockSpec(memory_space=pltpu.HBM)] * 3,
        scratch_shapes=[pltpu.VMEM(x.shape, x.dtype) for x in (ids, norm_gain, tokens)] + [pltpu.SemaphoreType.DMA((3,))],
        out_shape=[jax.ShapeDtypeStruct(s, BF16) for s in ((rows, tok), (rows, bulk), (tok, EARLY + SIDE))],
        cost_estimate=pl.CostEstimate(flops=2 * rows * tok * bulk, bytes_accessed=2 * tok * width, transcendentals=0),
        compiler_params=pltpu.CompilerParams(vmem_limit_bytes=24 * 2**20),
        name="head",
    )(*[pltpu.with_memory_space_constraint(x, pltpu.HBM) for x in (ids, norm_gain, tokens)])


def join_sums(low, high):
    half, width = low[0].shape

    def body(*refs):
        out = refs[-1]
        for k in (0, 1):
            a, b, c = (r[...].astype(F32) for r in refs[3 * k : 3 * k + 3])
            out[k * half : (k + 1) * half, :] = (a + b + c).astype(BF16)

    return pl.pallas_call(
        body,
        out_shape=jax.ShapeDtypeStruct((2 * half, width), BF16),
        cost_estimate=pl.CostEstimate(flops=6 * half * width, bytes_accessed=16 * half * width, transcendentals=0),
        compiler_params=pltpu.CompilerParams(vmem_limit_bytes=16 * 2**20),
        name="join_sums",
    )(*low, *high)


def early_near(pick, pieces, n_slices):
    rows = pick.shape[0]

    def body(pick_ref, *refs):
        xs, out, buf, sems = refs[: len(pieces)], refs[-3], refs[-2], refs[-1]
        copies = Copies(sems)
        waits = []
        for k, (number, _) in enumerate(pieces):
            buf[k] = jnp.dot(pick_ref[...], xs[k][:, :EARLY], preferred_element_type=F32).astype(BF16)
            waits.append(copies.start(buf.at[k], out.at[:, pl.ds(number * EARLY, EARLY)]))
        for w in waits:
            w.wait()

    return pl.pallas_call(
        body,
        out_specs=pl.BlockSpec(memory_space=pltpu.HBM),
        out_shape=jax.ShapeDtypeStruct((rows, n_slices * EARLY + SIDE), BF16),
        scratch_shapes=[pltpu.VMEM((len(pieces), rows, EARLY), BF16), pltpu.SemaphoreType.DMA((len(pieces),))],
        compiler_params=pltpu.CompilerParams(vmem_limit_bytes=16 * 2**20),
        name="early_near",
    )(pick, *[x for _, x in pieces])


def early_rest(pick, number, halves, others, partial, d_all):
    rows, _ = pick.shape

    def body(pick_ref, low, high, *refs):
        xs, (_, out, buf, sems) = refs[: len(others)], refs[len(others) :]
        copies = Copies(sems)
        total = jnp.concatenate([r[:, EARLY:].astype(F32) for r in (low, high)], axis=0)
        for x in xs:
            total = total + x[:, EARLY:].astype(F32)
        inverse = lax.rsqrt(jnp.sum(total, axis=1, keepdims=True) / d_all + epsilon)
        x = jnp.concatenate([low[:, :EARLY], high[:, :EARLY]], axis=0)
        buf[:, :EARLY] = jnp.dot(pick_ref[...], x, preferred_element_type=F32).astype(BF16)
        first = copies.start(buf.at[:, pl.ds(0, EARLY)], out.at[:, pl.ds(number * EARLY, EARLY)])
        buf[:, EARLY:] = jnp.dot(pick_ref[...], side_columns(inverse), preferred_element_type=F32).astype(BF16)
        second = copies.start(buf.at[:, pl.ds(EARLY, SIDE)], out.at[:, pl.ds(partial.shape[1] - SIDE, SIDE)])
        first.wait()
        second.wait()

    vmem, hbm = pl.BlockSpec(memory_space=pltpu.VMEM), pl.BlockSpec(memory_space=pltpu.HBM)
    return pl.pallas_call(
        body,
        in_specs=[vmem] * (3 + len(others)) + [hbm],
        out_specs=hbm,
        out_shape=jax.ShapeDtypeStruct(partial.shape, BF16),
        scratch_shapes=[pltpu.VMEM((rows, EARLY + SIDE), BF16), pltpu.SemaphoreType.DMA((2,))],
        input_output_aliases={3 + len(others): 0},
        compiler_params=pltpu.CompilerParams(vmem_limit_bytes=16 * 2**20),
        name="early_rest",
    )(pick, *halves, *others, partial)


def local(tokens, norm_gain, expert_ids, gate_prob, w_gate, w_up, w_down):
    window, n_tp = lax.axis_size("ep"), lax.axis_size("tp")
    where = lax.axis_index("tp").astype(jnp.int32).reshape(1)
    w_gate, w_up, w_down = w_gate[0], w_up[0], w_down[0]
    tok = tokens.shape[0]
    rows = window * CAP
    up = [(i, (i + 1) % n_tp) for i in range(n_tp)]
    dn = [(i, (i - 1) % n_tp) for i in range(n_tp)]

    def spread(x):
        half = x.shape[0] // 2
        below, above = lax.ppermute(x, "tp", up), lax.ppermute(x, "tp", dn)
        return below, above, lax.ppermute(below[:half], "tp", up), lax.ppermute(above[half:], "tp", dn)

    def fold(own, above, below, far_a, far_b):
        half = own.shape[0] // 2
        got_a, got_b = lax.ppermute(far_a, "tp", up), lax.ppermute(far_b, "tp", dn)
        sum_up = (above.astype(F32) + jnp.pad(got_a.astype(F32), ((0, half), (0, 0)))).astype(BF16)
        sum_dn = (below.astype(F32) + jnp.pad(got_b.astype(F32), ((half, 0), (0, 0)))).astype(BF16)
        from_dn, from_up = lax.ppermute(sum_up, "tp", up), lax.ppermute(sum_dn, "tp", dn)
        return (own.astype(F32) + from_dn.astype(F32) + from_up.astype(F32)).astype(BF16)

    def spread_halves(low, high):
        below_low, above_high = lax.ppermute(low, "tp", up), lax.ppermute(high, "tp", dn)
        below_high, above_low = lax.ppermute(high, "tp", up), lax.ppermute(low, "tp", dn)
        far = lax.ppermute(below_low, "tp", up), lax.ppermute(above_high, "tp", dn)
        return (below_low, below_high), (above_low, above_high), far

    def add(*terms):
        return sum(t.astype(F32) for t in terms).astype(BF16)

    def fold_halves(own, above, below, far):
        got_low, got_high = lax.ppermute(far[0], "tp", up), lax.ppermute(far[1], "tp", dn)
        dn_high, up_low = lax.ppermute(above[1], "tp", up), lax.ppermute(below[0], "tp", dn)
        dn_low = lax.ppermute(add(above[0], got_low), "tp", up)
        up_high = lax.ppermute(add(below[1], got_high), "tp", dn)
        return join_sums((own[0], dn_low, up_low), (own[1], dn_high, up_high))

    def exchange(x):
        shaped = x.reshape(window, CAP, x.shape[1])
        return lax.all_to_all(shaped, "ep", 0, 0, tiled=True).reshape(rows, x.shape[1])

    bulk = tokens.shape[1] - EARLY
    half = rows // 2
    ids, probs = expert_ids.T, gate_prob.T.astype(F32)
    pick, picked_bulk, early = head(tokens, norm_gain, ids, window)
    same = ids[:, None, :] == jnp.arange(window, dtype=jnp.int32)[None, :, None]
    prob = jnp.sum(jnp.where(same, probs[:, None, :], 0.0), axis=0)
    by_slot = jnp.broadcast_to(prob[:, None, :], (window, CAP, tok)).reshape(rows, tok)
    weight = jnp.where(pick > 0, by_slot, 0.0).astype(BF16)

    e_below, e_above, e_far_a, e_far_b = spread(early)
    mine = exchange(picked_bulk)
    picked_near = early_near(pick, ((0, early), (1, e_above), (3, e_below)), n_tp)
    picked = early_rest(pick, 2, (e_far_a, e_far_b), (early, e_above, e_below), picked_near, D)
    early_rows = exchange(picked)
    below, above, far = spread_halves(mine[:half], mine[half:])

    weights = (w_gate, w_up, w_down)
    low, high = (0, half), (half, half)
    far_segs = [((0, 1), 2, EARLY, bulk, 0)]
    far_jobs = [(2, EARLY, bulk, 0, rows, ((0, 0, half, 0), (1, half, half, 0)))]
    sums = expert_call(where, weights, [mine], [((0,), 0, EARLY, bulk, 0)])
    sums = expert_call(
        where, weights, [*above, *below],
        [((0, 1), 1, EARLY, bulk, 0), ((2, 3), 3, EARLY, bulk, 0)], sums,
    )
    early_jobs = [(k, 0, EARLY, 0, rows, ((0, 0, rows, k * EARLY),)) for k in range(n_tp)]
    gate_sum, up_sum, scale, *far_held = expert_call(
        where, weights, [early_rows], [((0,), k, 0, EARLY, k * EARLY) for k in range(n_tp)],
        stored=sums, keep=(0, n_tp * EARLY), stash=(far_segs, far_jobs),
    )
    hidden, f_low, f_high = expert_call(
        where, weights, [*far, scale], far_segs, (gate_sum, up_sum), inv=2,
        jobs=far_jobs, outs=[(half, bulk)] * 2, held=far_held,
    )
    (p_early,) = expert_call(where, weights, hidden=hidden, jobs=early_jobs, outs=[(rows, n_tp * EARLY)], leave=True)
    a_high, b_low = expert_call(
        where, weights, hidden=hidden,
        jobs=[(1, EARLY, bulk, *high, ((0, 0, half, 0),)), (3, EARLY, bulk, *low, ((1, 0, half, 0),))],
        outs=[(half, bulk)] * 2,
    )
    a_low, b_high, o_low, o_high = expert_call(
        where, weights, hidden=hidden,
        jobs=[
            (1, EARLY, bulk, *low, ((0, 0, half, 0),)),
            (3, EARLY, bulk, *high, ((1, 0, half, 0),)),
            (0, EARLY, bulk, 0, rows, ((2, 0, half, 0), (3, half, half, 0))),
        ],
        outs=[(half, bulk)] * 4,
    )

    def combine(back):
        return lax.dot_general(weight, back, (((0,), (0,)), ((), ())), preferred_element_type=F32).astype(BF16)

    early_back = combine(exchange(p_early))
    e = [early_back[:, k * EARLY : (k + 1) * EARLY] for k in range(n_tp)]
    out_early = fold(e[0], e[1], e[3], e[2][: tok // 2], e[2][tok // 2 :])
    folded = fold_halves((o_low, o_high), (a_low, a_high), (b_low, b_high), (f_low, f_high))
    out_bulk = combine(exchange(folded))
    return jnp.concatenate([out_early, out_bulk], axis=1)


def solution(mesh):
    placed = (
        P("ep", "tp"),
        P("tp"),
        P("ep", None),
        P("ep", None),
        P("ep", None, "tp"),
        P("ep", None, "tp"),
        P("ep", "tp", None),
    )

    return jax.shard_map(local, mesh=mesh, in_specs=placed, out_specs=P("ep", "tp"), check_vma=False)
```

```python
import jax
import jax.numpy as jnp
from jax import lax
from jax.experimental import pallas as pl
from jax.experimental.pallas import tpu as pltpu
from jax.sharding import PartitionSpec as P


D = 7168
epsilon = 1e-06
CAP = 16
EARLY = 512
SIDE = 128
F32, BF16 = jnp.float32, jnp.bfloat16


class Copies:
    def __init__(self, sems):
        self.sems, self.used = sems, 0

    def start(self, src, dst):
        copy = pltpu.make_async_copy(src, dst, self.sems.at[self.used])
        self.used += 1
        copy.start()
        return copy


def expert_call(where, weights, xs=(), segs=(), carry=(), inv=None, hidden=None, jobs=(), outs=(), stash=((), ()), held=(), stored=(), keep=None, leave=False):
    slices = lax.axis_size("tp")
    w_gate, w_up, w_down = weights
    d_all, ff = w_gate.shape
    span = d_all // slices
    finish = bool(segs) and bool(jobs)
    rows = hidden.shape[0] if hidden is not None else sum(xs[i].shape[0] for i in segs[0][0])

    def columns_of(some):
        found = []
        for step, offset, width, *_ in some:
            if (step, offset, width) not in found:
                found.append((step, offset, width))
        return found

    def weight_shapes(seg_list, column_list):
        shapes = []
        for _, _, _, width, _ in seg_list:
            shapes += [(width, ff)] * 2
        return shapes + [(ff, width) for _, _, width in column_list]

    columns, later = columns_of(jobs), columns_of(stash[1])
    results = [((rows, ff), F32)] * 2 if not jobs else [((rows, ff), BF16)] * finish + [(s, BF16) for s in outs]
    results = [(s, t) for s, t in results] + ([((rows, SIDE), BF16)] if keep else [])
    n_out = len(results)
    results += [(s, BF16) for s in weight_shapes(stash[0], later)]
    needed = weight_shapes(segs, columns)[len(held) :]
    streams = bool(needed) or len(results) > n_out
    resident = list(xs) + list(carry) + ([] if hidden is None else [hidden]) + list(held)
    streamed = ([w_gate, w_up, w_down] if streams else []) + list(stored)
    scratch = [pltpu.VMEM(s, BF16) for s in needed]
    if finish:
        scratch += [pltpu.VMEM((rows, ff), F32)] * 2
    scratch += [pltpu.VMEM((rows, ff), F32)] * len(stored)
    scratch += [pltpu.VMEM(s, BF16) for s in outs] * leave
    n_copies = len(jobs) * leave + len(stored) + len(needed) + len(results) - n_out
    scratch += [pltpu.SemaphoreType.DMA((max(n_copies, 1),))]

    def body(where_ref, *refs):
        refs = list(refs)
        take = lambda n: [refs.pop(0) for _ in range(n)]
        x_refs, carried = take(len(xs)), take(len(carry))
        hidden_ref = take(hidden is not None)
        held_refs = take(len(held))
        wg, wu, wd = take(3) if streams else (None,) * 3
        stored_refs = take(len(stored))
        out_refs = take(len(results))
        bufs = held_refs + take(len(needed))
        accs = take(2) if finish else out_refs[:2]
        stored_bufs = take(len(stored))
        staged = take(int(leave))
        copies = Copies(refs.pop(0))
        z = where_ref[0]

        def bring(seg_list, column_list, into, skip):
            waits, n = [None] * skip, 0
            for _, step, offset, width, _ in seg_list:
                at = pl.ds(pl.multiple_of(lax.rem(z + step, slices) * span + offset, 128), width)
                for w in (wg, wu):
                    if n >= skip:
                        waits.append(copies.start(w.at[at, :], into[n]))
                    n += 1
            for step, offset, width in column_list:
                at = pl.ds(pl.multiple_of(lax.rem(z + step, slices) * span + offset, 128), width)
                if n >= skip:
                    waits.append(copies.start(wd.at[:, at], into[n]))
                n += 1
            return waits

        def arrived(wait):
            if wait is not None:
                wait.wait()

        waits = bring(segs, columns, bufs, len(held))
        stored_waits = [copies.start(r, b) for r, b in zip(stored_refs, stored_bufs)]
        stash_waits = bring(stash[0], later, out_refs[n_out:], 0)
        if keep:
            out_refs[2][...] = x_refs[keep[0]][:, keep[1] : keep[1] + SIDE]
        for k, (index, _, _, width, col) in enumerate(segs):
            x = [x_refs[i][:, col : col + width] for i in index]
            x = x[0] if len(x) == 1 else jnp.concatenate(x, axis=0)
            for n, acc in enumerate(accs):
                arrived(waits[2 * k + n])
                term = jnp.dot(x, bufs[2 * k + n][...], preferred_element_type=F32)
                if k:
                    term = acc[...] + term
                elif carry:
                    term = carried[n][...] + term
                if stored and k == len(segs) - 1:
                    stored_waits[n].wait()
                    term = stored_bufs[n][...] + term
                acc[...] = term
        if finish:
            scale = jnp.sum(x_refs[inv][...].astype(F32), axis=1, keepdims=True)
            gate = accs[0][...] * scale
            hidden_ref = [out_refs.pop(0)]
            hidden_ref[0][...] = (jax.nn.silu(gate) * (accs[1][...] * scale)).astype(BF16)
        waited = set()
        for step, offset, width, row, count, targets in jobs:
            k = columns.index((step, offset, width))
            if k not in waited:
                arrived(waits[2 * len(segs) + k])
                waited.add(k)
            w = bufs[2 * len(segs) + k]
            term = jnp.dot(hidden_ref[0][row : row + count, :], w[...], preferred_element_type=F32).astype(BF16)
            for index, top, n, col in targets:
                to = staged[0] if leave else out_refs[index]
                to[:, col : col + width] = term[top : top + n, :]
                if leave:
                    at = pl.ds(col, width)
                    stash_waits.append(copies.start(to.at[:, at], out_refs[index].at[:, at]))
        for w in stash_waits:
            w.wait()

    vmem, hbm = pl.BlockSpec(memory_space=pltpu.VMEM), pl.BlockSpec(memory_space=pltpu.HBM)
    flops = sum(4 * rows * s[3] * ff for s in segs) + sum(2 * j[4] * ff * j[2] for j in jobs)
    return pl.pallas_call(
        body,
        in_specs=[pl.BlockSpec(memory_space=pltpu.SMEM)] + [vmem] * len(resident) + [hbm] * len(streamed),
        out_specs=[hbm if leave else vmem] * len(results),
        out_shape=[jax.ShapeDtypeStruct(s, t) if leave else pltpu.VMEM(s, t) for s, t in results],
        scratch_shapes=scratch,
        cost_estimate=pl.CostEstimate(flops=flops, bytes_accessed=flops // 256, transcendentals=0),
        compiler_params=pltpu.CompilerParams(vmem_limit_bytes=20 * 2**20),
    )(
        where,
        *[pltpu.with_memory_space_constraint(x, pltpu.VMEM) for x in resident],
        *[pltpu.with_memory_space_constraint(x, pltpu.HBM) for x in streamed],
    )


def side_columns(value):
    lane = lax.broadcasted_iota(jnp.int32, (value.shape[0], SIDE), 1)
    out = jnp.zeros((value.shape[0], SIDE), F32)
    for k in range(3):
        term = value.astype(BF16).astype(F32)
        out = jnp.where(lane == k, term, out)
        value = value - term
    return out.astype(BF16)


def head(tokens, norm_gain, ids, window):
    tok, width = tokens.shape
    rows, bulk = window * CAP, width - EARLY

    def body(ids_hbm, gain_hbm, tokens_hbm, pick_ref, bulk_ref, early_ref, ids_ref, gain_ref, tokens_ref, sems):
        copies = Copies(sems)
        pairs = ((ids_hbm, ids_ref), (gain_hbm, gain_ref), (tokens_hbm, tokens_ref))
        ids_load, gain_load, load = [copies.start(*pair) for pair in pairs]
        ids_load.wait()
        expert = lax.broadcasted_iota(jnp.int32, (window, tok), 0)
        match = jnp.zeros((window, tok), F32)
        for k in range(ids.shape[0]):
            match = match + jnp.where(ids_ref[k : k + 1, :] == expert, 1.0, 0.0)
        earlier = lax.broadcasted_iota(jnp.int32, (tok, tok), 0) < lax.broadcasted_iota(jnp.int32, (tok, tok), 1)
        earlier = jnp.where(earlier, 1.0, 0.0).astype(BF16)
        before = jnp.dot(match.astype(BF16), earlier, preferred_element_type=F32)
        slot = jnp.where(match > 0.0, before, -1.0)
        row = lax.broadcasted_iota(jnp.int32, (rows, window), 0)
        own = (row // CAP) == lax.broadcasted_iota(jnp.int32, (rows, window), 1)
        spread = jnp.dot(jnp.where(own, 1.0, 0.0).astype(BF16), slot.astype(BF16), preferred_element_type=F32)
        wanted = (lax.broadcasted_iota(jnp.int32, (rows, tok), 0) % CAP).astype(F32)
        pick = jnp.where(spread == wanted, 1.0, 0.0).astype(BF16)
        pick_ref[...] = pick
        gain_load.wait()
        gain = gain_ref[...].astype(F32).reshape(1, width)
        load.wait()
        values = tokens_ref[...].astype(F32)
        gained = (values * gain).astype(BF16)
        bulk_ref[...] = jnp.dot(pick, gained[:, EARLY:], preferred_element_type=F32).astype(BF16)
        early_ref[:, :EARLY] = gained[:, :EARLY]
        early_ref[:, EARLY:] = side_columns(jnp.sum(values * values, axis=1, keepdims=True))

    return pl.pallas_call(
        body,
        in_specs=[pl.BlockSpec(memory_space=pltpu.HBM)] * 3,
        scratch_shapes=[pltpu.VMEM(x.shape, x.dtype) for x in (ids, norm_gain, tokens)] + [pltpu.SemaphoreType.DMA((3,))],
        out_shape=[jax.ShapeDtypeStruct(s, BF16) for s in ((rows, tok), (rows, bulk), (tok, EARLY + SIDE))],
        cost_estimate=pl.CostEstimate(flops=2 * rows * tok * bulk, bytes_accessed=2 * tok * width, transcendentals=0),
        compiler_params=pltpu.CompilerParams(vmem_limit_bytes=24 * 2**20),
        name="head",
    )(*[pltpu.with_memory_space_constraint(x, pltpu.HBM) for x in (ids, norm_gain, tokens)])


def join_sums(low, high):
    cut, width = low[0].shape
    rows = cut + high[0].shape[0]

    def body(*refs):
        out = refs[-1]
        for k, at in ((0, slice(0, cut)), (1, slice(cut, rows))):
            a, b, c = (r[...].astype(F32) for r in refs[3 * k : 3 * k + 3])
            out[at, :] = (a + b + c).astype(BF16)

    return pl.pallas_call(
        body,
        out_shape=jax.ShapeDtypeStruct((rows, width), BF16),
        cost_estimate=pl.CostEstimate(flops=3 * rows * width, bytes_accessed=8 * rows * width, transcendentals=0),
        compiler_params=pltpu.CompilerParams(vmem_limit_bytes=16 * 2**20),
        name="join_sums",
    )(*low, *high)


def early_near(pick, pieces, n_slices):
    rows = pick.shape[0]

    def body(pick_ref, *refs):
        xs, out, buf, sems = refs[: len(pieces)], refs[-3], refs[-2], refs[-1]
        copies = Copies(sems)
        waits = []
        for k, (number, _) in enumerate(pieces):
            buf[k] = jnp.dot(pick_ref[...], xs[k][:, :EARLY], preferred_element_type=F32).astype(BF16)
            waits.append(copies.start(buf.at[k], out.at[:, pl.ds(number * EARLY, EARLY)]))
        for w in waits:
            w.wait()

    return pl.pallas_call(
        body,
        out_specs=pl.BlockSpec(memory_space=pltpu.HBM),
        out_shape=jax.ShapeDtypeStruct((rows, n_slices * EARLY + SIDE), BF16),
        scratch_shapes=[pltpu.VMEM((len(pieces), rows, EARLY), BF16), pltpu.SemaphoreType.DMA((len(pieces),))],
        compiler_params=pltpu.CompilerParams(vmem_limit_bytes=16 * 2**20),
        name="early_near",
    )(pick, *[x for _, x in pieces])


def early_rest(pick, number, halves, others, partial, d_all):
    rows, _ = pick.shape

    def body(pick_ref, low, high, *refs):
        xs, (_, out, buf, sems) = refs[: len(others)], refs[len(others) :]
        copies = Copies(sems)
        total = jnp.concatenate([r[:, EARLY:].astype(F32) for r in (low, high)], axis=0)
        for x in xs:
            total = total + x[:, EARLY:].astype(F32)
        inverse = lax.rsqrt(jnp.sum(total, axis=1, keepdims=True) / d_all + epsilon)
        x = jnp.concatenate([low[:, :EARLY], high[:, :EARLY]], axis=0)
        buf[:, :EARLY] = jnp.dot(pick_ref[...], x, preferred_element_type=F32).astype(BF16)
        first = copies.start(buf.at[:, pl.ds(0, EARLY)], out.at[:, pl.ds(number * EARLY, EARLY)])
        buf[:, EARLY:] = jnp.dot(pick_ref[...], side_columns(inverse), preferred_element_type=F32).astype(BF16)
        second = copies.start(buf.at[:, pl.ds(EARLY, SIDE)], out.at[:, pl.ds(partial.shape[1] - SIDE, SIDE)])
        first.wait()
        second.wait()

    vmem, hbm = pl.BlockSpec(memory_space=pltpu.VMEM), pl.BlockSpec(memory_space=pltpu.HBM)
    return pl.pallas_call(
        body,
        in_specs=[vmem] * (3 + len(others)) + [hbm],
        out_specs=hbm,
        out_shape=jax.ShapeDtypeStruct(partial.shape, BF16),
        scratch_shapes=[pltpu.VMEM((rows, EARLY + SIDE), BF16), pltpu.SemaphoreType.DMA((2,))],
        input_output_aliases={3 + len(others): 0},
        compiler_params=pltpu.CompilerParams(vmem_limit_bytes=16 * 2**20),
        name="early_rest",
    )(pick, *halves, *others, partial)


def local(tokens, norm_gain, expert_ids, gate_prob, w_gate, w_up, w_down):
    window, n_tp = lax.axis_size("ep"), lax.axis_size("tp")
    where = lax.axis_index("tp").astype(jnp.int32).reshape(1)
    w_gate, w_up, w_down = w_gate[0], w_up[0], w_down[0]
    tok = tokens.shape[0]
    rows = window * CAP
    up = [(i, (i + 1) % n_tp) for i in range(n_tp)]
    dn = [(i, (i - 1) % n_tp) for i in range(n_tp)]

    def send_up(x):
        return lax.ppermute(x, "tp", up)

    def send_dn(x):
        return lax.ppermute(x, "tp", dn)

    def spread(x):
        half = x.shape[0] // 2
        below, above = send_up(x), send_dn(x)
        return below, above, send_up(below[:half]), send_dn(above[half:])

    def fold(own, above, below, far_a, far_b):
        half = own.shape[0] // 2
        got_a, got_b = send_up(far_a), send_dn(far_b)
        sum_up = (above.astype(F32) + jnp.pad(got_a.astype(F32), ((0, half), (0, 0)))).astype(BF16)
        sum_dn = (below.astype(F32) + jnp.pad(got_b.astype(F32), ((half, 0), (0, 0)))).astype(BF16)
        from_dn, from_up = send_up(sum_up), send_dn(sum_dn)
        return (own.astype(F32) + from_dn.astype(F32) + from_up.astype(F32)).astype(BF16)

    def spread_halves(low, high):
        below_low, above_high = send_up(low), send_dn(high)
        below_high, above_low = send_up(high), send_dn(low)
        far = send_up(below_low), send_dn(above_high)
        return (below_low, below_high), (above_low, above_high), far

    def add(*terms):
        return sum(t.astype(F32) for t in terms).astype(BF16)

    def fold_halves(own, above, below, far):
        got_low, got_high = send_up(far[0]), send_dn(far[1])
        dn_high, up_low = send_up(above[1]), send_dn(below[0])
        dn_low = send_up(add(above[0], got_low))
        up_high = send_dn(add(below[1], got_high))
        return join_sums((own[0], dn_low, up_low), (own[1], dn_high, up_high))

    def exchange(x):
        shaped = x.reshape(window, CAP, x.shape[1])
        return lax.all_to_all(shaped, "ep", 0, 0, tiled=True).reshape(rows, x.shape[1])

    bulk = tokens.shape[1] - EARLY
    cut = rows // 2 + CAP
    ids, probs = expert_ids.T, gate_prob.T.astype(F32)
    pick, picked_bulk, early = head(tokens, norm_gain, ids, window)
    same = ids[:, None, :] == jnp.arange(window, dtype=jnp.int32)[None, :, None]
    prob = jnp.sum(jnp.where(same, probs[:, None, :], 0.0), axis=0)
    by_slot = jnp.broadcast_to(prob[:, None, :], (window, CAP, tok)).reshape(rows, tok)
    weight = jnp.where(pick > 0, by_slot, 0.0).astype(BF16)

    e_below, e_above, e_far_a, e_far_b = spread(early)
    mine = exchange(picked_bulk)
    picked_near = early_near(pick, ((0, early), (1, e_above), (3, e_below)), n_tp)
    picked = early_rest(pick, 2, (e_far_a, e_far_b), (early, e_above, e_below), picked_near, D)
    early_rows = exchange(picked)
    below, above, far = spread_halves(mine[:cut], mine[cut:])

    weights = (w_gate, w_up, w_down)
    low, high = (0, cut), (cut, rows - cut)
    far_segs = [((0, 1), 2, EARLY, bulk, 0)]
    far_jobs = [
        (2, EARLY, bulk, 0, rows, ((0, *low, 0), (1, *high, 0))),
        (1, EARLY, bulk, *high, ((2, 0, rows - cut, 0),)),
        (3, EARLY, bulk, *low, ((3, 0, cut, 0),)),
    ]
    sums = expert_call(where, weights, [mine], [((0,), 0, EARLY, bulk, 0)])
    sums = expert_call(
        where, weights, [*above, *below],
        [((0, 1), 1, EARLY, bulk, 0), ((2, 3), 3, EARLY, bulk, 0)], sums,
    )
    early_jobs = [(k, 0, EARLY, 0, rows, ((0, 0, rows, k * EARLY),)) for k in range(n_tp)]
    gate_sum, up_sum, scale, *far_held = expert_call(
        where, weights, [early_rows], [((0,), k, 0, EARLY, k * EARLY) for k in range(n_tp)],
        stored=sums, keep=(0, n_tp * EARLY), stash=(far_segs, far_jobs),
    )
    hidden, f_low, f_high, a_high, b_low = expert_call(
        where, weights, [*far, scale], far_segs, (gate_sum, up_sum), inv=2,
        jobs=far_jobs, outs=[(cut, bulk), (rows - cut, bulk), (rows - cut, bulk), (cut, bulk)], held=far_held,
    )
    (p_early,) = expert_call(where, weights, hidden=hidden, jobs=early_jobs, outs=[(rows, n_tp * EARLY)], leave=True)
    a_low, b_high, o_low, o_high = expert_call(
        where, weights, hidden=hidden,
        jobs=[
            (1, EARLY, bulk, *low, ((0, 0, cut, 0),)),
            (3, EARLY, bulk, *high, ((1, 0, rows - cut, 0),)),
            (0, EARLY, bulk, 0, rows, ((2, *low, 0), (3, *high, 0))),
        ],
        outs=[(cut, bulk), (rows - cut, bulk)] * 2,
    )

    def combine(back):
        return lax.dot_general(weight, back, (((0,), (0,)), ((), ())), preferred_element_type=F32).astype(BF16)

    early_back = combine(exchange(p_early))
    e = [early_back[:, k * EARLY : (k + 1) * EARLY] for k in range(n_tp)]
    out_early = fold(e[0], e[1], e[3], e[2][: tok // 2], e[2][tok // 2 :])
    folded = fold_halves((o_low, o_high), (a_low, a_high), (b_low, b_high), (f_low, f_high))
    out_bulk = combine(exchange(folded))
    return jnp.concatenate([out_early, out_bulk], axis=1)


def solution(mesh):
    placed = (
        P("ep", "tp"),
        P("tp"),
        P("ep", None),
        P("ep", None),
        P("ep", None, "tp"),
        P("ep", None, "tp"),
        P("ep", "tp", None),
    )

    return jax.shard_map(local, mesh=mesh, in_specs=placed, out_specs=P("ep", "tp"), check_vma=False)
```

```python
import jax
import jax.numpy as jnp
from jax import lax
from jax.experimental import pallas as pl
from jax.experimental.pallas import tpu as pltpu
from jax.sharding import PartitionSpec as P


D = 7168
epsilon = 1e-06
CAP = 16
EARLY = 512
SIDE = 128
F32, BF16 = jnp.float32, jnp.bfloat16


class Copies:
    def __init__(self, sems):
        self.sems, self.used = sems, 0

    def start(self, src, dst):
        copy = pltpu.make_async_copy(src, dst, self.sems.at[self.used])
        self.used += 1
        copy.start()
        return copy


def expert_call(where, weights, xs=(), segs=(), carry=(), inv=None, hidden=None, jobs=(), outs=(), stash=((), ()), held=(), stored=(), keep=None, leave=False):
    slices = lax.axis_size("tp")
    w_gate, w_up, w_down = weights
    d_all, ff = w_gate.shape
    span = d_all // slices
    finish = bool(segs) and bool(jobs)
    rows = hidden.shape[0] if hidden is not None else sum(xs[i].shape[0] for i in segs[0][0])

    def columns_of(some):
        found = []
        for step, offset, width, *_ in some:
            if (step, offset, width) not in found:
                found.append((step, offset, width))
        return found

    def weight_shapes(seg_list, column_list):
        shapes = []
        for _, _, _, width, _ in seg_list:
            shapes += [(width, ff)] * 2
        return shapes + [(ff, width) for _, _, width in column_list]

    columns, later = columns_of(jobs), columns_of(stash[1])
    results = [((rows, ff), F32)] * 2 if not jobs else [((rows, ff), BF16)] * finish + [(s, BF16) for s in outs]
    results = [(s, t) for s, t in results] + ([((rows, SIDE), BF16)] if keep else [])
    n_out = len(results)
    results += [(s, BF16) for s in weight_shapes(stash[0], later)]
    needed = weight_shapes(segs, columns)[len(held) :]
    streams = bool(needed) or len(results) > n_out
    resident = list(xs) + list(carry) + ([] if hidden is None else [hidden]) + list(held)
    streamed = ([w_gate, w_up, w_down] if streams else []) + list(stored)
    scratch = [pltpu.VMEM(s, BF16) for s in needed]
    if finish:
        scratch += [pltpu.VMEM((rows, ff), F32)] * 2
    scratch += [pltpu.VMEM((rows, ff), F32)] * len(stored)
    scratch += ([pltpu.VMEM(s, BF16) for s in outs] or [pltpu.VMEM((rows, ff), F32)] * 2) * leave
    n_copies = (len(jobs) or 2) * leave + len(stored) + len(needed) + len(results) - n_out
    scratch += [pltpu.SemaphoreType.DMA((max(n_copies, 1),))]

    def body(where_ref, *refs):
        refs = list(refs)
        take = lambda n: [refs.pop(0) for _ in range(n)]
        x_refs, carried = take(len(xs)), take(len(carry))
        hidden_ref = take(hidden is not None)
        held_refs = take(len(held))
        wg, wu, wd = take(3) if streams else (None,) * 3
        stored_refs = take(len(stored))
        out_refs = take(len(results))
        bufs = held_refs + take(len(needed))
        accs = take(2) if finish else out_refs[:2]
        stored_bufs = take(len(stored))
        staged = take(leave * (len(outs) or 2))
        accs = staged if leave and not jobs else accs
        copies = Copies(refs.pop(0))
        z = where_ref[0]

        def bring(seg_list, column_list, into, skip):
            waits, n = [None] * skip, 0
            for _, step, offset, width, _ in seg_list:
                at = pl.ds(pl.multiple_of(lax.rem(z + step, slices) * span + offset, 128), width)
                for w in (wg, wu):
                    if n >= skip:
                        waits.append(copies.start(w.at[at, :], into[n]))
                    n += 1
            for step, offset, width in column_list:
                at = pl.ds(pl.multiple_of(lax.rem(z + step, slices) * span + offset, 128), width)
                if n >= skip:
                    waits.append(copies.start(wd.at[:, at], into[n]))
                n += 1
            return waits

        def arrived(wait):
            if wait is not None:
                wait.wait()

        waits = bring(segs, columns, bufs, len(held))
        stored_waits = [copies.start(r, b) for r, b in zip(stored_refs, stored_bufs)]
        stash_waits = bring(stash[0], later, out_refs[n_out:], 0)
        if keep:
            out_refs[2][...] = x_refs[keep[0]][:, keep[1] : keep[1] + SIDE]
        for k, (index, _, _, width, col) in enumerate(segs):
            x = [x_refs[i][:, col : col + width] for i in index]
            x = x[0] if len(x) == 1 else jnp.concatenate(x, axis=0)
            for n, acc in enumerate(accs):
                arrived(waits[2 * k + n])
                term = jnp.dot(x, bufs[2 * k + n][...], preferred_element_type=F32)
                if k:
                    term = acc[...] + term
                elif carry:
                    term = carried[n][...] + term
                if stored and k == len(segs) - 1:
                    stored_waits[n].wait()
                    term = stored_bufs[n][...] + term
                acc[...] = term
                if leave and not jobs and k == len(segs) - 1:
                    stash_waits.append(copies.start(acc, out_refs[n]))
        if finish:
            scale = jnp.sum(x_refs[inv][...].astype(F32), axis=1, keepdims=True)
            gate = accs[0][...] * scale
            hidden_ref = [out_refs.pop(0)]
            hidden_ref[0][...] = (jax.nn.silu(gate) * (accs[1][...] * scale)).astype(BF16)
        waited = set()
        for step, offset, width, row, count, targets in jobs:
            k = columns.index((step, offset, width))
            if k not in waited:
                arrived(waits[2 * len(segs) + k])
                waited.add(k)
            w = bufs[2 * len(segs) + k]
            term = jnp.dot(hidden_ref[0][row : row + count, :], w[...], preferred_element_type=F32).astype(BF16)
            for index, top, n, col in targets:
                to = staged[0] if leave else out_refs[index]
                to[:, col : col + width] = term[top : top + n, :]
                if leave:
                    at = pl.ds(col, width)
                    stash_waits.append(copies.start(to.at[:, at], out_refs[index].at[:, at]))
        for w in stash_waits:
            w.wait()

    vmem, hbm = pl.BlockSpec(memory_space=pltpu.VMEM), pl.BlockSpec(memory_space=pltpu.HBM)
    flops = sum(4 * rows * s[3] * ff for s in segs) + sum(2 * j[4] * ff * j[2] for j in jobs)
    return pl.pallas_call(
        body,
        in_specs=[pl.BlockSpec(memory_space=pltpu.SMEM)] + [vmem] * len(resident) + [hbm] * len(streamed),
        out_specs=[hbm if leave else vmem] * len(results),
        out_shape=[jax.ShapeDtypeStruct(s, t) if leave else pltpu.VMEM(s, t) for s, t in results],
        scratch_shapes=scratch,
        cost_estimate=pl.CostEstimate(flops=flops, bytes_accessed=flops // 256, transcendentals=0),
        compiler_params=pltpu.CompilerParams(vmem_limit_bytes=20 * 2**20),
    )(
        where,
        *[pltpu.with_memory_space_constraint(x, pltpu.VMEM) for x in resident],
        *[pltpu.with_memory_space_constraint(x, pltpu.HBM) for x in streamed],
    )


def side_columns(value):
    lane = lax.broadcasted_iota(jnp.int32, (value.shape[0], SIDE), 1)
    out = jnp.zeros((value.shape[0], SIDE), F32)
    for k in range(3):
        term = value.astype(BF16).astype(F32)
        out = jnp.where(lane == k, term, out)
        value = value - term
    return out.astype(BF16)


def head(tokens, norm_gain, ids, window):
    tok, width = tokens.shape
    rows, bulk = window * CAP, width - EARLY

    def body(ids_hbm, gain_hbm, tokens_hbm, pick_ref, bulk_ref, early_ref, ids_ref, gain_ref, tokens_ref, sems):
        copies = Copies(sems)
        pairs = ((ids_hbm, ids_ref), (gain_hbm, gain_ref), (tokens_hbm, tokens_ref))
        ids_load, gain_load, load = [copies.start(*pair) for pair in pairs]
        ids_load.wait()
        expert = lax.broadcasted_iota(jnp.int32, (window, tok), 0)
        match = jnp.zeros((window, tok), F32)
        for k in range(ids.shape[0]):
            match = match + jnp.where(ids_ref[k : k + 1, :] == expert, 1.0, 0.0)
        earlier = lax.broadcasted_iota(jnp.int32, (tok, tok), 0) < lax.broadcasted_iota(jnp.int32, (tok, tok), 1)
        earlier = jnp.where(earlier, 1.0, 0.0).astype(BF16)
        before = jnp.dot(match.astype(BF16), earlier, preferred_element_type=F32)
        slot = jnp.where(match > 0.0, before, -1.0)
        row = lax.broadcasted_iota(jnp.int32, (rows, window), 0)
        own = (row // CAP) == lax.broadcasted_iota(jnp.int32, (rows, window), 1)
        spread = jnp.dot(jnp.where(own, 1.0, 0.0).astype(BF16), slot.astype(BF16), preferred_element_type=F32)
        wanted = (lax.broadcasted_iota(jnp.int32, (rows, tok), 0) % CAP).astype(F32)
        pick = jnp.where(spread == wanted, 1.0, 0.0).astype(BF16)
        pick_ref[...] = pick
        gain_load.wait()
        gain = gain_ref[...].astype(F32).reshape(1, width)
        load.wait()
        values = tokens_ref[...].astype(F32)
        gained = (values * gain).astype(BF16)
        bulk_ref[...] = jnp.dot(pick, gained[:, EARLY:], preferred_element_type=F32).astype(BF16)
        early_ref[:, :EARLY] = gained[:, :EARLY]
        early_ref[:, EARLY:] = side_columns(jnp.sum(values * values, axis=1, keepdims=True))

    return pl.pallas_call(
        body,
        in_specs=[pl.BlockSpec(memory_space=pltpu.HBM)] * 3,
        scratch_shapes=[pltpu.VMEM(x.shape, x.dtype) for x in (ids, norm_gain, tokens)] + [pltpu.SemaphoreType.DMA((3,))],
        out_shape=[jax.ShapeDtypeStruct(s, BF16) for s in ((rows, tok), (rows, bulk), (tok, EARLY + SIDE))],
        cost_estimate=pl.CostEstimate(flops=2 * rows * tok * bulk, bytes_accessed=2 * tok * width, transcendentals=0),
        compiler_params=pltpu.CompilerParams(vmem_limit_bytes=24 * 2**20),
        name="head",
    )(*[pltpu.with_memory_space_constraint(x, pltpu.HBM) for x in (ids, norm_gain, tokens)])


def join_sums(low, high):
    cut, width = low[0].shape
    rows = cut + high[0].shape[0]

    def body(*refs):
        out = refs[-1]
        for k, at in ((0, slice(0, cut)), (1, slice(cut, rows))):
            a, b, c = (r[...].astype(F32) for r in refs[3 * k : 3 * k + 3])
            out[at, :] = (a + b + c).astype(BF16)

    return pl.pallas_call(
        body,
        out_shape=jax.ShapeDtypeStruct((rows, width), BF16),
        cost_estimate=pl.CostEstimate(flops=3 * rows * width, bytes_accessed=8 * rows * width, transcendentals=0),
        compiler_params=pltpu.CompilerParams(vmem_limit_bytes=16 * 2**20),
        name="join_sums",
    )(*low, *high)


def early_near(pick, pieces, n_slices):
    rows = pick.shape[0]

    def body(pick_ref, *refs):
        xs, out, buf, sems = refs[: len(pieces)], refs[-3], refs[-2], refs[-1]
        copies = Copies(sems)
        waits = []
        for k, (number, _) in enumerate(pieces):
            buf[k] = jnp.dot(pick_ref[...], xs[k][:, :EARLY], preferred_element_type=F32).astype(BF16)
            waits.append(copies.start(buf.at[k], out.at[:, pl.ds(number * EARLY, EARLY)]))
        for w in waits:
            w.wait()

    return pl.pallas_call(
        body,
        out_specs=pl.BlockSpec(memory_space=pltpu.HBM),
        out_shape=jax.ShapeDtypeStruct((rows, n_slices * EARLY + SIDE), BF16),
        scratch_shapes=[pltpu.VMEM((len(pieces), rows, EARLY), BF16), pltpu.SemaphoreType.DMA((len(pieces),))],
        compiler_params=pltpu.CompilerParams(vmem_limit_bytes=16 * 2**20),
        name="early_near",
    )(pick, *[x for _, x in pieces])


def early_rest(pick, number, halves, others, partial, d_all):
    rows, _ = pick.shape

    def body(pick_ref, low, high, *refs):
        xs, (_, out, buf, sems) = refs[: len(others)], refs[len(others) :]
        copies = Copies(sems)
        total = jnp.concatenate([r[:, EARLY:].astype(F32) for r in (low, high)], axis=0)
        for x in xs:
            total = total + x[:, EARLY:].astype(F32)
        inverse = lax.rsqrt(jnp.sum(total, axis=1, keepdims=True) / d_all + epsilon)
        x = jnp.concatenate([low[:, :EARLY], high[:, :EARLY]], axis=0)
        buf[:, :EARLY] = jnp.dot(pick_ref[...], x, preferred_element_type=F32).astype(BF16)
        first = copies.start(buf.at[:, pl.ds(0, EARLY)], out.at[:, pl.ds(number * EARLY, EARLY)])
        buf[:, EARLY:] = jnp.dot(pick_ref[...], side_columns(inverse), preferred_element_type=F32).astype(BF16)
        second = copies.start(buf.at[:, pl.ds(EARLY, SIDE)], out.at[:, pl.ds(partial.shape[1] - SIDE, SIDE)])
        first.wait()
        second.wait()

    vmem, hbm = pl.BlockSpec(memory_space=pltpu.VMEM), pl.BlockSpec(memory_space=pltpu.HBM)
    return pl.pallas_call(
        body,
        in_specs=[vmem] * (3 + len(others)) + [hbm],
        out_specs=hbm,
        out_shape=jax.ShapeDtypeStruct(partial.shape, BF16),
        scratch_shapes=[pltpu.VMEM((rows, EARLY + SIDE), BF16), pltpu.SemaphoreType.DMA((2,))],
        input_output_aliases={3 + len(others): 0},
        compiler_params=pltpu.CompilerParams(vmem_limit_bytes=16 * 2**20),
        name="early_rest",
    )(pick, *halves, *others, partial)


def local(tokens, norm_gain, expert_ids, gate_prob, w_gate, w_up, w_down):
    window, n_tp = lax.axis_size("ep"), lax.axis_size("tp")
    where = lax.axis_index("tp").astype(jnp.int32).reshape(1)
    w_gate, w_up, w_down = w_gate[0], w_up[0], w_down[0]
    tok = tokens.shape[0]
    rows = window * CAP
    up = [(i, (i + 1) % n_tp) for i in range(n_tp)]
    dn = [(i, (i - 1) % n_tp) for i in range(n_tp)]

    def send_up(x):
        return lax.ppermute(x, "tp", up)

    def send_dn(x):
        return lax.ppermute(x, "tp", dn)

    def spread(x):
        half = x.shape[0] // 2
        below, above = send_up(x), send_dn(x)
        return below, above, send_up(below[:half]), send_dn(above[half:])

    def fold(own, above, below, far_a, far_b):
        half = own.shape[0] // 2
        got_a, got_b = send_up(far_a), send_dn(far_b)
        sum_up = (above.astype(F32) + jnp.pad(got_a.astype(F32), ((0, half), (0, 0)))).astype(BF16)
        sum_dn = (below.astype(F32) + jnp.pad(got_b.astype(F32), ((half, 0), (0, 0)))).astype(BF16)
        from_dn, from_up = send_up(sum_up), send_dn(sum_dn)
        return (own.astype(F32) + from_dn.astype(F32) + from_up.astype(F32)).astype(BF16)

    def spread_halves(low, high):
        below_low, above_high = send_up(low), send_dn(high)
        below_high, above_low = send_up(high), send_dn(low)
        far = send_up(below_low), send_dn(above_high)
        return (below_low, below_high), (above_low, above_high), far

    def add(*terms):
        return sum(t.astype(F32) for t in terms).astype(BF16)

    def fold_halves(own, above, below, far):
        got_low, got_high = send_up(far[0]), send_dn(far[1])
        dn_high, up_low = send_up(above[1]), send_dn(below[0])
        dn_low = send_up(add(above[0], got_low))
        up_high = send_dn(add(below[1], got_high))
        return join_sums((own[0], dn_low, up_low), (own[1], dn_high, up_high))

    def exchange(x):
        shaped = x.reshape(window, CAP, x.shape[1])
        return lax.all_to_all(shaped, "ep", 0, 0, tiled=True).reshape(rows, x.shape[1])

    bulk = tokens.shape[1] - EARLY
    cut = rows // 2 + CAP
    ids, probs = expert_ids.T, gate_prob.T.astype(F32)
    pick, picked_bulk, early = head(tokens, norm_gain, ids, window)
    same = ids[:, None, :] == jnp.arange(window, dtype=jnp.int32)[None, :, None]
    prob = jnp.sum(jnp.where(same, probs[:, None, :], 0.0), axis=0)
    by_slot = jnp.broadcast_to(prob[:, None, :], (window, CAP, tok)).reshape(rows, tok)
    weight = jnp.where(pick > 0, by_slot, 0.0).astype(BF16)

    e_below, e_above, e_far_a, e_far_b = spread(early)
    mine = exchange(picked_bulk)
    picked_near = early_near(pick, ((0, early), (1, e_above), (3, e_below)), n_tp)
    picked = early_rest(pick, 2, (e_far_a, e_far_b), (early, e_above, e_below), picked_near, D)
    early_rows = exchange(picked)
    below, above, far = spread_halves(mine[:cut], mine[cut:])

    weights = (w_gate, w_up, w_down)
    low, high = (0, cut), (cut, rows - cut)
    far_segs = [((0, 1), 2, EARLY, bulk, 0)]
    far_jobs = [
        (2, EARLY, bulk, 0, rows, ((0, *low, 0), (1, *high, 0))),
        (1, EARLY, bulk, *high, ((2, 0, rows - cut, 0),)),
        (3, EARLY, bulk, *low, ((3, 0, cut, 0),)),
    ]
    sums = expert_call(where, weights, [mine], [((0,), 0, EARLY, bulk, 0)])
    sums = expert_call(
        where, weights, [*above, *below],
        [((0, 1), 1, EARLY, bulk, 0), ((2, 3), 3, EARLY, bulk, 0)], sums, leave=True,
    )
    early_jobs = [(k, 0, EARLY, 0, rows, ((0, 0, rows, k * EARLY),)) for k in range(n_tp)]
    gate_sum, up_sum, scale, *far_held = expert_call(
        where, weights, [early_rows], [((0,), k, 0, EARLY, k * EARLY) for k in range(n_tp)],
        stored=sums, keep=(0, n_tp * EARLY), stash=(far_segs, far_jobs[:1]),
    )
    hidden, f_low, f_high, a_high, b_low = expert_call(
        where, weights, [*far, scale], far_segs, (gate_sum, up_sum), inv=2,
        jobs=far_jobs, outs=[(cut, bulk), (rows - cut, bulk), (rows - cut, bulk), (cut, bulk)], held=far_held,
    )
    (p_early,) = expert_call(where, weights, hidden=hidden, jobs=early_jobs, outs=[(rows, n_tp * EARLY)], leave=True)
    a_low, b_high, o_low, o_high = expert_call(
        where, weights, hidden=hidden,
        jobs=[
            (1, EARLY, bulk, *low, ((0, 0, cut, 0),)),
            (3, EARLY, bulk, *high, ((1, 0, rows - cut, 0),)),
            (0, EARLY, bulk, 0, rows, ((2, *low, 0), (3, *high, 0))),
        ],
        outs=[(cut, bulk), (rows - cut, bulk)] * 2,
    )

    def combine(back):
        return lax.dot_general(weight, back, (((0,), (0,)), ((), ())), preferred_element_type=F32).astype(BF16)

    early_back = combine(exchange(p_early))
    e = [early_back[:, k * EARLY : (k + 1) * EARLY] for k in range(n_tp)]
    out_early = fold(e[0], e[1], e[3], e[2][: tok // 2], e[2][tok // 2 :])
    folded = fold_halves((o_low, o_high), (a_low, a_high), (b_low, b_high), (f_low, f_high))
    out_bulk = combine(exchange(folded))
    return jnp.concatenate([out_early, out_bulk], axis=1)


def solution(mesh):
    placed = (
        P("ep", "tp"),
        P("tp"),
        P("ep", None),
        P("ep", None),
        P("ep", None, "tp"),
        P("ep", None, "tp"),
        P("ep", "tp", None),
    )

    return jax.shard_map(local, mesh=mesh, in_specs=placed, out_specs=P("ep", "tp"), check_vma=False)
```

```python
import jax
import jax.numpy as jnp
from jax import lax
from jax.experimental import pallas as pl
from jax.experimental.pallas import tpu as pltpu
from jax.sharding import PartitionSpec as P


D = 7168
epsilon = 1e-06
CAP = 16
EARLY = 512
SIDE = 128
F32, BF16 = jnp.float32, jnp.bfloat16


class Copies:
    def __init__(self, sems):
        self.sems, self.used = sems, 0

    def start(self, src, dst):
        copy = pltpu.make_async_copy(src, dst, self.sems.at[self.used])
        self.used += 1
        copy.start()
        return copy


def expert_call(where, weights, xs=(), segs=(), carry=(), inv=None, hidden=None, jobs=(), outs=(), stash=((), ()), held=(), stored=(), keep=None, leave=False):
    slices = lax.axis_size("tp")
    w_gate, w_up, w_down = weights
    d_all, ff = w_gate.shape
    span = d_all // slices
    finish = bool(segs) and bool(jobs)
    rows = hidden.shape[0] if hidden is not None else sum(xs[i].shape[0] for i in segs[0][0])

    def columns_of(some):
        found = []
        for step, offset, width, *_ in some:
            if (step, offset, width) not in found:
                found.append((step, offset, width))
        return found

    def weight_shapes(seg_list, column_list):
        shapes = []
        for _, _, _, width, _ in seg_list:
            shapes += [(width, ff)] * 2
        return shapes + [(ff, width) for _, _, width in column_list]

    columns, later = columns_of(jobs), columns_of(stash[1])
    results = [((rows, ff), F32)] * 2 if not jobs else [((rows, ff), BF16)] * finish + [(s, BF16) for s in outs]
    results = [(s, t) for s, t in results] + ([((rows, SIDE), BF16)] if keep else [])
    n_out = len(results)
    results += [(s, BF16) for s in weight_shapes(stash[0], later)]
    needed = weight_shapes(segs, columns)[len(held) :]
    streams = bool(needed) or len(results) > n_out
    resident = list(xs) + list(carry) + ([] if hidden is None else [hidden]) + list(held)
    streamed = ([w_gate, w_up, w_down] if streams else []) + list(stored)
    scratch = [pltpu.VMEM(s, BF16) for s in needed]
    if finish:
        scratch += [pltpu.VMEM((rows, ff), F32)] * 2
    scratch += [pltpu.VMEM((rows, ff), F32)] * len(stored)
    scratch += ([pltpu.VMEM(s, BF16) for s in outs] or [pltpu.VMEM((rows, ff), F32)] * 2) * leave
    n_copies = (len(jobs) or 2) * leave + len(stored) + len(needed) + len(results) - n_out
    scratch += [pltpu.SemaphoreType.DMA((max(n_copies, 1),))]

    def body(where_ref, *refs):
        refs = list(refs)
        take = lambda n: [refs.pop(0) for _ in range(n)]
        x_refs, carried = take(len(xs)), take(len(carry))
        hidden_ref = take(hidden is not None)
        held_refs = take(len(held))
        wg, wu, wd = take(3) if streams else (None,) * 3
        stored_refs = take(len(stored))
        out_refs = take(len(results))
        bufs = held_refs + take(len(needed))
        accs = take(2) if finish else out_refs[:2]
        stored_bufs = take(len(stored))
        staged = take(leave * (len(outs) or 2))
        accs = staged if leave and not jobs else accs
        copies = Copies(refs.pop(0))
        z = where_ref[0]

        def bring(seg_list, column_list, into, skip):
            waits, n = [None] * skip, 0
            for _, step, offset, width, _ in seg_list:
                at = pl.ds(pl.multiple_of(lax.rem(z + step, slices) * span + offset, 128), width)
                for w in (wg, wu):
                    if n >= skip:
                        waits.append(copies.start(w.at[at, :], into[n]))
                    n += 1
            for step, offset, width in column_list:
                at = pl.ds(pl.multiple_of(lax.rem(z + step, slices) * span + offset, 128), width)
                if n >= skip:
                    waits.append(copies.start(wd.at[:, at], into[n]))
                n += 1
            return waits

        def arrived(wait):
            if wait is not None:
                wait.wait()

        waits = bring(segs, columns, bufs, len(held))
        stored_waits = [copies.start(r, b) for r, b in zip(stored_refs, stored_bufs)]
        stash_waits = bring(stash[0], later, out_refs[n_out:], 0)
        if keep:
            out_refs[2][...] = x_refs[keep[0]][:, keep[1] : keep[1] + SIDE]
        for k, (index, _, _, width, col) in enumerate(segs):
            x = [x_refs[i][:, col : col + width] for i in index]
            x = x[0] if len(x) == 1 else jnp.concatenate(x, axis=0)
            for n, acc in enumerate(accs):
                arrived(waits[2 * k + n])
                term = jnp.dot(x, bufs[2 * k + n][...], preferred_element_type=F32)
                if k:
                    term = acc[...] + term
                elif carry:
                    term = carried[n][...] + term
                if stored and k == len(segs) - 1:
                    stored_waits[n].wait()
                    term = stored_bufs[n][...] + term
                acc[...] = term
                if leave and not jobs and k == len(segs) - 1:
                    stash_waits.append(copies.start(acc, out_refs[n]))
        if finish:
            scale = jnp.sum(x_refs[inv][...].astype(F32), axis=1, keepdims=True)
            gate = accs[0][...] * scale
            hidden_ref = [out_refs.pop(0)]
            hidden_ref[0][...] = (jax.nn.silu(gate) * (accs[1][...] * scale)).astype(BF16)
        waited = set()
        for step, offset, width, row, count, targets in jobs:
            k = columns.index((step, offset, width))
            if k not in waited:
                arrived(waits[2 * len(segs) + k])
                waited.add(k)
            w = bufs[2 * len(segs) + k]
            term = jnp.dot(hidden_ref[0][row : row + count, :], w[...], preferred_element_type=F32).astype(BF16)
            for index, top, n, col in targets:
                to = staged[0] if leave else out_refs[index]
                to[:, col : col + width] = term[top : top + n, :]
                if leave:
                    at = pl.ds(col, width)
                    stash_waits.append(copies.start(to.at[:, at], out_refs[index].at[:, at]))
        for w in stash_waits:
            w.wait()

    vmem, hbm = pl.BlockSpec(memory_space=pltpu.VMEM), pl.BlockSpec(memory_space=pltpu.HBM)
    flops = sum(4 * rows * s[3] * ff for s in segs) + sum(2 * j[4] * ff * j[2] for j in jobs)
    return pl.pallas_call(
        body,
        in_specs=[pl.BlockSpec(memory_space=pltpu.SMEM)] + [vmem] * len(resident) + [hbm] * len(streamed),
        out_specs=[hbm if leave else vmem] * len(results),
        out_shape=[(pltpu.HBM if leave else pltpu.VMEM)(s, t) for s, t in results],
        scratch_shapes=scratch,
        cost_estimate=pl.CostEstimate(flops=flops, bytes_accessed=flops // 256, transcendentals=0),
        compiler_params=pltpu.CompilerParams(vmem_limit_bytes=20 * 2**20),
    )(
        where,
        *[pltpu.with_memory_space_constraint(x, pltpu.VMEM) for x in resident],
        *[pltpu.with_memory_space_constraint(x, pltpu.HBM) for x in streamed],
    )


def side_columns(value):
    lane = lax.broadcasted_iota(jnp.int32, (value.shape[0], SIDE), 1)
    out = jnp.zeros((value.shape[0], SIDE), F32)
    for k in range(3):
        term = value.astype(BF16).astype(F32)
        out = jnp.where(lane == k, term, out)
        value = value - term
    return out.astype(BF16)


def head(tokens, norm_gain, ids, window):
    tok, width = tokens.shape
    rows, bulk = window * CAP, width - EARLY

    def body(ids_hbm, gain_hbm, tokens_hbm, pick_ref, bulk_ref, early_ref, ids_ref, gain_ref, tokens_ref, sems):
        copies = Copies(sems)
        pairs = ((ids_hbm, ids_ref), (gain_hbm, gain_ref), (tokens_hbm, tokens_ref))
        ids_load, gain_load, load = [copies.start(*pair) for pair in pairs]
        ids_load.wait()
        expert = lax.broadcasted_iota(jnp.int32, (window, tok), 0)
        match = jnp.zeros((window, tok), F32)
        for k in range(ids.shape[0]):
            match = match + jnp.where(ids_ref[k : k + 1, :] == expert, 1.0, 0.0)
        earlier = lax.broadcasted_iota(jnp.int32, (tok, tok), 0) < lax.broadcasted_iota(jnp.int32, (tok, tok), 1)
        earlier = jnp.where(earlier, 1.0, 0.0).astype(BF16)
        before = jnp.dot(match.astype(BF16), earlier, preferred_element_type=F32)
        slot = jnp.where(match > 0.0, before, -1.0)
        row = lax.broadcasted_iota(jnp.int32, (rows, window), 0)
        own = (row // CAP) == lax.broadcasted_iota(jnp.int32, (rows, window), 1)
        spread = jnp.dot(jnp.where(own, 1.0, 0.0).astype(BF16), slot.astype(BF16), preferred_element_type=F32)
        wanted = (lax.broadcasted_iota(jnp.int32, (rows, tok), 0) % CAP).astype(F32)
        pick = jnp.where(spread == wanted, 1.0, 0.0).astype(BF16)
        pick_ref[...] = pick
        gain_load.wait()
        gain = gain_ref[...].astype(F32).reshape(1, width)
        load.wait()
        values = tokens_ref[...].astype(F32)
        gained = (values * gain).astype(BF16)
        bulk_ref[...] = jnp.dot(pick, gained[:, EARLY:], preferred_element_type=F32).astype(BF16)
        early_ref[:, :EARLY] = gained[:, :EARLY]
        early_ref[:, EARLY:] = side_columns(jnp.sum(values * values, axis=1, keepdims=True))

    return pl.pallas_call(
        body,
        in_specs=[pl.BlockSpec(memory_space=pltpu.HBM)] * 3,
        scratch_shapes=[pltpu.VMEM(x.shape, x.dtype) for x in (ids, norm_gain, tokens)] + [pltpu.SemaphoreType.DMA((3,))],
        out_shape=[jax.ShapeDtypeStruct(s, BF16) for s in ((rows, tok), (rows, bulk), (tok, EARLY + SIDE))],
        cost_estimate=pl.CostEstimate(flops=2 * rows * tok * bulk, bytes_accessed=2 * tok * width, transcendentals=0),
        compiler_params=pltpu.CompilerParams(vmem_limit_bytes=24 * 2**20),
        name="head",
    )(*[pltpu.with_memory_space_constraint(x, pltpu.HBM) for x in (ids, norm_gain, tokens)])


def join_sums(low, high):
    cut, width = low[0].shape
    rows = cut + high[0].shape[0]

    def body(*refs):
        out = refs[-1]
        for k, at in ((0, slice(0, cut)), (1, slice(cut, rows))):
            a, b, c = (r[...].astype(F32) for r in refs[3 * k : 3 * k + 3])
            out[at, :] = (a + b + c).astype(BF16)

    return pl.pallas_call(
        body,
        out_shape=jax.ShapeDtypeStruct((rows, width), BF16),
        cost_estimate=pl.CostEstimate(flops=3 * rows * width, bytes_accessed=8 * rows * width, transcendentals=0),
        compiler_params=pltpu.CompilerParams(vmem_limit_bytes=16 * 2**20),
        name="join_sums",
    )(*low, *high)


def early_near(pick, pieces, n_slices):
    rows = pick.shape[0]

    def body(pick_ref, *refs):
        xs, out, buf, sems = refs[: len(pieces)], refs[-3], refs[-2], refs[-1]
        copies = Copies(sems)
        waits = []
        for k, (number, _) in enumerate(pieces):
            buf[k] = jnp.dot(pick_ref[...], xs[k][:, :EARLY], preferred_element_type=F32).astype(BF16)
            waits.append(copies.start(buf.at[k], out.at[:, pl.ds(number * EARLY, EARLY)]))
        for w in waits:
            w.wait()

    return pl.pallas_call(
        body,
        out_specs=pl.BlockSpec(memory_space=pltpu.HBM),
        out_shape=jax.ShapeDtypeStruct((rows, n_slices * EARLY + SIDE), BF16),
        scratch_shapes=[pltpu.VMEM((len(pieces), rows, EARLY), BF16), pltpu.SemaphoreType.DMA((len(pieces),))],
        compiler_params=pltpu.CompilerParams(vmem_limit_bytes=16 * 2**20),
        name="early_near",
    )(pick, *[x for _, x in pieces])


def early_rest(pick, number, halves, others, partial, d_all):
    rows, _ = pick.shape

    def body(pick_ref, low, high, *refs):
        xs, (_, out, buf, sems) = refs[: len(others)], refs[len(others) :]
        copies = Copies(sems)
        total = jnp.concatenate([r[:, EARLY:].astype(F32) for r in (low, high)], axis=0)
        for x in xs:
            total = total + x[:, EARLY:].astype(F32)
        inverse = lax.rsqrt(jnp.sum(total, axis=1, keepdims=True) / d_all + epsilon)
        x = jnp.concatenate([low[:, :EARLY], high[:, :EARLY]], axis=0)
        buf[:, :EARLY] = jnp.dot(pick_ref[...], x, preferred_element_type=F32).astype(BF16)
        first = copies.start(buf.at[:, pl.ds(0, EARLY)], out.at[:, pl.ds(number * EARLY, EARLY)])
        buf[:, EARLY:] = jnp.dot(pick_ref[...], side_columns(inverse), preferred_element_type=F32).astype(BF16)
        second = copies.start(buf.at[:, pl.ds(EARLY, SIDE)], out.at[:, pl.ds(partial.shape[1] - SIDE, SIDE)])
        first.wait()
        second.wait()

    vmem, hbm = pl.BlockSpec(memory_space=pltpu.VMEM), pl.BlockSpec(memory_space=pltpu.HBM)
    return pl.pallas_call(
        body,
        in_specs=[vmem] * (3 + len(others)) + [hbm],
        out_specs=hbm,
        out_shape=jax.ShapeDtypeStruct(partial.shape, BF16),
        scratch_shapes=[pltpu.VMEM((rows, EARLY + SIDE), BF16), pltpu.SemaphoreType.DMA((2,))],
        input_output_aliases={3 + len(others): 0},
        compiler_params=pltpu.CompilerParams(vmem_limit_bytes=16 * 2**20),
        name="early_rest",
    )(pick, *halves, *others, partial)


def local(tokens, norm_gain, expert_ids, gate_prob, w_gate, w_up, w_down):
    window, n_tp = lax.axis_size("ep"), lax.axis_size("tp")
    where = lax.axis_index("tp").astype(jnp.int32).reshape(1)
    w_gate, w_up, w_down = w_gate[0], w_up[0], w_down[0]
    tok = tokens.shape[0]
    rows = window * CAP
    up = [(i, (i + 1) % n_tp) for i in range(n_tp)]
    dn = [(i, (i - 1) % n_tp) for i in range(n_tp)]

    def send_up(x):
        return lax.ppermute(x, "tp", up)

    def send_dn(x):
        return lax.ppermute(x, "tp", dn)

    def spread(x):
        half = x.shape[0] // 2
        below, above = send_up(x), send_dn(x)
        return below, above, send_up(below[:half]), send_dn(above[half:])

    def fold(own, above, below, far_a, far_b):
        half = own.shape[0] // 2
        got_a, got_b = send_up(far_a), send_dn(far_b)
        sum_up = (above.astype(F32) + jnp.pad(got_a.astype(F32), ((0, half), (0, 0)))).astype(BF16)
        sum_dn = (below.astype(F32) + jnp.pad(got_b.astype(F32), ((half, 0), (0, 0)))).astype(BF16)
        from_dn, from_up = send_up(sum_up), send_dn(sum_dn)
        return (own.astype(F32) + from_dn.astype(F32) + from_up.astype(F32)).astype(BF16)

    def spread_halves(low, high):
        below_low, above_high = send_up(low), send_dn(high)
        below_high, above_low = send_up(high), send_dn(low)
        far = send_up(below_low), send_dn(above_high)
        return (below_low, below_high), (above_low, above_high), far

    def add(*terms):
        return sum(t.astype(F32) for t in terms).astype(BF16)

    def fold_halves(own, above, below, far):
        got_low, got_high = send_up(far[0]), send_dn(far[1])
        dn_high, up_low = send_up(above[1]), send_dn(below[0])
        dn_low = send_up(add(above[0], got_low))
        up_high = send_dn(add(below[1], got_high))
        return join_sums((own[0], dn_low, up_low), (own[1], dn_high, up_high))

    def exchange(x):
        shaped = x.reshape(window, CAP, x.shape[1])
        return lax.all_to_all(shaped, "ep", 0, 0, tiled=True).reshape(rows, x.shape[1])

    bulk = tokens.shape[1] - EARLY
    cut = rows // 2
    ids, probs = expert_ids.T, gate_prob.T.astype(F32)
    pick, picked_bulk, early = head(tokens, norm_gain, ids, window)
    same = ids[:, None, :] == jnp.arange(window, dtype=jnp.int32)[None, :, None]
    prob = jnp.sum(jnp.where(same, probs[:, None, :], 0.0), axis=0)
    by_slot = jnp.broadcast_to(prob[:, None, :], (window, CAP, tok)).reshape(rows, tok)
    weight = jnp.where(pick > 0, by_slot, 0.0).astype(BF16)

    e_below, e_above, e_far_a, e_far_b = spread(early)
    mine = exchange(picked_bulk)
    picked_near = early_near(pick, ((0, early), (1, e_above), (3, e_below)), n_tp)
    picked = early_rest(pick, 2, (e_far_a, e_far_b), (early, e_above, e_below), picked_near, D)
    early_rows = exchange(picked)
    below, above, far = spread_halves(mine[:cut], mine[cut:])

    weights = (w_gate, w_up, w_down)
    low, high = (0, cut), (cut, rows - cut)
    far_segs = [((0, 1), 2, EARLY, bulk, 0)]
    far_jobs = [
        (2, EARLY, bulk, 0, rows, ((0, *low, 0), (1, *high, 0))),
        (1, EARLY, bulk, *high, ((2, 0, rows - cut, 0),)),
        (3, EARLY, bulk, *low, ((3, 0, cut, 0),)),
    ]
    sums = expert_call(where, weights, [mine], [((0,), 0, EARLY, bulk, 0)])
    sums = expert_call(
        where, weights, [*above, *below],
        [((0, 1), 1, EARLY, bulk, 0), ((2, 3), 3, EARLY, bulk, 0)], sums, leave=True,
    )
    early_jobs = [(k, 0, EARLY, 0, rows, ((0, 0, rows, k * EARLY),)) for k in range(n_tp)]
    gate_sum, up_sum, scale, *far_held = expert_call(
        where, weights, [early_rows], [((0,), k, 0, EARLY, k * EARLY) for k in range(n_tp)],
        keep=(0, n_tp * EARLY), stash=(far_segs, far_jobs),
    )
    hidden, f_low, f_high, a_high, b_low = expert_call(
        where, weights, [*far, scale], far_segs, (gate_sum, up_sum), inv=2, stored=sums,
        jobs=far_jobs, outs=[(cut, bulk), (rows - cut, bulk), (rows - cut, bulk), (cut, bulk)], held=far_held,
    )
    (p_early,) = expert_call(where, weights, hidden=hidden, jobs=early_jobs, outs=[(rows, n_tp * EARLY)], leave=True)
    a_low, b_high, o_low, o_high = expert_call(
        where, weights, hidden=hidden,
        jobs=[
            (1, EARLY, bulk, *low, ((0, 0, cut, 0),)),
            (3, EARLY, bulk, *high, ((1, 0, rows - cut, 0),)),
            (0, EARLY, bulk, 0, rows, ((2, *low, 0), (3, *high, 0))),
        ],
        outs=[(cut, bulk), (rows - cut, bulk)] * 2,
    )

    def combine(back):
        return lax.dot_general(weight, back, (((0,), (0,)), ((), ())), preferred_element_type=F32).astype(BF16)

    early_back = combine(exchange(p_early))
    e = [early_back[:, k * EARLY : (k + 1) * EARLY] for k in range(n_tp)]
    out_early = fold(e[0], e[1], e[3], e[2][: tok // 2], e[2][tok // 2 :])
    folded = fold_halves((o_low, o_high), (a_low, a_high), (b_low, b_high), (f_low, f_high))
    out_bulk = combine(exchange(folded))
    return jnp.concatenate([out_early, out_bulk], axis=1)


def solution(mesh):
    placed = (
        P("ep", "tp"),
        P("tp"),
        P("ep", None),
        P("ep", None),
        P("ep", None, "tp"),
        P("ep", None, "tp"),
        P("ep", "tp", None),
    )

    return jax.shard_map(local, mesh=mesh, in_specs=placed, out_specs=P("ep", "tp"), check_vma=False)
```
